32 devices in a mesh: px: 4 (over y, x), py: 8 (over z, core).
Axes of the slice: x: 2, y: 2, z: 4, core: 2. Of those that a mesh axis runs over, the one named last changes fastest.
Arguments:
- velocity: float32 [3, 8, 256, 1024], P(None, None, 'py', 'px'), may hold values from -6 to 6
- thickness: float32 [8, 256, 1024], P(None, 'py', 'px'), may hold values from 1 to 4
- velocity_tendency: float32 [3, 8, 256, 1024], P(None, None, 'py', 'px'), may hold values from -6 to 6
- thickness_tendency: float32 [8, 256, 1024], P(None, 'py', 'px'), may hold values from -0.5 to 0.5
- cell_distance: float32 [3, 256, 1024], P(None, 'py', 'px'), may hold values from 0.5 to 2
- edge_length: float32 [3, 256, 1024], P(None, 'py', 'px'), may hold values from 0.5 to 2
- cell_area: float32 [256, 1024], P('py', 'px'), may hold values from 1 to 4
- kite_area: float32 [2, 3, 256, 1024], P(None, None, 'py', 'px'), may hold values from 0.2 to 0.8
- coriolis: float32 [2, 256, 1024], P(None, 'py', 'px'), may hold values from -1 to 1
Outputs:
- vertex_potential: float32 [2, 8, 256, 1024], P(None, None, 'py', 'px')
- kinetic_energy: float32 [8, 256, 1024], P(None, 'py', 'px')
- cell_potential: float32 [8, 256, 1024], P(None, 'py', 'px')
- edge_potential: float32 [3, 8, 256, 1024], P(None, None, 'py', 'px')
The draws below stay inside these ranges and needn't reach their ends.
All inputs are finite; a program needn't handle non-finite values.
Results may differ from the reference program's by a relative error of at most 0.00002.
Values sent between devices are 32-bit elements; how exact they have to be, the bound alone decides.
A program may use at most 64 MiB of HBM per device.

```python
import math
import jax
import jax.numpy as jnp

NLEV = 8
SECTIONS = 4
NX = 256
NY = 1024


def levels(key, shape, split, least, top_value):
    def one(position, blocks):
        draws = jax.random.uniform(jax.random.fold_in(jax.random.fold_in(key, 6), position), (blocks,), jnp.float32, least / len(split), top_value / len(split))
        return jnp.repeat(jnp.exp(draws), shape[position] // blocks).reshape((-1,) + (1,) * (len(shape) - position - 1))

    loudness = one(*split[0])
    for cut in split[1:]:
        loudness = loudness * one(*cut)
    return loudness


def noise(own_key, extent, scale, bound, shards=(), dtype=jnp.bfloat16):
    values = scale * jax.random.normal(own_key, extent, jnp.float32)
    if shards:
        values = values * levels(own_key, extent, shards, -0.22, 0.18)
    return jnp.clip(values, -bound, bound).astype(dtype)


def setup_inputs(seed: int = 0) -> dict:
    arg_keys = jax.random.split(jax.random.key(seed), 10)
    velocity = noise(arg_keys[0], (3, NLEV, NX, NY), 1.0, 6.0, ((2, 8), (3, 4)), jnp.float32)
    thickness = jnp.clip(jnp.exp(math.log(4.0) - 1.3862944 * jax.random.uniform(arg_keys[1], (NLEV, NX, NY), jnp.float32) ** levels(arg_keys[1], (NLEV, NX, NY), ((1, 8), (2, 4)), -0.2, 0.2)), 1.0, 4.0)
    velocity_tendency = noise(arg_keys[2], (3, NLEV, NX, NY), 1.0, 6.0, ((2, 8), (3, 4)), jnp.float32)
    thickness_tendency = jnp.clip(jax.random.uniform(arg_keys[3], (NLEV, NX, NY), jnp.float32, -0.5, 0.5) * levels(arg_keys[3], (NLEV, NX, NY), ((1, 8), (2, 4)), -0.4, 0.0), -0.5, 0.5)
    cell_distance = jnp.clip(jnp.exp(math.log(2.0) - 1.3862944 * jax.random.uniform(arg_keys[4], (3, NX, NY), jnp.float32) ** levels(arg_keys[4], (3, NX, NY), ((1, 8), (2, 4)), -0.2, 0.2)), 0.5, 2.0)
    edge_length = jnp.clip(jnp.exp(math.log(2.0) - 1.3862944 * jax.random.uniform(arg_keys[5], (3, NX, NY), jnp.float32) ** levels(arg_keys[5], (3, NX, NY), ((1, 8), (2, 4)), -0.2, 0.2)), 0.5, 2.0)
    cell_area = jnp.clip(jnp.exp(math.log(4.0) - 1.3862944 * jax.random.uniform(arg_keys[6], (NX, NY), jnp.float32) ** levels(arg_keys[6], (NX, NY), ((0, 8), (1, 4)), -0.2, 0.2)), 1.0, 4.0)
    kite_area = jnp.clip(jnp.exp(math.log(0.8) - 1.3862944 * jax.random.uniform(arg_keys[7], (2, 3, NX, NY), jnp.float32) ** levels(arg_keys[7], (2, 3, NX, NY), ((2, 8), (3, 4)), -0.2, 0.2)), 0.2, 0.8)
    coriolis = jnp.clip(jax.random.uniform(arg_keys[8], (2, NX, NY), jnp.float32, -1.0, 1.0) * levels(arg_keys[8], (2, NX, NY), ((1, 8), (2, 4)), -0.4, 0.0), -1.0, 1.0)
    return dict(velocity=velocity, thickness=thickness, velocity_tendency=velocity_tendency, thickness_tendency=thickness_tendency, cell_distance=cell_distance, edge_length=edge_length, cell_area=cell_area, kite_area=kite_area, coriolis=coriolis)


SECTION_STEP = (0.0, 0.5, 0.5, 1.0)
SECTION_WEIGHT = (1.0 / 6.0, 1.0 / 3.0, 1.0 / 3.0, 1.0 / 6.0)
UPWIND_FACTOR = 0.5


def neighbour(field, first_off, second_off):
    return jnp.roll(field, (-first_off, -second_off), axis=(-2, -1))


def reference(velocity, thickness, velocity_tendency, thickness_tendency, cell_distance, edge_length, cell_area, kite_area, coriolis):
    triangle_area = jnp.sum(kite_area, axis=1)
    edge_weight = 0.25 * cell_distance * edge_length
    vertex_total = jnp.zeros((2,) + thickness.shape, jnp.float32)
    energy_total = jnp.zeros(thickness.shape, jnp.float32)
    cell_total = jnp.zeros(thickness.shape, jnp.float32)
    edge_total = jnp.zeros(velocity.shape, jnp.float32)
    for section_index in range(SECTIONS):
        step_size = SECTION_STEP[section_index]
        weight_now = SECTION_WEIGHT[section_index]
        section_velocity = velocity + step_size * velocity_tendency
        section_thickness = thickness + step_size * thickness_tendency
        edge_flux = section_velocity * cell_distance[:, None]
        circulation_first = edge_flux[0] + neighbour(edge_flux[2], 1, 0) - edge_flux[1]
        circulation_second = edge_flux[1] - edge_flux[2] - neighbour(edge_flux[0], -1, 1)
        height_first = (kite_area[0, 0] * section_thickness + kite_area[0, 1] * neighbour(section_thickness, 1, 0)
                        + kite_area[0, 2] * neighbour(section_thickness, 0, 1)) / triangle_area[0]
        height_second = (kite_area[1, 0] * section_thickness + kite_area[1, 1] * neighbour(section_thickness, 0, 1)
                         + kite_area[1, 2] * neighbour(section_thickness, -1, 1)) / triangle_area[1]
        potential_first = (coriolis[0] + circulation_first / triangle_area[0]) / height_first
        potential_second = (coriolis[1] + circulation_second / triangle_area[1]) / height_second
        energy = edge_weight[:, None] * section_velocity * section_velocity
        kinetic = (energy[0] + energy[1] + energy[2] + neighbour(energy[0], -1, 0)
                   + neighbour(energy[1], 0, -1) + neighbour(energy[2], 1, -1)) / cell_area
        cell_value = (potential_first + potential_second + neighbour(potential_first, -1, 0)
                      + neighbour(potential_first, 0, -1) + neighbour(potential_second, 0, -1)
                      + neighbour(potential_second, 1, -1)) / 6.0
        mean_zero = 0.5 * (potential_first + neighbour(potential_second, 1, -1))
        mean_one = 0.5 * (potential_first + potential_second)
        mean_two = 0.5 * (potential_second + neighbour(potential_first, -1, 0))
        grad_zero = (neighbour(cell_value, 1, 0) - cell_value) / cell_distance[0]
        grad_one = (neighbour(cell_value, 0, 1) - cell_value) / cell_distance[1]
        grad_two = (neighbour(cell_value, -1, 1) - cell_value) / cell_distance[2]
        section_edge = jnp.stack([
            mean_zero - UPWIND_FACTOR * section_velocity[0] * grad_zero,
            mean_one - UPWIND_FACTOR * section_velocity[1] * grad_one,
            mean_two - UPWIND_FACTOR * section_velocity[2] * grad_two])
        vertex_total = vertex_total + weight_now * jnp.stack([potential_first, potential_second])
        energy_total = energy_total + weight_now * kinetic
        cell_total = cell_total + weight_now * cell_value
        edge_total = edge_total + weight_now * section_edge
    return vertex_total, energy_total, cell_total, edge_total
```

```python
import jax
import jax.numpy as jnp
from jax import lax
from jax.experimental import pallas as pl
from jax.experimental.pallas import tpu as pltpu
from jax.sharding import PartitionSpec as P

SUB = 8
LANE = 128
GROUP = 16
PAIR = 2
MESH = pl.DeviceIdType.MESH
F32 = jnp.float32
SLOPE = -0.5 / 36.0


def iotas():
    sub = lax.broadcasted_iota(jnp.int32, (SUB, LANE), 0)
    lane = lax.broadcasted_iota(jnp.int32, (SUB, LANE), 1)
    return sub, lane


def roll(x, shift, axis):
    n = (SUB, LANE)[axis]
    return pltpu.roll(x, shift % n, axis) if shift % n else x


def span(r, c):
    return (slice(r * SUB, (r + 1) * SUB), slice(c * LANE, (c + 1) * LANE))


class Field:
    def __init__(self, grid, make):
        self.grid, self.make, self.memo = grid, make, {}

    def __call__(self, r, c):
        key = (r % self.grid[0], c % self.grid[1])
        if key not in self.memo:
            self.memo[key] = self.make(*key)
        return self.memo[key]


def chain(grid, v, h, t, g, dist, ew, kt, ct, swap=lambda i, f: f):
    sub, lane = iotas()

    def lift(fn, *fields):
        return Field(grid, lambda r, c: fn(*[f(r, c) for f in fields]))

    def row_shift(f, a):
        rolled = Field(grid, lambda r, c: roll(f(r, c), -a, 0))
        if grid[0] == 1:
            return rolled
        keep = sub < SUB - 1 if a == 1 else sub > 0
        return Field(grid, lambda r, c: jnp.where(keep, rolled(r, c), rolled(r + a, c)))

    def col_shift(f, b):
        rolled = Field(grid, lambda r, c: roll(f(r, c), -b, 1))
        if grid[1] == 1:
            return rolled
        keep = lane < LANE - 1 if b == 1 else lane > 0
        return Field(grid, lambda r, c: jnp.where(keep, rolled(r, c), rolled(r, c + b)))

    def parts(vv, hh):
        flux = [lift(lambda a, b: a * b, vv[k], dist[k]) for k in range(3)]
        c0 = lift(lambda a, b, c: a + b - c, flux[0], row_shift(flux[2], 1), flux[1])
        c1 = lift(lambda a, b, c: a - b - c, flux[1], flux[2], col_shift(row_shift(flux[0], -1), 1))
        hc = col_shift(hh, 1)
        hr = row_shift(hh, 1)
        hd = row_shift(hc, -1)
        mix = lambda a, b, c, p, q, s: a * p + b * q + c * s
        h0 = lift(mix, kt[0], kt[1], kt[2], hh, hr, hc)
        h1 = lift(mix, kt[3], kt[4], kt[5], hh, hc, hd)
        return (c0, c1), (h0, h1)

    cv, hv = parts(v, h)
    cw, hw = parts(t, g)

    def potential(k):
        def make(r, c):
            a0 = ct[k](r, c) + cv[k](r, c)
            a1 = cw[k](r, c)
            b0 = hv[k](r, c)
            b1 = hw[k](r, c)
            bm, be = b0 + 0.5 * b1, b0 + b1
            m = bm * be
            scale_all = 1.0 / (b0 * m)
            mid = (a0 + a0 + a1) * (b0 * be)
            late = mid + (a0 + a1) * (b0 * bm)
            return (a0 * m + mid + late) * scale_all, late * scale_all

        both = Field(grid, make)
        return Field(grid, lambda r, c: both(r, c)[0]), Field(grid, lambda r, c: both(r, c)[1])

    p0, q0 = potential(0)
    p1, q1 = potential(1)
    add = lambda a, b: a + b
    add3 = lambda a, b, c: a + b + c

    def cell(f0, f1):
        f0_up = row_shift(f0, -1)
        f1_down = row_shift(f1, 1)
        pair = lift(add, f0, f1)
        return lift(add3, pair, f0_up, col_shift(lift(add, pair, f1_down), -1)), f0_up, f1_down, pair

    cc, p0_up, p1_down, pair = cell(p0, p1)
    dd = cell(q0, q1)[0]
    cc, dd = swap(0, cc), swap(1, dd)
    p1_low = col_shift(p1_down, -1)

    def neighbours(f):
        fc = col_shift(f, 1)
        return row_shift(f, 1), fc, row_shift(fc, -1)

    cn, dn = neighbours(cc), neighbours(dd)
    ends = [lift(add, p0, p1_low), pair, lift(add, p1, p0_up)]
    en = [
        lift(lambda w, a, b: w * (a * (a + b) + (1.0 / 3.0) * (b * b)), ew[k], v[k], t[k])
        for k in range(3)
    ]
    e_up = row_shift(en[0], -1)
    e_low = col_shift(lift(add, en[1], row_shift(en[2], 1)), -1)

    def outputs(scale):
        def edge(k):
            def make(r, c):
                slope = v[k](r, c) * (cn[k](r, c) - cc(r, c)) + t[k](r, c) * (dn[k](r, c) - dd(r, c))
                return ends[k](r, c) * (1.0 / 12.0) + scale[k](r, c) * slope

            return Field(grid, make)

        kin = Field(
            grid,
            lambda r, c: (en[0](r, c) + en[1](r, c) + en[2](r, c) + e_up(r, c) + e_low(r, c)) * scale[3](r, c),
        )
        return [
            lift(lambda a: a * (1.0 / 6.0), p0),
            lift(lambda a: a * (1.0 / 6.0), p1),
            kin,
            lift(lambda a: a * (1.0 / 36.0), cc),
        ] + [edge(k) for k in range(3)]

    return cc, dd, outputs


def main_kernel(counts, *refs):
    hbm = refs[:9]
    o_vert, o_kin, o_cell, o_edge = refs[9:13]
    bufs = refs[13:22]
    bands = refs[22:31]
    p_right, p_left, g_right, g_left = refs[31:35]
    geo, kgeo, sgeo, slev, saved = refs[35:40]
    in_sem, own_sem, send_row, recv_row, send_col, recv_col = refs[40:46]
    ny, nx = counts
    py, px = lax.axis_index("py"), lax.axis_index("px")
    down, up = lax.rem(py + 1, ny), lax.rem(py + ny - 1, ny)
    right, left = lax.rem(px + 1, nx), lax.rem(px + nx - 1, nx)

    barrier = pltpu.get_barrier_semaphore()
    near = [
        (up, px), (down, px), (py, left), (py, right),
        (up, left), (up, right), (down, left), (down, right),
    ]
    for y, x in near:
        pl.semaphore_signal(barrier, inc=1, device_id={"py": y, "px": x}, device_id_type=MESH)

    b_vel, b_th, b_vt, b_tt, b_cd, b_el, b_kite, b_cor, b_area = bufs
    levels, rows, cols = b_th.shape
    nr, nc = rows // SUB, cols // LANE
    sub, lane = iotas()
    pos, group = lane & (GROUP - 1), lane >> 4
    head, tail = slice(0, LANE), slice(cols - LANE, cols)

    loads = [pltpu.make_async_copy(a, b, in_sem.at[i]) for i, (a, b) in enumerate(zip(hbm, bufs))]
    for i in (4, 5, 6, 7, 0, 1, 2, 3, 8):
        loads[i].start()

    def part(ref, a, b):
        return ref.at[(slice(None),) * (len(ref.shape) - 2) + (slice(a, b), slice(None))]

    own = []
    for i, (a, b) in enumerate(zip(hbm, bands)):
        own.append(pltpu.make_async_copy(part(a, rows - 2, rows), part(b, 0, 2), own_sem.at[2 * i]))
        own.append(pltpu.make_async_copy(part(a, 0, 2), part(b, 6, 8), own_sem.at[2 * i + 1]))
    for copy in own:
        copy.start()

    def remote(src, dst, sems, i, y, x):
        return pltpu.make_async_remote_copy(
            src_ref=src,
            dst_ref=dst,
            send_sem=sems[0].at[i],
            recv_sem=sems[1].at[i],
            device_id={"py": y, "px": x},
            device_id_type=MESH,
        )

    row_copies = []
    for i, (a, b) in enumerate(zip(hbm[:8], bands)):
        sems = (send_row, recv_row)
        row_copies.append(remote(part(a, 0, 2), part(b, 2, 4), sems, 2 * i, up, px))
        row_copies.append(remote(part(a, rows - 2, rows), part(b, 4, 6), sems, 2 * i + 1, down, px))
    pl.semaphore_wait(barrier, len(near))
    for copy in row_copies:
        copy.start()

    def view(ref, *lead):
        return lambda r, c: ref[lead + (r, c)]

    def level_views(l, src):
        vel, th, vt, tt = src
        return (
            [view(vel, k, l) for k in range(3)]
            + [view(th, l)]
            + [view(vt, k, l) for k in range(3)]
            + [view(tt, l)]
        )

    def geo_views(src):
        cd, el, kite, cor = src
        return (
            [view(cd, k) for k in range(3)]
            + [view(el, k) for k in range(3)]
            + [view(kite, v, k) for v in range(2) for k in range(3)]
            + [view(cor, v) for v in range(2)]
        )

    def pack_cols(items, tile):
        for r in range(nr):
            rs = slice(r * SUB, (r + 1) * SUB)
            ra = la = jnp.zeros((SUB, LANE), F32)
            for s, f in items:
                m = jnp.where(lane < LANE // 2, f(rs, head), f(rs, tail))
                m = roll(m, s, 1)
                ra = jnp.where((lane == s) | (lane == s + 1), m, ra)
                la = jnp.where(lane == (s + LANE - 1) % LANE, m, la)
            cs = slice(tile * LANE, (tile + 1) * LANE)
            p_right[rs, cs] = ra
            p_left[rs, cs] = la

    for i in (4, 5, 6, 7):
        loads[i].wait()
    own_geo = geo_views(bufs[4:8])
    pack_cols([(2 * k, f) for k, f in enumerate(own_geo)], 1)
    for i in (0, 1, 2, 3):
        loads[i].wait()
    items = []
    for l in range(levels):
        items += [(l * GROUP + 2 * k, f) for k, f in enumerate(level_views(l, bufs[:4]))]
    pack_cols(items, 0)

    sems = (send_col, recv_col)
    col_copies = [
        remote(p_right, g_right.at[0:rows], sems, 0, py, left),
        remote(p_left, g_left.at[0:rows], sems, 1, py, right),
        remote(p_right.at[rows - 2 : rows], g_right.at[rows + 6 : rows + 8], sems, 2, down, left),
        remote(p_right.at[0:2], g_right.at[rows : rows + 2], sems, 3, up, left),
        remote(p_left.at[0:2], g_left.at[rows : rows + 2], sems, 4, up, right),
    ]
    for copy in col_copies:
        copy.start()
    loads[8].wait()

    def put_geo(dst, at, f, area=None):
        for k in range(3):
            dst[(k,) + at] = 0.25 * f[k] * f[3 + k]
            if area is not None:
                dst[(5 + k,) + at] = SLOPE / f[k]
        for v in range(2):
            dst[(3 + v,) + at] = f[12 + v] * (f[6 + 3 * v] + f[7 + 3 * v] + f[8 + 3 * v])
        if area is not None:
            dst[(8,) + at] = 1.0 / area

    for r in range(nr):
        for c in range(nc):
            put_geo(geo, span(r, c), [f(*span(r, c)) for f in own_geo], b_area[span(r, c)])

    def strip(fl, ft, l):
        m = jnp.where(lane < 5, fl, roll(ft, 9, 1))
        return roll(m, l * GROUP + 2, 1)

    def spread(x):
        for w in (GROUP, 2 * GROUP, 4 * GROUP):
            x = jnp.where(lane < w, x, roll(x, w, 1))
        return x

    def strip_levels(src, rs):
        out = []
        for k in range(8):
            acc = jnp.zeros((SUB, LANE), F32)
            for l in range(levels):
                f = level_views(l, src)[k]
                acc = jnp.where(group == l, strip(f(rs, head), f(rs, tail), l), acc)
            out.append(acc)
        return out

    for r in range(nr):
        rs = slice(r * SUB, (r + 1) * SUB)
        for k, x in enumerate(strip_levels(bufs[:4], rs)):
            slev[k, rs] = x
        for k, f in enumerate(own_geo):
            sgeo[k, rs] = strip(f(rs, head), f(rs, tail), 0)
        sgeo[14, rs] = spread(strip(b_area[rs, head], b_area[rs, tail], 0))

    def fields(grid, views):
        return [Field(grid, lambda r, c, f=f: f(*span(r, c))) for f in views]

    def run(grid, x, kites, dist, derived, swap=lambda i, f: f):
        f = fields(grid, derived)
        d = fields(grid, dist)
        cc, dd, outputs = chain(
            grid, x[0:3], x[3], x[4:7], x[7], d, f[0:3], fields(grid, kites), f[3:5], swap
        )
        return cc, dd, outputs(f[5:9])

    def block(l):
        grid = (nr, nc)
        cc, dd, outs = run(
            grid,
            fields(grid, level_views(l, bufs[:4])),
            own_geo[6:12],
            own_geo[0:3],
            [view(geo, k) for k in range(9)],
        )
        dst = [view_at(o_vert, 0, l), view_at(o_vert, 1, l), view_at(o_kin, l), view_at(o_cell, l)]
        dst += [view_at(o_edge, k, l) for k in range(3)]
        for c in range(nc):
            for i, f in enumerate((cc, dd)):
                saved[i, l, :, span(0, c)[1]] = jnp.where(
                    sub < 4, roll(f(nr - 1, c), 2, 0), roll(f(0, c), -2, 0)
                )
        for r in range(nr):
            for c in range(nc):
                for put, f in zip(dst, outs):
                    put(span(r, c), f(r, c))

    def view_at(ref, *lead):
        def put(at, x):
            ref[lead + at] = x

        return put

    def inner(i, carry):
        for u in range(PAIR):
            block(i * PAIR + u)
        return carry

    lax.fori_loop(0, levels // PAIR, inner, 0)

    for copy in own:
        copy.wait()
    for copy in row_copies + col_copies:
        copy.wait()

    band_geo = geo_views(bands[4:8])
    for c in range(nc):
        at = span(0, c)
        put_geo(kgeo, at, [f(*at) for f in band_geo], bands[8][at])

    merge = (sub == 0) | (sub == SUB - 1)
    for l in range(levels):
        grid = (1, nc)

        def swap(i, f, l=l):
            return Field(
                grid, lambda r, c: jnp.where(merge, saved[i, l, :, span(0, c)[1]], f(r, c))
            )

        outs = run(
            grid,
            fields(grid, level_views(l, bands[:4])),
            band_geo[6:12],
            band_geo[0:3],
            [view(kgeo, k) for k in range(9)],
            swap,
        )[2]
        dst = [(o_vert, (0, l)), (o_vert, (1, l)), (o_kin, (l,)), (o_cell, (l,))]
        dst += [(o_edge, (k, l)) for k in range(3)]
        both = ((rows - 1, 1, 1), (0, 6, 1))
        which = [
            ((rows - 1, 1, 1),),
            ((0, 6, 1),),
            both,
            both,
            ((rows - 2, 0, 2), (0, 6, 1)),
            both,
            ((rows - 1, 1, 1), (0, 6, 2)),
        ]
        for c in range(nc):
            cs = span(0, c)[1]
            for (ref, lead), f, ranges in zip(dst, outs, which):
                x = f(0, c)
                for to, src, n in ranges:
                    ref[lead + (slice(to, to + n), cs)] = x[src : src + n]

    def turn(x):
        return jnp.where(sub < 4, roll(x, -2, 0), roll(x, 2, 0))

    low = slice(0, SUB)
    edge_rows = slice(rows, rows + SUB)
    for k, x in enumerate(strip_levels(bands[:4], low)):
        slev[k, edge_rows] = turn(x)
    for k, f in enumerate(band_geo):
        sgeo[k, edge_rows] = turn(strip(f(low, head), f(low, tail), 0))

    def insert(x, k, rs, cs):
        rt = roll(g_right[rs, cs], 11 - 2 * k, 1)
        lt = roll(g_left[rs, cs], 2 - 2 * k, 1)
        return jnp.where((pos == 11) | (pos == 12), rt, jnp.where(pos == 1, lt, x))

    for r in range(nr + 1):
        rs = slice(r * SUB, (r + 1) * SUB)
        raw = [
            spread(insert(sgeo[k, rs], k, rs, slice(LANE, 2 * LANE))) for k in range(14)
        ]
        for k in list(range(3)) + list(range(6, 12)):
            sgeo[k, rs] = raw[k]
        ws = [0.25 * raw[k] * raw[3 + k] for k in range(3)]
        ts = [raw[12 + v] * (raw[6 + 3 * v] + raw[7 + 3 * v] + raw[8 + 3 * v]) for v in range(2)]
        for k, x in zip((3, 4, 5, 12, 13), ws + ts):
            sgeo[k, rs] = x

    grid = (nr + 1, 1)
    one = lambda r: slice(r * SUB, (r + 1) * SUB)
    sfield = lambda k: Field(grid, lambda r, c: sgeo[k, one(r)])
    x = [
        Field(grid, lambda r, c, k=k: insert(slev[k, one(r)], k, one(r), slice(0, LANE)))
        for k in range(8)
    ]
    outputs = chain(
        grid, x[0:3], x[3], x[4:7], x[7],
        [sfield(k) for k in range(3)],
        [sfield(k) for k in (3, 4, 5)],
        [sfield(k) for k in range(6, 12)],
        [sfield(k) for k in (12, 13)],
    )[2]
    scale = [Field(grid, lambda r, c, k=k: SLOPE / sgeo[k, one(r)]) for k in range(3)]
    scale.append(Field(grid, lambda r, c: 1.0 / sgeo[14, one(r)]))
    outs = outputs(scale)
    refs_of = [(o_vert, (0,)), (o_vert, (1,)), (o_kin, ()), (o_cell, ())]
    refs_of += [(o_edge, (k,)) for k in range(3)]
    first, ends = lane == 0, lane >= LANE - 2
    end = lane == LANE - 1
    masks = [(None, end), (None, end), (first, None), (first, end), (first, ends), (first, ends), (first, ends)]
    for r in range(nr):
        for (ref, lead), f, (mf, me) in zip(refs_of, outs, masks):
            y = f(r, 0)
            y = jnp.where(pos == 2, y, roll(y, -9, 1))
            for l in range(levels):
                z = roll(y, -(l * GROUP + 2), 1)
                if mf is not None:
                    pltpu.store(ref.at[lead + (l, one(r), head)], z, mask=mf)
                if me is not None:
                    pltpu.store(ref.at[lead + (l, one(r), tail)], z, mask=me)


def drain_kernel(*refs):
    src, dst, sem = refs[:4], refs[4:8], refs[8]
    copies = [pltpu.make_async_copy(a, b, sem.at[i]) for i, (a, b) in enumerate(zip(src, dst))]
    for copy in copies:
        copy.start()
    for copy in copies:
        copy.wait()


def local(counts, vel, th, vt, tt, cd, el, area, kite, cor):
    args = (vel, th, vt, tt, cd, el, kite, cor, area)
    levels, rows, cols = th.shape
    outs = [(2, levels, rows, cols), (levels, rows, cols), (levels, rows, cols), (3, levels, rows, cols)]
    band = lambda a: a.shape[:-2] + (SUB, cols)
    hbm, vmem = pl.BlockSpec(memory_space=pl.ANY), pl.BlockSpec(memory_space=pltpu.VMEM)
    side = (rows + SUB, 2 * LANE)
    kept = pl.pallas_call(
        lambda *refs: main_kernel(counts, *refs),
        out_shape=[pltpu.VMEM(s, F32) for s in outs],
        in_specs=[hbm] * len(args),
        out_specs=[vmem] * len(outs),
        scratch_shapes=[pltpu.VMEM(a.shape, F32) for a in args]
        + [pltpu.VMEM(band(a), F32) for a in args]
        + [pltpu.VMEM(s, F32) for s in ((rows, 2 * LANE), (rows, 2 * LANE), side, side)]
        + [
            pltpu.VMEM((9, rows, cols), F32),
            pltpu.VMEM((9, SUB, cols), F32),
            pltpu.VMEM((15, rows + SUB, LANE), F32),
            pltpu.VMEM((8, rows + SUB, LANE), F32),
            pltpu.VMEM((2, levels, SUB, cols), F32),
            pltpu.SemaphoreType.DMA((9,)),
            pltpu.SemaphoreType.DMA((18,)),
            pltpu.SemaphoreType.DMA((16,)),
            pltpu.SemaphoreType.DMA((16,)),
            pltpu.SemaphoreType.DMA((5,)),
            pltpu.SemaphoreType.DMA((5,)),
        ],
        compiler_params=pltpu.CompilerParams(collective_id=0, has_side_effects=True),
        name="main",
    )(*args)
    return pl.pallas_call(
        drain_kernel,
        out_shape=[jax.ShapeDtypeStruct(s, F32) for s in outs],
        in_specs=[vmem] * len(outs),
        out_specs=[hbm] * len(outs),
        scratch_shapes=[pltpu.SemaphoreType.DMA((len(outs),))],
        name="drain",
    )(*kept)


def solution(mesh):
    counts = (mesh.shape["py"], mesh.shape["px"])
    p4, p3 = P(None, None, "py", "px"), P(None, "py", "px")
    return jax.shard_map(
        lambda *args: local(counts, *args),
        mesh=mesh,
        in_specs=(p4, p3, p4, p3, p3, p3, P("py", "px"), p4, p3),
        out_specs=(p4, p3, p3, p4),
        check_vma=False,
    )
```

```python
import jax
import jax.numpy as jnp
from jax import lax
from jax.experimental import pallas as pl
from jax.experimental.pallas import tpu as pltpu
from jax.sharding import PartitionSpec as P

SUB = 8
LANE = 128
GROUP = 16
PAIR = 2
MESH = pl.DeviceIdType.MESH
F32 = jnp.float32
SLOPE = -0.5 / 36.0


def iotas():
    sub = lax.broadcasted_iota(jnp.int32, (SUB, LANE), 0)
    lane = lax.broadcasted_iota(jnp.int32, (SUB, LANE), 1)
    return sub, lane


def roll(x, shift, axis):
    n = (SUB, LANE)[axis]
    return pltpu.roll(x, shift % n, axis) if shift % n else x


def pick(x, index):
    return jnp.take_along_axis(x, index, axis=1)


def span(r, c):
    return (slice(r * SUB, (r + 1) * SUB), slice(c * LANE, (c + 1) * LANE))


class Field:
    def __init__(self, grid, make):
        self.grid, self.make, self.memo = grid, make, {}

    def __call__(self, r, c):
        key = (r % self.grid[0], c % self.grid[1])
        if key not in self.memo:
            self.memo[key] = self.make(*key)
        return self.memo[key]


def chain(grid, v, h, t, g, dist, ew, kt, ct, swap=lambda i, f: f, staged=False):
    sub, lane = iotas()

    def lift(fn, *fields):
        return Field(grid, lambda r, c: fn(*[f(r, c) for f in fields]))

    def row_shift(f, a):
        rolled = Field(grid, lambda r, c: roll(f(r, c), -a, 0))
        if grid[0] == 1:
            return rolled
        keep = sub < SUB - 1 if a == 1 else sub > 0
        return Field(grid, lambda r, c: jnp.where(keep, rolled(r, c), rolled(r + a, c)))

    def col_shift(f, b):
        rolled = Field(grid, lambda r, c: roll(f(r, c), -b, 1))
        if grid[1] == 1:
            return rolled
        keep = lane < LANE - 1 if b == 1 else lane > 0
        return Field(grid, lambda r, c: jnp.where(keep, rolled(r, c), rolled(r, c + b)))

    def parts(vv, hh):
        flux = [lift(lambda a, b: a * b, vv[k], dist[k]) for k in range(3)]
        c0 = lift(lambda a, b, c: a + b - c, flux[0], row_shift(flux[2], 1), flux[1])
        c1 = lift(lambda a, b, c: a - b - c, flux[1], flux[2], col_shift(row_shift(flux[0], -1), 1))
        hc = col_shift(hh, 1)
        hr = row_shift(hh, 1)
        hd = row_shift(hc, -1)
        mix = lambda a, b, c, p, q, s: a * p + b * q + c * s
        h0 = lift(mix, kt[0], kt[1], kt[2], hh, hr, hc)
        h1 = lift(mix, kt[3], kt[4], kt[5], hh, hc, hd)
        return (c0, c1), (h0, h1)

    def now(*fs):
        if staged:
            for f in fs:
                for r in range(grid[0]):
                    for c in range(grid[1]):
                        f(r, c)

    now(*v, h, *t, g)
    cv, hv = parts(v, h)
    cw, hw = parts(t, g)
    now(*cv, *hv, *cw, *hw)

    def potential(k):
        def make(r, c):
            a0 = ct[k](r, c) + cv[k](r, c)
            a1 = cw[k](r, c)
            b0 = hv[k](r, c)
            b1 = hw[k](r, c)
            bm, be = b0 + 0.5 * b1, b0 + b1
            m = bm * be
            scale_all = 1.0 / (b0 * m)
            mid = (a0 + a0 + a1) * (b0 * be)
            late = mid + (a0 + a1) * (b0 * bm)
            return (a0 * m + mid + late) * scale_all, late * scale_all

        both = Field(grid, make)
        return Field(grid, lambda r, c: both(r, c)[0]), Field(grid, lambda r, c: both(r, c)[1])

    p0, q0 = potential(0)
    p1, q1 = potential(1)
    now(p0, q0, p1, q1)
    add = lambda a, b: a + b
    add3 = lambda a, b, c: a + b + c

    def cell(f0, f1):
        f0_up = row_shift(f0, -1)
        f1_down = row_shift(f1, 1)
        pair = lift(add, f0, f1)
        return lift(add3, pair, f0_up, col_shift(lift(add, pair, f1_down), -1)), f0_up, f1_down, pair

    cc, p0_up, p1_down, pair = cell(p0, p1)
    dd = cell(q0, q1)[0]
    cc, dd = swap(0, cc), swap(1, dd)
    p1_low = col_shift(p1_down, -1)
    now(cc, dd, p1_low)

    def neighbours(f):
        fc = col_shift(f, 1)
        return row_shift(f, 1), fc, row_shift(fc, -1)

    cn, dn = neighbours(cc), neighbours(dd)
    now(*cn, *dn)
    ends = [lift(add, p0, p1_low), pair, lift(add, p1, p0_up)]
    en = [
        lift(lambda w, a, b: w * (a * (a + b) + (1.0 / 3.0) * (b * b)), ew[k], v[k], t[k])
        for k in range(3)
    ]
    e_up = row_shift(en[0], -1)
    e_low = col_shift(lift(add, en[1], row_shift(en[2], 1)), -1)
    now(e_low)

    def outputs(scale):
        def edge(k):
            def make(r, c):
                slope = v[k](r, c) * (cn[k](r, c) - cc(r, c)) + t[k](r, c) * (dn[k](r, c) - dd(r, c))
                return ends[k](r, c) * (1.0 / 12.0) + scale[k](r, c) * slope

            return Field(grid, make)

        kin = Field(
            grid,
            lambda r, c: (en[0](r, c) + en[1](r, c) + en[2](r, c) + e_up(r, c) + e_low(r, c)) * scale[3](r, c),
        )
        return [
            lift(lambda a: a * (1.0 / 6.0), p0),
            lift(lambda a: a * (1.0 / 6.0), p1),
            kin,
            lift(lambda a: a * (1.0 / 36.0), cc),
        ] + [edge(k) for k in range(3)]

    return cc, dd, outputs


def main_kernel(counts, *refs):
    hbm = refs[:9]
    o_vert, o_kin, o_cell, o_edge = refs[9:13]
    bufs = refs[13:22]
    bands = refs[22:31]
    p_right, p_left, g_right, g_left = refs[31:35]
    geo, kgeo, sgeo, slev, saved = refs[35:40]
    in_sem, own_sem, send_row, recv_row, send_col, recv_col = refs[40:46]
    ny, nx = counts
    py, px = lax.axis_index("py"), lax.axis_index("px")
    down, up = lax.rem(py + 1, ny), lax.rem(py + ny - 1, ny)
    right, left = lax.rem(px + 1, nx), lax.rem(px + nx - 1, nx)

    barrier = pltpu.get_barrier_semaphore()
    near = [
        (up, px), (down, px), (py, left), (py, right),
        (up, left), (up, right), (down, left), (down, right),
    ]
    for y, x in near:
        pl.semaphore_signal(barrier, inc=1, device_id={"py": y, "px": x}, device_id_type=MESH)

    b_vel, b_th, b_vt, b_tt, b_cd, b_el, b_kite, b_cor, b_area = bufs
    levels, rows, cols = b_th.shape
    nr, nc = rows // SUB, cols // LANE
    sub, lane = iotas()
    pos, group = lane & (GROUP - 1), lane >> 4
    head, tail = slice(0, LANE), slice(cols - LANE, cols)

    loads = [pltpu.make_async_copy(a, b, in_sem.at[i]) for i, (a, b) in enumerate(zip(hbm, bufs))]
    for i in (4, 5, 6, 7, 0, 1, 2, 3, 8):
        loads[i].start()

    def part(ref, a, b):
        return ref.at[(slice(None),) * (len(ref.shape) - 2) + (slice(a, b), slice(None))]

    own = []
    for i, (a, b) in enumerate(zip(hbm, bands)):
        own.append(pltpu.make_async_copy(part(a, rows - 2, rows), part(b, 0, 2), own_sem.at[2 * i]))
        own.append(pltpu.make_async_copy(part(a, 0, 2), part(b, 6, 8), own_sem.at[2 * i + 1]))
    for copy in own:
        copy.start()

    def remote(src, dst, sems, i, y, x):
        return pltpu.make_async_remote_copy(
            src_ref=src,
            dst_ref=dst,
            send_sem=sems[0].at[i],
            recv_sem=sems[1].at[i],
            device_id={"py": y, "px": x},
            device_id_type=MESH,
        )

    row_copies = []
    for i, (a, b) in enumerate(zip(hbm[:8], bands)):
        sems = (send_row, recv_row)
        row_copies.append(remote(part(a, 0, 2), part(b, 2, 4), sems, 2 * i, up, px))
        row_copies.append(remote(part(a, rows - 2, rows), part(b, 4, 6), sems, 2 * i + 1, down, px))
    pl.semaphore_wait(barrier, len(near))
    for copy in row_copies:
        copy.start()

    def view(ref, *lead):
        return lambda r, c: ref[lead + (r, c)]

    def level_views(l, src):
        vel, th, vt, tt = src
        return (
            [view(vel, k, l) for k in range(3)]
            + [view(th, l)]
            + [view(vt, k, l) for k in range(3)]
            + [view(tt, l)]
        )

    def geo_views(src):
        cd, el, kite, cor = src
        return (
            [view(cd, k) for k in range(3)]
            + [view(el, k) for k in range(3)]
            + [view(kite, v, k) for v in range(2) for k in range(3)]
            + [view(cor, v) for v in range(2)]
        )

    def pack_cols(items, tile):
        for r in range(nr):
            rs = slice(r * SUB, (r + 1) * SUB)
            ra = la = jnp.zeros((SUB, LANE), F32)
            for s, f in items:
                m = jnp.where(lane < LANE // 2, f(rs, head), f(rs, tail))
                m = roll(m, s, 1)
                ra = jnp.where((lane == s) | (lane == s + 1), m, ra)
                la = jnp.where(lane == (s + LANE - 1) % LANE, m, la)
            cs = slice(tile * LANE, (tile + 1) * LANE)
            p_right[rs, cs] = ra
            p_left[rs, cs] = la

    for i in (4, 5, 6, 7):
        loads[i].wait()
    own_geo = geo_views(bufs[4:8])
    pack_cols([(2 * k, f) for k, f in enumerate(own_geo)], 1)
    for i in (0, 1, 2, 3):
        loads[i].wait()
    items = []
    for l in range(levels):
        items += [(l * GROUP + 2 * k, f) for k, f in enumerate(level_views(l, bufs[:4]))]
    pack_cols(items, 0)

    sems = (send_col, recv_col)
    col_copies = [
        remote(p_right, g_right.at[0:rows], sems, 0, py, left),
        remote(p_left, g_left.at[0:rows], sems, 1, py, right),
        remote(p_right.at[rows - 2 : rows], g_right.at[rows + 6 : rows + 8], sems, 2, down, left),
        remote(p_right.at[0:2], g_right.at[rows : rows + 2], sems, 3, up, left),
        remote(p_left.at[0:2], g_left.at[rows : rows + 2], sems, 4, up, right),
    ]
    for copy in col_copies:
        copy.start()
    loads[8].wait()

    def put_geo(dst, at, f, area=None):
        for k in range(3):
            dst[(k,) + at] = 0.25 * f[k] * f[3 + k]
            if area is not None:
                dst[(5 + k,) + at] = SLOPE / f[k]
        for v in range(2):
            dst[(3 + v,) + at] = f[12 + v] * (f[6 + 3 * v] + f[7 + 3 * v] + f[8 + 3 * v])
        if area is not None:
            dst[(8,) + at] = 1.0 / area

    for r in range(nr):
        for c in range(nc):
            put_geo(geo, span(r, c), [f(*span(r, c)) for f in own_geo], b_area[span(r, c)])

    near_index = jnp.where(pos < 5, jnp.maximum(pos - 2, 0), jnp.minimum(pos + LANE - 11, LANE - 1))

    def strip(f, rs):
        return pick(jnp.where(lane < LANE // 2, f(rs, head), f(rs, tail)), near_index)

    def strip_levels(src, rs):
        got = [[strip(f, rs) for f in level_views(l, src)] for l in range(levels)]
        out = got[0]
        for l in range(1, levels):
            out = [jnp.where(group == l, x, y) for x, y in zip(got[l], out)]
        return out

    for r in range(nr):
        rs = slice(r * SUB, (r + 1) * SUB)
        for k, x in enumerate(strip_levels(bufs[:4], rs)):
            slev[k, rs] = x
        for k, f in enumerate(own_geo):
            sgeo[k, rs] = strip(f, rs)
        sgeo[14, rs] = strip(view(b_area), rs)

    def fields(grid, views):
        return [Field(grid, lambda r, c, f=f: f(*span(r, c))) for f in views]

    def run(grid, x, kites, dist, derived, swap=lambda i, f: f):
        f = fields(grid, derived)
        d = fields(grid, dist)
        cc, dd, outputs = chain(
            grid, x[0:3], x[3], x[4:7], x[7], d, f[0:3], fields(grid, kites), f[3:5], swap
        )
        return cc, dd, outputs(f[5:9])

    def block(l):
        grid = (nr, nc)
        cc, dd, outs = run(
            grid,
            fields(grid, level_views(l, bufs[:4])),
            own_geo[6:12],
            own_geo[0:3],
            [view(geo, k) for k in range(9)],
        )
        dst = [view_at(o_vert, 0, l), view_at(o_vert, 1, l), view_at(o_kin, l), view_at(o_cell, l)]
        dst += [view_at(o_edge, k, l) for k in range(3)]
        for c in range(nc):
            for i, f in enumerate((cc, dd)):
                saved[i, l, :, span(0, c)[1]] = jnp.where(
                    sub < 4, roll(f(nr - 1, c), 2, 0), roll(f(0, c), -2, 0)
                )
        for r in range(nr):
            for c in range(nc):
                for put, f in zip(dst, outs):
                    put(span(r, c), f(r, c))

    def view_at(ref, *lead):
        def put(at, x):
            ref[lead + at] = x

        return put

    def inner(i, carry):
        for u in range(PAIR):
            block(i * PAIR + u)
        return carry

    lax.fori_loop(0, levels // PAIR, inner, 0)

    for copy in own:
        copy.wait()
    for copy in row_copies + col_copies:
        copy.wait()

    band_geo = geo_views(bands[4:8])
    for c in range(nc):
        at = span(0, c)
        put_geo(kgeo, at, [f(*at) for f in band_geo], bands[8][at])

    merge = (sub == 0) | (sub == SUB - 1)
    for l in range(levels):
        grid = (1, nc)

        def swap(i, f, l=l):
            return Field(
                grid, lambda r, c: jnp.where(merge, saved[i, l, :, span(0, c)[1]], f(r, c))
            )

        outs = run(
            grid,
            fields(grid, level_views(l, bands[:4])),
            band_geo[6:12],
            band_geo[0:3],
            [view(kgeo, k) for k in range(9)],
            swap,
        )[2]
        dst = [(o_vert, (0, l)), (o_vert, (1, l)), (o_kin, (l,)), (o_cell, (l,))]
        dst += [(o_edge, (k, l)) for k in range(3)]
        both = ((rows - 1, 1, 1), (0, 6, 1))
        which = [
            ((rows - 1, 1, 1),),
            ((0, 6, 1),),
            both,
            both,
            ((rows - 2, 0, 2), (0, 6, 1)),
            both,
            ((rows - 1, 1, 1), (0, 6, 2)),
        ]
        for c in range(nc):
            cs = span(0, c)[1]
            for (ref, lead), f, ranges in zip(dst, outs, which):
                x = f(0, c)
                for to, src, n in ranges:
                    ref[lead + (slice(to, to + n), cs)] = x[src : src + n]

    def turn(x):
        return jnp.where(sub < 4, roll(x, -2, 0), roll(x, 2, 0))

    low = slice(0, SUB)
    edge_rows = slice(rows, rows + SUB)
    right_pos, left_pos = (pos == 11) | (pos == 12), pos == 1
    tiles = [slice(r * SUB, (r + 1) * SUB) for r in range(nr + 1)]
    band_levels = [turn(x) for x in strip_levels(bands[:4], low)]
    band_near = [turn(strip(f, low)) for f in band_geo]
    last = slice(LANE, 2 * LANE)

    def insert_geo(k, r):
        rt = pick(g_right[tiles[r], last], jnp.where(pos == 12, 2 * k + 1, 2 * k))
        lt = pick(g_left[tiles[r], last], jnp.full((SUB, LANE), (2 * k - 1) % LANE, jnp.int32))
        own_part = band_near[k] if r == nr else sgeo[k, tiles[r]]
        return jnp.where(right_pos, rt, jnp.where(left_pos, lt, own_part))

    def insert(k, r):
        rt = roll(g_right[tiles[r], head], 11 - 2 * k, 1)
        lt = roll(g_left[tiles[r], head], 2 - 2 * k, 1)
        own_part = band_levels[k] if r == nr else slev[k, tiles[r]]
        return jnp.where(right_pos, rt, jnp.where(left_pos, lt, own_part))

    grid = (nr + 1, 1)
    x = [Field(grid, lambda r, c, k=k: insert(k, r)) for k in range(8)]
    raw = [Field(grid, lambda r, c, k=k: insert_geo(k, r)) for k in range(14)]
    for f in x + raw:
        for r in range(nr + 1):
            f(r, 0)
    ws = [Field(grid, lambda r, c, k=k: 0.25 * raw[k](r, c) * raw[3 + k](r, c)) for k in range(3)]

    def weighed(v):
        a = [raw[6 + 3 * v + k] for k in range(3)]
        return Field(grid, lambda r, c: raw[12 + v](r, c) * (a[0](r, c) + a[1](r, c) + a[2](r, c)))

    outputs = chain(
        grid, x[0:3], x[3], x[4:7], x[7], raw[0:3], ws, raw[6:12], [weighed(v) for v in range(2)],
        staged=True,
    )[2]
    scale = [Field(grid, lambda r, c, k=k: SLOPE / raw[k](r, c)) for k in range(3)]
    scale.append(Field(grid, lambda r, c: 1.0 / sgeo[14, tiles[r]]))
    outs = outputs(scale)
    refs_of = [(o_vert, (0,)), (o_vert, (1,)), (o_kin, ()), (o_cell, ())]
    refs_of += [(o_edge, (k,)) for k in range(3)]
    first, ends = lane == 0, lane >= LANE - 2
    end = lane == LANE - 1
    masks = [(None, end), (None, end), (first, None), (first, end), (first, ends), (first, ends), (first, ends)]
    back = [
        jnp.where(lane < LANE // 2, l * GROUP + 2, l * GROUP + 11 - LANE + lane) & (LANE - 1)
        for l in range(levels)
    ]
    done = [[f(r, 0) for f in outs] for r in range(nr)]
    for r in range(nr):
        moved = [[pick(y, back[l]) for l in range(levels)] for y in done[r]]
        for (ref, lead), zs, (mf, me) in zip(refs_of, moved, masks):
            for l, z in enumerate(zs):
                if mf is not None:
                    pltpu.store(ref.at[lead + (l, tiles[r], head)], z, mask=mf)
                if me is not None:
                    pltpu.store(ref.at[lead + (l, tiles[r], tail)], z, mask=me)


def drain_kernel(*refs):
    src, dst, sem = refs[:4], refs[4:8], refs[8]
    copies = [pltpu.make_async_copy(a, b, sem.at[i]) for i, (a, b) in enumerate(zip(src, dst))]
    for copy in copies:
        copy.start()
    for copy in copies:
        copy.wait()


def local(counts, vel, th, vt, tt, cd, el, area, kite, cor):
    args = (vel, th, vt, tt, cd, el, kite, cor, area)
    levels, rows, cols = th.shape
    outs = [(2, levels, rows, cols), (levels, rows, cols), (levels, rows, cols), (3, levels, rows, cols)]
    band = lambda a: a.shape[:-2] + (SUB, cols)
    hbm, vmem = pl.BlockSpec(memory_space=pl.ANY), pl.BlockSpec(memory_space=pltpu.VMEM)
    side = (rows + SUB, 2 * LANE)
    kept = pl.pallas_call(
        lambda *refs: main_kernel(counts, *refs),
        out_shape=[pltpu.VMEM(s, F32) for s in outs],
        in_specs=[hbm] * len(args),
        out_specs=[vmem] * len(outs),
        scratch_shapes=[pltpu.VMEM(a.shape, F32) for a in args]
        + [pltpu.VMEM(band(a), F32) for a in args]
        + [pltpu.VMEM(s, F32) for s in ((rows, 2 * LANE), (rows, 2 * LANE), side, side)]
        + [
            pltpu.VMEM((9, rows, cols), F32),
            pltpu.VMEM((9, SUB, cols), F32),
            pltpu.VMEM((15, rows + SUB, LANE), F32),
            pltpu.VMEM((8, rows + SUB, LANE), F32),
            pltpu.VMEM((2, levels, SUB, cols), F32),
            pltpu.SemaphoreType.DMA((9,)),
            pltpu.SemaphoreType.DMA((18,)),
            pltpu.SemaphoreType.DMA((16,)),
            pltpu.SemaphoreType.DMA((16,)),
            pltpu.SemaphoreType.DMA((5,)),
            pltpu.SemaphoreType.DMA((5,)),
        ],
        compiler_params=pltpu.CompilerParams(collective_id=0, has_side_effects=True),
        name="main",
    )(*args)
    return pl.pallas_call(
        drain_kernel,
        out_shape=[jax.ShapeDtypeStruct(s, F32) for s in outs],
        in_specs=[vmem] * len(outs),
        out_specs=[pl.BlockSpec(memory_space=pltpu.HBM)] * len(outs),
        scratch_shapes=[pltpu.SemaphoreType.DMA((len(outs),))],
        name="drain",
    )(*kept)


def solution(mesh):
    counts = (mesh.shape["py"], mesh.shape["px"])
    p4, p3 = P(None, None, "py", "px"), P(None, "py", "px")
    return jax.shard_map(
        lambda *args: local(counts, *args),
        mesh=mesh,
        in_specs=(p4, p3, p4, p3, p3, p3, P("py", "px"), p4, p3),
        out_specs=(p4, p3, p3, p4),
        check_vma=False,
    )
```

```python
import jax
import jax.numpy as jnp
from jax import lax
from jax.experimental import pallas as pl
from jax.experimental.pallas import tpu as pltpu
from jax.sharding import PartitionSpec as P

SUB = 8
LANE = 128
GROUP = 16
PAIR = 2
BATCH = 8
MESH = pl.DeviceIdType.MESH
F32 = jnp.float32
SLOPE = -0.5 / 36.0


def iotas():
    sub = lax.broadcasted_iota(jnp.int32, (SUB, LANE), 0)
    lane = lax.broadcasted_iota(jnp.int32, (SUB, LANE), 1)
    return sub, lane


def roll(x, shift, axis):
    n = (SUB, LANE)[axis]
    return pltpu.roll(x, shift % n, axis) if shift % n else x


def pick(x, index):
    return jnp.take_along_axis(x, index, axis=1)


def span(r, c):
    return (slice(r * SUB, (r + 1) * SUB), slice(c * LANE, (c + 1) * LANE))


class Field:
    def __init__(self, grid, make):
        self.grid, self.make, self.memo = grid, make, {}

    def __call__(self, r, c):
        key = (r % self.grid[0], c % self.grid[1])
        if key not in self.memo:
            self.memo[key] = self.make(*key)
        return self.memo[key]


def chain(grid, v, h, t, g, dist, ew, kt, ct, swap=lambda i, f: f):
    sub, lane = iotas()

    def lift(fn, *fields):
        return Field(grid, lambda r, c: fn(*[f(r, c) for f in fields]))

    def row_shift(f, a):
        rolled = Field(grid, lambda r, c: roll(f(r, c), -a, 0))
        if grid[0] == 1:
            return rolled
        keep = sub < SUB - 1 if a == 1 else sub > 0
        return Field(grid, lambda r, c: jnp.where(keep, rolled(r, c), rolled(r + a, c)))

    def col_shift(f, b):
        rolled = Field(grid, lambda r, c: roll(f(r, c), -b, 1))
        if grid[1] == 1:
            return rolled
        keep = lane < LANE - 1 if b == 1 else lane > 0
        return Field(grid, lambda r, c: jnp.where(keep, rolled(r, c), rolled(r, c + b)))

    def parts(vv, hh):
        flux = [lift(lambda a, b: a * b, vv[k], dist[k]) for k in range(3)]
        c0 = lift(lambda a, b, c: a + b - c, flux[0], row_shift(flux[2], 1), flux[1])
        c1 = lift(lambda a, b, c: a - b - c, flux[1], flux[2], col_shift(row_shift(flux[0], -1), 1))
        hc = col_shift(hh, 1)
        hr = row_shift(hh, 1)
        hd = row_shift(hc, -1)
        mix = lambda a, b, c, p, q, s: a * p + b * q + c * s
        h0 = lift(mix, kt[0], kt[1], kt[2], hh, hr, hc)
        h1 = lift(mix, kt[3], kt[4], kt[5], hh, hc, hd)
        return (c0, c1), (h0, h1)

    cv, hv = parts(v, h)
    cw, hw = parts(t, g)

    def potential(k):
        def make(r, c):
            a0 = ct[k](r, c) + cv[k](r, c)
            a1 = cw[k](r, c)
            b0 = hv[k](r, c)
            b1 = hw[k](r, c)
            bm, be = b0 + 0.5 * b1, b0 + b1
            m = bm * be
            scale_all = 1.0 / (b0 * m)
            mid = (a0 + a0 + a1) * (b0 * be)
            late = mid + (a0 + a1) * (b0 * bm)
            return (a0 * m + mid + late) * scale_all, late * scale_all

        both = Field(grid, make)
        return Field(grid, lambda r, c: both(r, c)[0]), Field(grid, lambda r, c: both(r, c)[1])

    p0, q0 = potential(0)
    p1, q1 = potential(1)
    add = lambda a, b: a + b
    add3 = lambda a, b, c: a + b + c

    def cell(f0, f1):
        f0_up = row_shift(f0, -1)
        f1_down = row_shift(f1, 1)
        pair = lift(add, f0, f1)
        return lift(add3, pair, f0_up, col_shift(lift(add, pair, f1_down), -1)), f0_up, f1_down, pair

    cc, p0_up, p1_down, pair = cell(p0, p1)
    dd = cell(q0, q1)[0]
    cc, dd = swap(0, cc), swap(1, dd)
    p1_low = col_shift(p1_down, -1)

    def neighbours(f):
        fc = col_shift(f, 1)
        return row_shift(f, 1), fc, row_shift(fc, -1)

    cn, dn = neighbours(cc), neighbours(dd)
    ends = [lift(add, p0, p1_low), pair, lift(add, p1, p0_up)]
    en = [
        lift(lambda w, a, b: w * (a * (a + b) + (1.0 / 3.0) * (b * b)), ew[k], v[k], t[k])
        for k in range(3)
    ]
    e_up = row_shift(en[0], -1)
    e_low = col_shift(lift(add, en[1], row_shift(en[2], 1)), -1)

    def outputs(scale):
        def edge(k):
            def make(r, c):
                slope = v[k](r, c) * (cn[k](r, c) - cc(r, c)) + t[k](r, c) * (dn[k](r, c) - dd(r, c))
                return ends[k](r, c) * (1.0 / 12.0) + scale[k](r, c) * slope

            return Field(grid, make)

        kin = Field(
            grid,
            lambda r, c: (en[0](r, c) + en[1](r, c) + en[2](r, c) + e_up(r, c) + e_low(r, c)) * scale[3](r, c),
        )
        return [
            lift(lambda a: a * (1.0 / 6.0), p0),
            lift(lambda a: a * (1.0 / 6.0), p1),
            kin,
            lift(lambda a: a * (1.0 / 36.0), cc),
        ] + [edge(k) for k in range(3)]

    stages = [[*cv, *hv, *cw, *hw, e_low], [p0, q0, p1, q1], [cc, dd, p1_low], [*cn, *dn]]
    return cc, dd, outputs, stages


def main_kernel(counts, *refs):
    hbm = refs[:9]
    o_vert, o_kin, o_cell, o_edge = refs[9:13]
    bufs = refs[13:22]
    bands = refs[22:31]
    p_right, p_left, g_right, g_left = refs[31:35]
    geo, kgeo, sgeo, slev, saved = refs[35:40]
    in_sem, own_sem, send_row, recv_row, send_col, recv_col = refs[40:46]
    ny, nx = counts
    py, px = lax.axis_index("py"), lax.axis_index("px")
    down, up = lax.rem(py + 1, ny), lax.rem(py + ny - 1, ny)
    right, left = lax.rem(px + 1, nx), lax.rem(px + nx - 1, nx)

    barrier = pltpu.get_barrier_semaphore()
    near = [
        (up, px), (down, px), (py, left), (py, right),
        (up, left), (up, right), (down, left), (down, right),
    ]
    for y, x in near:
        pl.semaphore_signal(barrier, inc=1, device_id={"py": y, "px": x}, device_id_type=MESH)

    b_vel, b_th, b_vt, b_tt, b_cd, b_el, b_kite, b_cor, b_area = bufs
    levels, rows, cols = b_th.shape
    nr, nc = rows // SUB, cols // LANE
    sub, lane = iotas()
    pos, group = lane & (GROUP - 1), lane >> 4
    head, tail = slice(0, LANE), slice(cols - LANE, cols)

    def part(ref, a, b, *lead):
        rest = (slice(None),) * (len(ref.shape) - 2 - len(lead))
        return ref.at[lead + rest + (slice(a, b), slice(None))]

    own = []
    for i, (a, b) in enumerate(zip(hbm, bands)):
        own.append(pltpu.make_async_copy(part(a, rows - 2, rows), part(b, 0, 2), own_sem.at[2 * i]))
        own.append(pltpu.make_async_copy(part(a, 0, 2), part(b, 6, 8), own_sem.at[2 * i + 1]))
    for copy in own:
        copy.start()
    loads = [pltpu.make_async_copy(a, b, in_sem.at[i]) for i, (a, b) in enumerate(zip(hbm, bufs))]
    for i in (4, 5, 6, 7, 0, 1, 2, 3, 8):
        loads[i].start()

    def remote(src, dst, sems, i, y, x):
        return pltpu.make_async_remote_copy(
            src_ref=src,
            dst_ref=dst,
            send_sem=sems[0].at[i],
            recv_sem=sems[1].at[i],
            device_id={"py": y, "px": x},
            device_id_type=MESH,
        )

    vel, th, vt, tt, cd, el, kite, cor = bands[:8]
    to_up = [
        (2, vel, slice(1, 3)), (1, vel, 0), (2, th), (2, vt, slice(1, 3)), (1, vt, 0), (2, tt),
        (2, cd, slice(1, 3)), (1, cd, 0), (1, el, 2), (2, kite, 1), (1, kite, 0), (2, cor, 1), (1, cor, 0),
    ]
    to_down = [
        (2, vel, slice(0, 2)), (1, vel, 2), (2, th), (2, vt, slice(0, 2)), (1, vt, 2), (2, tt),
        (2, cd, slice(0, 2)), (1, cd, 2), (1, el, 0), (2, kite, 0), (1, kite, 1), (2, cor, 0), (1, cor, 1),
    ]
    sems = (send_row, recv_row)
    row_copies = []
    for i, (n, b, *lead) in enumerate(to_up):
        lead = tuple(lead)
        row_copies.append(remote(part(b, 6, 6 + n, *lead), part(b, 2, 2 + n, *lead), sems, i, up, px))
    for i, (n, b, *lead) in enumerate(to_down):
        lead, i = tuple(lead), i + len(to_up)
        row_copies.append(remote(part(b, 2 - n, 2, *lead), part(b, 6 - n, 6, *lead), sems, i, down, px))
    for copy in own:
        copy.wait()
    pl.semaphore_wait(barrier, len(near))
    for copy in row_copies:
        copy.start()

    def view(ref, *lead):
        return lambda r, c: ref[lead + (r, c)]

    def level_views(l, src):
        vel, th, vt, tt = src
        return (
            [view(vel, k, l) for k in range(3)]
            + [view(th, l)]
            + [view(vt, k, l) for k in range(3)]
            + [view(tt, l)]
        )

    def geo_views(src):
        cd, el, kite, cor = src
        return (
            [view(cd, k) for k in range(3)]
            + [view(el, k) for k in range(3)]
            + [view(kite, v, k) for v in range(2) for k in range(3)]
            + [view(cor, v) for v in range(2)]
        )

    def pack_cols(items, tile):
        for r in range(nr):
            rs = slice(r * SUB, (r + 1) * SUB)
            ra = la = jnp.zeros((SUB, LANE), F32)
            for s, f in items:
                m = jnp.where(lane < LANE // 2, f(rs, head), f(rs, tail))
                m = roll(m, s, 1)
                ra = jnp.where((lane == s) | (lane == s + 1), m, ra)
                la = jnp.where(lane == (s + LANE - 1) % LANE, m, la)
            cs = slice(tile * LANE, (tile + 1) * LANE)
            p_right[rs, cs] = ra
            p_left[rs, cs] = la

    for i in (4, 5, 6, 7):
        loads[i].wait()
    own_geo = geo_views(bufs[4:8])
    pack_cols([(2 * k, f) for k, f in enumerate(own_geo)], 1)
    for i in (0, 1, 2, 3):
        loads[i].wait()
    items = []
    for l in range(levels):
        items += [(l * GROUP + 2 * k, f) for k, f in enumerate(level_views(l, bufs[:4]))]
    pack_cols(items, 0)

    sems = (send_col, recv_col)
    col_copies = [
        remote(p_right, g_right.at[0:rows], sems, 0, py, left),
        remote(p_left, g_left.at[0:rows], sems, 1, py, right),
        remote(p_right.at[rows - 2 : rows], g_right.at[rows + 6 : rows + 8], sems, 2, down, left),
        remote(p_right.at[0:2], g_right.at[rows : rows + 2], sems, 3, up, left),
        remote(p_left.at[0:2], g_left.at[rows : rows + 2], sems, 4, up, right),
    ]
    for copy in col_copies:
        copy.start()
    loads[8].wait()

    def put_geo(dst, at, f, area=None):
        for k in range(3):
            dst[(k,) + at] = 0.25 * f[k] * f[3 + k]
            if area is not None:
                dst[(5 + k,) + at] = SLOPE / f[k]
        for v in range(2):
            dst[(3 + v,) + at] = f[12 + v] * (f[6 + 3 * v] + f[7 + 3 * v] + f[8 + 3 * v])
        if area is not None:
            dst[(8,) + at] = 1.0 / area

    for r in range(nr):
        for c in range(nc):
            put_geo(geo, span(r, c), [f(*span(r, c)) for f in own_geo], b_area[span(r, c)])

    near_index = jnp.where(pos < 5, jnp.maximum(pos - 2, 0), jnp.minimum(pos + LANE - 11, LANE - 1))

    def strip(f, rs):
        return pick(jnp.where(lane < LANE // 2, f(rs, head), f(rs, tail)), near_index)

    def strip_levels(src, rs):
        got = [[strip(f, rs) for f in level_views(l, src)] for l in range(levels)]
        out = got[0]
        for l in range(1, levels):
            out = [jnp.where(group == l, x, y) for x, y in zip(got[l], out)]
        return out

    for r in range(nr):
        rs = slice(r * SUB, (r + 1) * SUB)
        for k, x in enumerate(strip_levels(bufs[:4], rs)):
            slev[k, rs] = x
        for k, f in enumerate(own_geo):
            sgeo[k, rs] = strip(f, rs)
        sgeo[14, rs] = strip(view(b_area), rs)

    def fields(grid, views):
        return [Field(grid, lambda r, c, f=f: f(*span(r, c))) for f in views]

    def run(grid, x, kites, dist, derived, swap=lambda i, f: f):
        f = fields(grid, derived)
        d = fields(grid, dist)
        cc, dd, outputs, stages = chain(
            grid, x[0:3], x[3], x[4:7], x[7], d, f[0:3], fields(grid, kites), f[3:5], swap
        )
        return cc, dd, outputs(f[5:9]), stages

    def block(l):
        grid = (nr, nc)
        cc, dd, outs, _ = run(
            grid,
            fields(grid, level_views(l, bufs[:4])),
            own_geo[6:12],
            own_geo[0:3],
            [view(geo, k) for k in range(9)],
        )
        dst = [view_at(o_vert, 0, l), view_at(o_vert, 1, l), view_at(o_kin, l), view_at(o_cell, l)]
        dst += [view_at(o_edge, k, l) for k in range(3)]
        for c in range(nc):
            for i, f in enumerate((cc, dd)):
                saved[i, l, :, span(0, c)[1]] = jnp.where(
                    sub < 4, roll(f(nr - 1, c), 2, 0), roll(f(0, c), -2, 0)
                )
        for r in range(nr):
            for c in range(nc):
                for put, f in zip(dst, outs):
                    put(span(r, c), f(r, c))

    def view_at(ref, *lead):
        def put(at, x):
            ref[lead + at] = x

        return put

    def inner(i, carry):
        for u in range(PAIR):
            block(i * PAIR + u)
        return carry

    lax.fori_loop(0, levels // PAIR, inner, 0)

    band_geo = geo_views(bands[4:8])
    merge = (sub == 0) | (sub == SUB - 1)
    def border_rows(l):
        grid = (1, nc)

        def swap(i, f, l=l):
            return Field(
                grid, lambda r, c: jnp.where(merge, saved[i, l, :, span(0, c)[1]], f(r, c))
            )

        outs, stages = run(
            grid,
            fields(grid, level_views(l, bands[:4])),
            band_geo[6:12],
            band_geo[0:3],
            [view(kgeo, k) for k in range(9)],
            swap,
        )[2:]
        dst = [(o_vert, (0, l)), (o_vert, (1, l)), (o_kin, (l,)), (o_cell, (l,))]
        dst += [(o_edge, (k, l)) for k in range(3)]
        both = ((rows - 1, 1, 1), (0, 6, 1))
        which = [
            ((rows - 1, 1, 1),),
            ((0, 6, 1),),
            both,
            both,
            ((rows - 2, 0, 2), (0, 6, 1)),
            both,
            ((rows - 1, 1, 1), (0, 6, 2)),
        ]

        def put():
            for c in range(nc):
                cs = span(0, c)[1]
                for (ref, lead), f, ranges in zip(dst, outs, which):
                    x = f(0, c)
                    for to, src, n in ranges:
                        ref[lead + (slice(to, to + n), cs)] = x[src : src + n]

        return stages, put

    def turn(x):
        return jnp.where(sub < 4, roll(x, -2, 0), roll(x, 2, 0))

    low = slice(0, SUB)
    edge_rows = slice(rows, rows + SUB)
    right_pos, left_pos = (pos == 11) | (pos == 12), pos == 1
    tiles = [slice(r * SUB, (r + 1) * SUB) for r in range(nr + 1)]
    last = slice(LANE, 2 * LANE)

    def insert_geo(k, r):
        rt = pick(g_right[tiles[r], last], jnp.where(pos == 12, 2 * k + 1, 2 * k))
        lt = pick(g_left[tiles[r], last], jnp.full((SUB, LANE), (2 * k - 1) % LANE, jnp.int32))
        own_part = edge_geo[k] if r == nr else sgeo[k, tiles[r]]
        return jnp.where(right_pos, rt, jnp.where(left_pos, lt, own_part))

    def insert(k, r):
        rt = roll(g_right[tiles[r], head], 11 - 2 * k, 1)
        lt = roll(g_left[tiles[r], head], 2 - 2 * k, 1)
        own_part = edge_levels[k] if r == nr else slev[k, tiles[r]]
        return jnp.where(right_pos, rt, jnp.where(left_pos, lt, own_part))

    grid = (nr + 1, 1)
    x = [Field(grid, lambda r, c, k=k: insert(k, r)) for k in range(8)]
    raw = [Field(grid, lambda r, c, k=k: insert_geo(k, r)) for k in range(14)]
    ws = [Field(grid, lambda r, c, k=k: 0.25 * raw[k](r, c) * raw[3 + k](r, c)) for k in range(3)]

    def weighed(v):
        a = [raw[6 + 3 * v + k] for k in range(3)]
        return Field(grid, lambda r, c: raw[12 + v](r, c) * (a[0](r, c) + a[1](r, c) + a[2](r, c)))

    _, _, outputs, stages = chain(
        grid, x[0:3], x[3], x[4:7], x[7], raw[0:3], ws, raw[6:12], [weighed(v) for v in range(2)],
    )
    scale = [Field(grid, lambda r, c, k=k: SLOPE / raw[k](r, c)) for k in range(3)]
    scale.append(Field(grid, lambda r, c: 1.0 / sgeo[14, tiles[r]]))
    outs = outputs(scale)
    own_tiles = range(nr)

    def build(fields_of, at, across=(0,)):
        for f in fields_of:
            for r in at:
                for c in across:
                    f(r, c)

    edge_levels, edge_geo = [], []
    for copy in col_copies[:2]:
        copy.wait()
    build(x + raw, own_tiles)
    cv, hv, cw, hw = (stages[0][2 * i : 2 * i + 2] for i in range(4))
    build([cv[0], hv[0], cw[0], hw[0]], range(nr - 1))
    build([cv[1], hv[1], cw[1], hw[1]], range(1, nr))
    build(stages[1][:2], range(nr - 1))
    build(stages[1][2:], range(1, nr))
    build(stages[2][:2], range(1, nr - 1))

    for copy in row_copies + col_copies[2:]:
        copy.wait()
    edge_levels += [turn(f) for f in strip_levels(bands[:4], low)]
    edge_geo += [turn(strip(f, low)) for f in band_geo]
    for c in range(nc):
        at = span(0, c)
        put_geo(kgeo, at, [f(*at) for f in band_geo], bands[8][at])
    build(x + raw, (nr,))
    for start in range(0, levels, BATCH):
        jobs = [border_rows(l) for l in range(start, start + BATCH)]
        for i in range(len(stages)):
            for kstages, _ in jobs:
                build(kstages[i], (0,), range(nc))
            if start + BATCH == levels:
                build(stages[i], range(nr + 1))
        for _, put in jobs:
            put()
    build(outs, own_tiles)
    refs_of = [(o_vert, (0,)), (o_vert, (1,)), (o_kin, ()), (o_cell, ())]
    refs_of += [(o_edge, (k,)) for k in range(3)]
    first, ends = lane == 0, lane >= LANE - 2
    end = lane == LANE - 1
    masks = [(None, end), (None, end), (first, None), (first, end), (first, ends), (first, ends), (first, ends)]
    back = [
        jnp.where(lane < LANE // 2, l * GROUP + 2, l * GROUP + 11 - LANE + lane) & (LANE - 1)
        for l in range(levels)
    ]
    done = [[f(r, 0) for f in outs] for r in range(nr)]
    for l in range(levels):
        for r in range(nr):
            moved = [pick(y, back[l]) for y in done[r]]
            for (ref, lead), z, (mf, me) in zip(refs_of, moved, masks):
                if mf is not None:
                    pltpu.store(ref.at[lead + (l, tiles[r], head)], z, mask=mf)
                if me is not None:
                    pltpu.store(ref.at[lead + (l, tiles[r], tail)], z, mask=me)


def drain_kernel(*refs):
    src, dst, sem = refs[:4], refs[4:8], refs[8]
    copies = [pltpu.make_async_copy(a, b, sem.at[i]) for i, (a, b) in enumerate(zip(src, dst))]
    for copy in copies:
        copy.start()
    for copy in copies:
        copy.wait()


def local(counts, vel, th, vt, tt, cd, el, area, kite, cor):
    args = (vel, th, vt, tt, cd, el, kite, cor, area)
    levels, rows, cols = th.shape
    outs = [(2, levels, rows, cols), (levels, rows, cols), (levels, rows, cols), (3, levels, rows, cols)]
    band = lambda a: a.shape[:-2] + (SUB, cols)
    hbm, vmem = pl.BlockSpec(memory_space=pl.ANY), pl.BlockSpec(memory_space=pltpu.VMEM)
    side = (rows + SUB, 2 * LANE)
    kept = pl.pallas_call(
        lambda *refs: main_kernel(counts, *refs),
        out_shape=[pltpu.VMEM(s, F32) for s in outs],
        in_specs=[hbm] * len(args),
        out_specs=[vmem] * len(outs),
        scratch_shapes=[pltpu.VMEM(a.shape, F32) for a in args]
        + [pltpu.VMEM(band(a), F32) for a in args]
        + [pltpu.VMEM(s, F32) for s in ((rows, 2 * LANE), (rows, 2 * LANE), side, side)]
        + [
            pltpu.VMEM((9, rows, cols), F32),
            pltpu.VMEM((9, SUB, cols), F32),
            pltpu.VMEM((15, rows + SUB, LANE), F32),
            pltpu.VMEM((8, rows + SUB, LANE), F32),
            pltpu.VMEM((2, levels, SUB, cols), F32),
            pltpu.SemaphoreType.DMA((9,)),
            pltpu.SemaphoreType.DMA((18,)),
            pltpu.SemaphoreType.DMA((26,)),
            pltpu.SemaphoreType.DMA((26,)),
            pltpu.SemaphoreType.DMA((5,)),
            pltpu.SemaphoreType.DMA((5,)),
        ],
        compiler_params=pltpu.CompilerParams(collective_id=0, has_side_effects=True),
        name="main",
    )(*args)
    return pl.pallas_call(
        drain_kernel,
        out_shape=[jax.ShapeDtypeStruct(s, F32) for s in outs],
        in_specs=[vmem] * len(outs),
        out_specs=[pl.BlockSpec(memory_space=pltpu.HBM)] * len(outs),
        scratch_shapes=[pltpu.SemaphoreType.DMA((len(outs),))],
        name="drain",
    )(*[pltpu.with_memory_space_constraint(x, pltpu.VMEM) for x in kept])


def solution(mesh):
    counts = (mesh.shape["py"], mesh.shape["px"])
    p4, p3 = P(None, None, "py", "px"), P(None, "py", "px")
    return jax.shard_map(
        lambda *args: local(counts, *args),
        mesh=mesh,
        in_specs=(p4, p3, p4, p3, p3, p3, P("py", "px"), p4, p3),
        out_specs=(p4, p3, p3, p4),
        check_vma=False,
    )
```

```python
import jax
import jax.numpy as jnp
from jax import lax
from jax.experimental import pallas as pl
from jax.experimental.pallas import tpu as pltpu
from jax.sharding import PartitionSpec as P

SUB = 8
LANE = 128
GROUP = 16
PAIR = 2
MESH = pl.DeviceIdType.MESH
F32 = jnp.float32
SLOPE = -0.5 / 36.0


def iotas():
    sub = lax.broadcasted_iota(jnp.int32, (SUB, LANE), 0)
    lane = lax.broadcasted_iota(jnp.int32, (SUB, LANE), 1)
    return sub, lane


def roll(x, shift, axis):
    n = (SUB, LANE)[axis]
    return pltpu.roll(x, shift % n, axis) if shift % n else x


def pick(x, index):
    return jnp.take_along_axis(x, index, axis=1)


def span(r, c):
    return (slice(r * SUB, (r + 1) * SUB), slice(c * LANE, (c + 1) * LANE))


class Field:
    def __init__(self, grid, make):
        self.grid, self.make, self.memo = grid, make, {}

    def __call__(self, r, c):
        key = (r % self.grid[0], c % self.grid[1])
        if key not in self.memo:
            self.memo[key] = self.make(*key)
        return self.memo[key]


def chain(grid, v, h, t, g, dist, ew, kt, ct, swap=lambda i, f: f):
    sub, lane = iotas()

    def lift(fn, *fields):
        return Field(grid, lambda r, c: fn(*[f(r, c) for f in fields]))

    def row_shift(f, a):
        rolled = Field(grid, lambda r, c: roll(f(r, c), -a, 0))
        if grid[0] == 1:
            return rolled
        keep = sub < SUB - 1 if a == 1 else sub > 0
        return Field(grid, lambda r, c: jnp.where(keep, rolled(r, c), rolled(r + a, c)))

    def col_shift(f, b):
        rolled = Field(grid, lambda r, c: roll(f(r, c), -b, 1))
        if grid[1] == 1:
            return rolled
        keep = lane < LANE - 1 if b == 1 else lane > 0
        return Field(grid, lambda r, c: jnp.where(keep, rolled(r, c), rolled(r, c + b)))

    def parts(vv, hh):
        flux = [lift(lambda a, b: a * b, vv[k], dist[k]) for k in range(3)]
        c0 = lift(lambda a, b, c: a + b - c, flux[0], row_shift(flux[2], 1), flux[1])
        c1 = lift(lambda a, b, c: a - b - c, flux[1], flux[2], col_shift(row_shift(flux[0], -1), 1))
        hc = col_shift(hh, 1)
        hr = row_shift(hh, 1)
        hd = row_shift(hc, -1)
        mix = lambda a, b, c, p, q, s: a * p + b * q + c * s
        h0 = lift(mix, kt[0], kt[1], kt[2], hh, hr, hc)
        h1 = lift(mix, kt[3], kt[4], kt[5], hh, hc, hd)
        return (c0, c1), (h0, h1)

    cv, hv = parts(v, h)
    cw, hw = parts(t, g)

    def potential(k):
        def make(r, c):
            a0 = ct[k](r, c) + cv[k](r, c)
            a1 = cw[k](r, c)
            b0 = hv[k](r, c)
            b1 = hw[k](r, c)
            bm, be = b0 + 0.5 * b1, b0 + b1
            m = bm * be
            scale_all = 1.0 / (b0 * m)
            mid = (a0 + a0 + a1) * (b0 * be)
            late = mid + (a0 + a1) * (b0 * bm)
            return (a0 * m + mid + late) * scale_all, late * scale_all

        both = Field(grid, make)
        return Field(grid, lambda r, c: both(r, c)[0]), Field(grid, lambda r, c: both(r, c)[1])

    p0, q0 = potential(0)
    p1, q1 = potential(1)
    add = lambda a, b: a + b
    add3 = lambda a, b, c: a + b + c

    def cell(f0, f1):
        f0_up = row_shift(f0, -1)
        f1_down = row_shift(f1, 1)
        pair = lift(add, f0, f1)
        return lift(add3, pair, f0_up, col_shift(lift(add, pair, f1_down), -1)), f0_up, f1_down, pair

    cc, p0_up, p1_down, pair = cell(p0, p1)
    dd = cell(q0, q1)[0]
    cc, dd = swap(0, cc), swap(1, dd)
    p1_low = col_shift(p1_down, -1)

    def neighbours(f):
        fc = col_shift(f, 1)
        return row_shift(f, 1), fc, row_shift(fc, -1)

    cn, dn = neighbours(cc), neighbours(dd)
    ends = [lift(add, p0, p1_low), pair, lift(add, p1, p0_up)]
    en = [
        lift(lambda w, a, b: w * (a * (a + b) + (1.0 / 3.0) * (b * b)), ew[k], v[k], t[k])
        for k in range(3)
    ]
    e_up = row_shift(en[0], -1)
    e_low = col_shift(lift(add, en[1], row_shift(en[2], 1)), -1)

    def outputs(scale):
        def edge(k):
            def make(r, c):
                slope = v[k](r, c) * (cn[k](r, c) - cc(r, c)) + t[k](r, c) * (dn[k](r, c) - dd(r, c))
                return ends[k](r, c) * (1.0 / 12.0) + scale[k](r, c) * slope

            return Field(grid, make)

        kin = Field(
            grid,
            lambda r, c: (en[0](r, c) + en[1](r, c) + en[2](r, c) + e_up(r, c) + e_low(r, c)) * scale[3](r, c),
        )
        return [
            lift(lambda a: a * (1.0 / 6.0), p0),
            lift(lambda a: a * (1.0 / 6.0), p1),
            kin,
            lift(lambda a: a * (1.0 / 36.0), cc),
        ] + [edge(k) for k in range(3)]

    stages = [[*cv, *hv, *cw, *hw, e_low], [p0, q0, p1, q1], [cc, dd, p1_low], [*cn, *dn]]
    return cc, dd, outputs, stages


def view(ref, *lead):
    return lambda r, c: ref[lead + (r, c)]


def level_views(l, src):
    vel, th, vt, tt = src
    return (
        [view(vel, k, l) for k in range(3)]
        + [view(th, l)]
        + [view(vt, k, l) for k in range(3)]
        + [view(tt, l)]
    )


def geo_views(src):
    cd, el, kite, cor = src
    return (
        [view(cd, k) for k in range(3)]
        + [view(el, k) for k in range(3)]
        + [view(kite, v, k) for v in range(2) for k in range(3)]
        + [view(cor, v) for v in range(2)]
    )


def put_geo(dst, at, f, area):
    for k in range(3):
        dst[(k,) + at] = 0.25 * f[k] * f[3 + k]
        dst[(5 + k,) + at] = SLOPE / f[k]
    for v in range(2):
        dst[(3 + v,) + at] = f[12 + v] * (f[6 + 3 * v] + f[7 + 3 * v] + f[8 + 3 * v])
    dst[(8,) + at] = 1.0 / area


def fields(grid, views):
    return [Field(grid, lambda r, c, f=f: f(*span(r, c))) for f in views]


def run(grid, x, kites, dist, derived, swap=lambda i, f: f):
    f = fields(grid, derived)
    d = fields(grid, dist)
    cc, dd, outputs, stages = chain(
        grid, x[0:3], x[3], x[4:7], x[7], d, f[0:3], fields(grid, kites), f[3:5], swap
    )
    return cc, dd, outputs(f[5:9]), stages


def build(fields_of):
    for f in fields_of:
        for r in range(f.grid[0]):
            for c in range(f.grid[1]):
                f(r, c)


class Strips:
    def __init__(self, levels, cols):
        _, lane = iotas()
        self.levels, self.lane = levels, lane
        self.head, self.tail = slice(0, LANE), slice(cols - LANE, cols)
        pos = lane & (GROUP - 1)
        self.pos, self.group = pos, lane >> 4
        self.index = jnp.where(pos < 5, jnp.maximum(pos - 2, 0), jnp.minimum(pos + LANE - 11, LANE - 1))
        self.back = [
            jnp.where(lane < LANE // 2, l * GROUP + 2, l * GROUP + 11 - LANE + lane) & (LANE - 1)
            for l in range(levels)
        ]

    def own(self, f, rs):
        return pick(jnp.where(self.lane < LANE // 2, f(rs, self.head), f(rs, self.tail)), self.index)

    def own_levels(self, src, rs):
        got = [[self.own(f, rs) for f in level_views(l, src)] for l in range(self.levels)]
        out = got[0]
        for l in range(1, self.levels):
            out = [jnp.where(self.group == l, x, y) for x, y in zip(got[l], out)]
        return out

    def insert(self, x, right, left):
        pos = self.pos
        return jnp.where((pos == 11) | (pos == 12), right, jnp.where(pos == 1, left, x))

    def with_level(self, k, x, right, left):
        return self.insert(x, roll(right, 11 - 2 * k, 1), roll(left, 2 - 2 * k, 1))

    def with_geo(self, k, x, right, left):
        rt = pick(right, jnp.where(self.pos == 12, 2 * k + 1, 2 * k))
        lt = pick(left, jnp.full((SUB, LANE), (2 * k - 1) % LANE, jnp.int32))
        return self.insert(x, rt, lt)

    def masks(self):
        lane = self.lane
        first, end, ends = lane == 0, lane == LANE - 1, lane >= LANE - 2
        return [(None, end), (None, end), (first, None), (first, end)] + [(first, ends)] * 3


def strip_chain(grid, x, raw, area, swap=lambda i, f: f):
    ws = [Field(grid, lambda r, c, k=k: 0.25 * raw[k](r, c) * raw[3 + k](r, c)) for k in range(3)]

    def weighed(v):
        a = [raw[6 + 3 * v + k] for k in range(3)]
        return Field(grid, lambda r, c: raw[12 + v](r, c) * (a[0](r, c) + a[1](r, c) + a[2](r, c)))

    cc, dd, outputs, stages = chain(
        grid, x[0:3], x[3], x[4:7], x[7], raw[0:3], ws, raw[6:12], [weighed(v) for v in range(2)], swap
    )
    scale = [Field(grid, lambda r, c, k=k: SLOPE / raw[k](r, c)) for k in range(3)]
    scale.append(Field(grid, lambda r, c: 1.0 / area(r, c)))
    return cc, dd, outputs(scale), stages


def planes(vert, kin, cell, edge):
    return [(vert, (0,)), (vert, (1,)), (kin, ()), (cell, ())] + [(edge, (k,)) for k in range(3)]


def main_kernel(counts, *refs):
    hbm = refs[:9]
    o_vert, o_kin, o_cell, o_edge = refs[9:13]
    bands = refs[13:22]
    g_right, g_left, saved, ssaved = refs[22:26]
    bufs = refs[26:35]
    p_right, p_left, geo, slev, sgeo, tally = refs[35:41]
    in_sem, own_sem, send_row, recv_row, send_col, recv_col = refs[41:47]
    ny, nx = counts
    py, px = lax.axis_index("py"), lax.axis_index("px")
    down, up = lax.rem(py + 1, ny), lax.rem(py + ny - 1, ny)
    right, left = lax.rem(px + 1, nx), lax.rem(px + nx - 1, nx)

    barrier = pltpu.get_barrier_semaphore()
    near = [
        (up, px), (down, px), (py, left), (py, right),
        (up, left), (up, right), (down, left), (down, right),
    ]
    for y, x in near:
        pl.semaphore_signal(barrier, inc=1, device_id={"py": y, "px": x}, device_id_type=MESH)

    b_area = bufs[8]
    levels, rows, cols = bufs[1].shape
    nr, nc = rows // SUB, cols // LANE
    sub, lane = iotas()

    def await_rows(sem, n):
        pltpu.make_async_copy(tally.at[0:n], tally.at[0:n], sem).wait()

    def part(ref, a, b, *lead):
        rest = (slice(None),) * (len(ref.shape) - 2 - len(lead))
        return ref.at[lead + rest + (slice(a, b), slice(None))]

    def count(ref):
        n = 1
        for d in ref.shape[:-1]:
            n *= d
        return n

    own = []
    for a, b in zip(hbm, bands):
        own.append(pltpu.make_async_copy(part(a, rows - 2, rows), part(b, 0, 2), own_sem.at[0]))
        own.append(pltpu.make_async_copy(part(a, 0, 2), part(b, 6, 8), own_sem.at[0]))
    for copy in own:
        copy.start()
    own_rows = sum(4 * count(b) // SUB for b in bands)
    late = (4, 5, 6, 7, 8, 0, 1, 2, 3)
    for i in late:
        pltpu.make_async_copy(hbm[i], bufs[i], in_sem.at[0 if i >= 4 else 1]).start()

    def remote(src, dst, send, recv, y, x):
        return pltpu.make_async_remote_copy(
            src_ref=src,
            dst_ref=dst,
            send_sem=send,
            recv_sem=recv,
            device_id={"py": y, "px": x},
            device_id_type=MESH,
        )

    vel, th, vt, tt, cd, el, kite, cor = bands[:8]
    to_up = [
        (2, vel, slice(1, 3)), (1, vel, 0), (2, th), (2, vt, slice(1, 3)), (1, vt, 0), (2, tt),
        (2, cd, slice(1, 3)), (1, cd, 0), (1, el, 2), (2, kite, 1), (1, kite, 0), (2, cor, 1), (1, cor, 0),
    ]
    to_down = [
        (2, vel, slice(0, 2)), (1, vel, 2), (2, th), (2, vt, slice(0, 2)), (1, vt, 2), (2, tt),
        (2, cd, slice(0, 2)), (1, cd, 2), (1, el, 0), (2, kite, 0), (1, kite, 1), (2, cor, 0), (1, cor, 1),
    ]
    sems = (send_row.at[0], recv_row.at[0])
    row_copies, sent = [], 0
    for n, b, *lead in to_up:
        src = part(b, 6, 6 + n, *lead)
        row_copies.append(remote(src, part(b, 2, 2 + n, *lead), *sems, up, px))
        sent += count(src)
    for n, b, *lead in to_down:
        src = part(b, 2 - n, 2, *lead)
        row_copies.append(remote(src, part(b, 6 - n, 6, *lead), *sems, down, px))
        sent += count(src)
    await_rows(own_sem.at[0], own_rows)
    pl.semaphore_wait(barrier, len(near))
    for copy in row_copies:
        copy.start()

    strips = Strips(levels, cols)
    head, tail = strips.head, strips.tail
    tiles = [slice(r * SUB, (r + 1) * SUB) for r in range(nr + 1)]

    def pack_cols(items, tile):
        for rs in tiles[:nr]:
            ra = la = jnp.zeros((SUB, LANE), F32)
            for s, f in items:
                m = jnp.where(lane < LANE // 2, f(rs, head), f(rs, tail))
                m = roll(m, s, 1)
                ra = jnp.where((lane == s) | (lane == s + 1), m, ra)
                la = jnp.where(lane == (s + LANE - 1) % LANE, m, la)
            cs = slice(tile * LANE, (tile + 1) * LANE)
            p_right[rs, cs] = ra
            p_left[rs, cs] = la

    await_rows(in_sem.at[0], sum(count(b) for b in bufs[4:]))
    own_geo = geo_views(bufs[4:8])
    pack_cols([(2 * k, f) for k, f in enumerate(own_geo)], 1)
    await_rows(in_sem.at[1], sum(count(b) for b in bufs[:4]))
    items = []
    for l in range(levels):
        items += [(l * GROUP + 2 * k, f) for k, f in enumerate(level_views(l, bufs[:4]))]
    pack_cols(items, 0)

    def column(src, dst, i, y, x):
        return remote(src, dst, send_col.at[i], recv_col.at[i], y, x)

    col_copies = [
        column(p_right, g_right.at[0:rows], 0, py, left),
        column(p_left, g_left.at[0:rows], 1, py, right),
        column(p_right.at[rows - 2 : rows], g_right.at[rows + 4 : rows + 6], 2, down, left),
        column(p_right.at[0:2], g_right.at[rows + 2 : rows + 4], 3, up, left),
        column(p_left.at[0:2], g_left.at[rows + 2 : rows + 4], 4, up, right),
    ]
    for copy in col_copies:
        copy.start()

    for r in range(nr):
        for c in range(nc):
            put_geo(geo, span(r, c), [f(*span(r, c)) for f in own_geo], b_area[span(r, c)])

    for rs in tiles[:nr]:
        for k, x in enumerate(strips.own_levels(bufs[:4], rs)):
            slev[k, rs] = x
        for k, f in enumerate(own_geo + [view(b_area)]):
            sgeo[k, rs] = strips.own(f, rs)

    outputs_of = planes(o_vert, o_kin, o_cell, o_edge)

    def block(l):
        cc, dd, outs, _ = run(
            (nr, nc),
            fields((nr, nc), level_views(l, bufs[:4])),
            own_geo[6:12],
            own_geo[0:3],
            [view(geo, k) for k in range(9)],
        )
        for c in range(nc):
            for i, f in enumerate((cc, dd)):
                saved[i, l, :, span(0, c)[1]] = jnp.where(
                    sub < 4, roll(f(nr - 1, c), 2, 0), roll(f(0, c), -2, 0)
                )
        for r in range(nr):
            for c in range(nc):
                for (ref, lead), f in zip(outputs_of, outs):
                    ref[lead + (l,) + span(r, c)] = f(r, c)

    def inner(i, carry):
        for u in range(PAIR):
            block(i * PAIR + u)
        return carry

    lax.fori_loop(0, levels // PAIR, inner, 0)

    for copy in col_copies[:2]:
        copy.wait()
    grid = (nr, 1)
    last = slice(LANE, 2 * LANE)
    x = [
        Field(
            grid,
            lambda r, c, k=k: strips.with_level(
                k, slev[k, tiles[r]], g_right[tiles[r], head], g_left[tiles[r], 0:LANE]
            ),
        )
        for k in range(8)
    ]
    raw = [
        Field(
            grid,
            lambda r, c, k=k: strips.with_geo(
                k, sgeo[k, tiles[r]], g_right[tiles[r], last], g_left[tiles[r], last]
            ),
        )
        for k in range(14)
    ]
    cc, dd, outs, stages = strip_chain(grid, x, raw, lambda r, c: sgeo[14, tiles[r]])
    for stage in [x + raw] + stages + [outs]:
        build(stage)
    for i, f in enumerate((cc, dd)):
        ssaved[i] = jnp.where(sub < 4, roll(f(nr - 1, 0), 2, 0), roll(f(0, 0), -2, 0))
    for l in range(levels):
        for r in range(nr):
            moved = [pick(f(r, 0), strips.back[l]) for f in outs]
            for (ref, lead), z, (mf, me) in zip(outputs_of, moved, strips.masks()):
                if mf is not None:
                    pltpu.store(ref.at[lead + (l, tiles[r], head)], z, mask=mf)
                if me is not None:
                    pltpu.store(ref.at[lead + (l, tiles[r], tail)], z, mask=me)

    for copy in col_copies[2:]:
        copy.wait()
    await_rows(send_row.at[0], sent)
    await_rows(recv_row.at[0], sent)


def finish_kernel(*refs):
    kept = refs[0:4]
    bands = refs[4:13]
    g_right, g_left, saved, ssaved = refs[13:17]
    final = refs[17:21]
    ends = refs[21:25]
    kgeo, sem = refs[25:27]
    levels, rows, cols = kept[1].shape
    nr, nc = rows // SUB, cols // LANE
    sub, lane = iotas()
    copies = []

    def send(src, dst):
        copies.append(pltpu.make_async_copy(src, dst, sem.at[len(copies)]))
        copies[-1].start()

    def part(ref, a, b, *lead):
        rest = (slice(None),) * (len(ref.shape) - 2 - len(lead))
        return ref.at[lead + rest + (slice(a, b), slice(None))]

    if nr > 2:
        for a, b in zip(kept, final):
            send(part(a, SUB, rows - SUB), part(b, SUB, rows - SUB))

    strips = Strips(levels, cols)
    low, top = slice(0, SUB), slice(rows, rows + SUB)
    last, head = slice(LANE, 2 * LANE), slice(0, LANE)
    first_rows, last_rows = slice(0, SUB), slice(rows - SUB, rows)

    def border(g, cs):
        a, b = roll(g[last_rows, cs], 2, 0), roll(g[first_rows, cs], -2, 0)
        return jnp.where(sub < 2, a, jnp.where(sub >= 6, b, g[top, cs]))

    band_geo = geo_views(bands[4:8])
    one = (1, 1)
    const = lambda t: Field(one, lambda r, c: t)
    sides = [(border(g_right, cs), border(g_left, cs)) for cs in (head, last)]
    own_levels = strips.own_levels(bands[:4], low)
    own_geo = [strips.own(f, low) for f in band_geo]
    area = strips.own(view(bands[8]), low)
    x = [const(strips.with_level(k, own_levels[k], *sides[0])) for k in range(8)]
    raw = [const(strips.with_geo(k, own_geo[k], *sides[1])) for k in range(14)]
    for c in range(nc):
        at = span(0, c)
        put_geo(kgeo, at, [f(*at) for f in band_geo], bands[8][at])

    merge = (sub == 0) | (sub == SUB - 1)

    def swap_with(grid, load):
        return lambda i, f: Field(grid, lambda r, c: jnp.where(merge, load(i, c), f(r, c)))

    _, _, souts, sstages = strip_chain(
        one, x, raw, lambda r, c: area, swap_with(one, lambda i, c: ssaved[i])
    )
    grid = (1, nc)
    jobs = []
    for l in range(levels):
        jobs.append(
            run(
                grid,
                fields(grid, level_views(l, bands[:4])),
                band_geo[6:12],
                band_geo[0:3],
                [view(kgeo, k) for k in range(9)],
                swap_with(grid, lambda i, c, l=l: saved[i, l, :, span(0, c)[1]]),
            )[2:]
        )

    changed = [(0, 1), (1, 0), (1, 1), (1, 1), (1, 2), (1, 1), (2, 1)]
    src_of, end_of, dst_of = planes(*kept), planes(*ends), planes(*final)
    masks = strips.masks()

    def finalize(i):
        ref, lead = src_of[i]
        end = end_of[i][0]
        n_top, n_low = changed[i]
        y = souts[i](0, 0)
        zs = [pick(y, strips.back[l]) for l in range(levels)]
        for l in range(levels):
            for c in range(nc):
                cs = span(0, c)[1]
                t = jobs[l][0][i](0, c)
                for m, at in zip(masks[i], (0, nc - 1)):
                    if m is not None and at == c:
                        t = jnp.where(m, zs[l], t)
                for n, to, own, shift, where in (
                    (n_top, first_rows, first_rows, 2, sub < n_top),
                    (n_low, slice(SUB, 2 * SUB), last_rows, -2, sub >= SUB - n_low),
                ):
                    u = ref[lead + (l, own, cs)]
                    if n:
                        u = jnp.where(where, roll(t, shift, 0), u)
                    end[lead + (l, to, cs)] = u
        dst = dst_of[i][0]
        send(part(end, 0, SUB, *lead), part(dst, 0, SUB, *lead))
        send(part(end, SUB, 2 * SUB, *lead), part(dst, rows - SUB, rows, *lead))

    ready = [(), (0, 1, 2), (3,), (4, 5, 6)]
    for stage, done in enumerate(ready):
        for _, stages in jobs:
            build(stages[stage])
        build(sstages[stage])
        for i in done:
            finalize(i)
    for copy in copies:
        copy.wait()


def local(counts, vel, th, vt, tt, cd, el, area, kite, cor):
    args = (vel, th, vt, tt, cd, el, kite, cor, area)
    levels, rows, cols = th.shape
    outs = [(2, levels, rows, cols), (levels, rows, cols), (levels, rows, cols), (3, levels, rows, cols)]
    short = lambda s, n: s[:-2] + (n, cols)
    hbm, vmem = pl.BlockSpec(memory_space=pl.ANY), pl.BlockSpec(memory_space=pltpu.VMEM)
    side = (rows + SUB, 2 * LANE)
    passed = outs + [short(a.shape, SUB) for a in args]
    passed += [side, side, (2, levels, SUB, cols), (2, SUB, LANE)]
    kept = pl.pallas_call(
        lambda *refs: main_kernel(counts, *refs),
        out_shape=[pltpu.VMEM(s, F32) for s in passed],
        in_specs=[hbm] * len(args),
        out_specs=[vmem] * len(passed),
        scratch_shapes=[pltpu.VMEM(a.shape, F32) for a in args]
        + [
            pltpu.VMEM((rows, 2 * LANE), F32),
            pltpu.VMEM((rows, 2 * LANE), F32),
            pltpu.VMEM((9, rows, cols), F32),
            pltpu.VMEM((8, rows, LANE), F32),
            pltpu.VMEM((15, rows, LANE), F32),
            pltpu.VMEM((8 * levels * rows, 1, cols), F32),
        ]
        + [pltpu.SemaphoreType.DMA((n,)) for n in (2, 1, 1, 1, 5, 5)],
        compiler_params=pltpu.CompilerParams(collective_id=0, has_side_effects=True),
        name="main",
    )(*args)
    return pl.pallas_call(
        finish_kernel,
        out_shape=[jax.ShapeDtypeStruct(s, F32) for s in outs],
        in_specs=[vmem] * len(passed),
        out_specs=[pl.BlockSpec(memory_space=pltpu.HBM)] * len(outs),
        scratch_shapes=[pltpu.VMEM(short(s, 2 * SUB), F32) for s in outs]
        + [pltpu.VMEM((9, SUB, cols), F32), pltpu.SemaphoreType.DMA((18,))],
        name="finish",
    )(*[pltpu.with_memory_space_constraint(x, pltpu.VMEM) for x in kept])


def solution(mesh):
    counts = (mesh.shape["py"], mesh.shape["px"])
    p4, p3 = P(None, None, "py", "px"), P(None, "py", "px")
    return jax.shard_map(
        lambda *args: local(counts, *args),
        mesh=mesh,
        in_specs=(p4, p3, p4, p3, p3, p3, P("py", "px"), p4, p3),
        out_specs=(p4, p3, p3, p4),
        check_vma=False,
    )
```

```python
import jax
import jax.numpy as jnp
from jax import lax
from jax.experimental import pallas as pl
from jax.experimental.pallas import tpu as pltpu
from jax.sharding import PartitionSpec as P

SUB = 8
LANE = 128
GROUP = 16
PAIR = 2
SLOT = (0, 8, 9, 2, 4, 10, 11, 6)
TWO = (0, 3, 4, 7)
MESH = pl.DeviceIdType.MESH
F32 = jnp.float32
SLOPE = -0.5 / 36.0


def iotas():
    sub = lax.broadcasted_iota(jnp.int32, (SUB, LANE), 0)
    lane = lax.broadcasted_iota(jnp.int32, (SUB, LANE), 1)
    return sub, lane


def roll(x, shift, axis):
    n = (SUB, LANE)[axis]
    return pltpu.roll(x, shift % n, axis) if shift % n else x


def pick(x, index):
    return jnp.take_along_axis(x, index, axis=1)


def span(r, c):
    return (slice(r * SUB, (r + 1) * SUB), slice(c * LANE, (c + 1) * LANE))


class Field:
    def __init__(self, grid, make):
        self.grid, self.make, self.memo = grid, make, {}

    def __call__(self, r, c):
        key = (r % self.grid[0], c % self.grid[1])
        if key not in self.memo:
            self.memo[key] = self.make(*key)
        return self.memo[key]


def chain(grid, v, h, t, g, dist, ew, kt, ct, swap=lambda i, f: f):
    sub, lane = iotas()

    def lift(fn, *fields):
        return Field(grid, lambda r, c: fn(*[f(r, c) for f in fields]))

    def row_shift(f, a):
        rolled = Field(grid, lambda r, c: roll(f(r, c), -a, 0))
        if grid[0] == 1:
            return rolled
        keep = sub < SUB - 1 if a == 1 else sub > 0
        return Field(grid, lambda r, c: jnp.where(keep, rolled(r, c), rolled(r + a, c)))

    def col_shift(f, b):
        rolled = Field(grid, lambda r, c: roll(f(r, c), -b, 1))
        if grid[1] == 1:
            return rolled
        keep = lane < LANE - 1 if b == 1 else lane > 0
        return Field(grid, lambda r, c: jnp.where(keep, rolled(r, c), rolled(r, c + b)))

    def parts(vv, hh):
        flux = [lift(lambda a, b: a * b, vv[k], dist[k]) for k in range(3)]
        c0 = lift(lambda a, b, c: a + b - c, flux[0], row_shift(flux[2], 1), flux[1])
        c1 = lift(lambda a, b, c: a - b - c, flux[1], flux[2], col_shift(row_shift(flux[0], -1), 1))
        hc = col_shift(hh, 1)
        hr = row_shift(hh, 1)
        hd = row_shift(hc, -1)
        mix = lambda a, b, c, p, q, s: a * p + b * q + c * s
        h0 = lift(mix, kt[0], kt[1], kt[2], hh, hr, hc)
        h1 = lift(mix, kt[3], kt[4], kt[5], hh, hc, hd)
        return (c0, c1), (h0, h1)

    cv, hv = parts(v, h)
    cw, hw = parts(t, g)

    def potential(k):
        def make(r, c):
            a0 = ct[k](r, c) + cv[k](r, c)
            a1 = cw[k](r, c)
            b0 = hv[k](r, c)
            b1 = hw[k](r, c)
            bm, be = b0 + 0.5 * b1, b0 + b1
            m = bm * be
            scale_all = 1.0 / (b0 * m)
            mid = (a0 + a0 + a1) * (b0 * be)
            late = mid + (a0 + a1) * (b0 * bm)
            return (a0 * m + mid + late) * scale_all, late * scale_all

        both = Field(grid, make)
        return Field(grid, lambda r, c: both(r, c)[0]), Field(grid, lambda r, c: both(r, c)[1])

    p0, q0 = potential(0)
    p1, q1 = potential(1)
    add = lambda a, b: a + b
    add3 = lambda a, b, c: a + b + c

    def cell(f0, f1):
        f0_up = row_shift(f0, -1)
        f1_down = row_shift(f1, 1)
        pair = lift(add, f0, f1)
        return lift(add3, pair, f0_up, col_shift(lift(add, pair, f1_down), -1)), f0_up, f1_down, pair

    cc, p0_up, p1_down, pair = cell(p0, p1)
    dd = cell(q0, q1)[0]
    cc, dd = swap(0, cc), swap(1, dd)
    p1_low = col_shift(p1_down, -1)

    def neighbours(f):
        fc = col_shift(f, 1)
        return row_shift(f, 1), fc, row_shift(fc, -1)

    cn, dn = neighbours(cc), neighbours(dd)
    ends = [lift(add, p0, p1_low), pair, lift(add, p1, p0_up)]
    en = [
        lift(lambda w, a, b: w * (a * (a + b) + (1.0 / 3.0) * (b * b)), ew[k], v[k], t[k])
        for k in range(3)
    ]
    e_up = row_shift(en[0], -1)
    e_low = col_shift(lift(add, en[1], row_shift(en[2], 1)), -1)

    def outputs(scale):
        def edge(k):
            def make(r, c):
                slope = v[k](r, c) * (cn[k](r, c) - cc(r, c)) + t[k](r, c) * (dn[k](r, c) - dd(r, c))
                return ends[k](r, c) * (1.0 / 12.0) + scale[k](r, c) * slope

            return Field(grid, make)

        kin = Field(
            grid,
            lambda r, c: (en[0](r, c) + en[1](r, c) + en[2](r, c) + e_up(r, c) + e_low(r, c)) * scale[3](r, c),
        )
        return [
            lift(lambda a: a * (1.0 / 6.0), p0),
            lift(lambda a: a * (1.0 / 6.0), p1),
            kin,
            lift(lambda a: a * (1.0 / 36.0), cc),
        ] + [edge(k) for k in range(3)]

    stages = [[*cv, *hv, *cw, *hw, e_low], [p0, q0, p1, q1], [cc, dd, p1_low], [*cn, *dn]]
    return cc, dd, outputs, stages


def view(ref, *lead):
    return lambda r, c: ref[lead + (r, c)]


def level_views(l, src):
    vel, th, vt, tt = src
    return (
        [view(vel, k, l) for k in range(3)]
        + [view(th, l)]
        + [view(vt, k, l) for k in range(3)]
        + [view(tt, l)]
    )


def geo_views(src):
    cd, el, kite, cor = src
    return (
        [view(cd, k) for k in range(3)]
        + [view(el, k) for k in range(3)]
        + [view(kite, v, k) for v in range(2) for k in range(3)]
        + [view(cor, v) for v in range(2)]
    )


def geo_slot(k):
    return 12 if k == 0 else (1 + (k - 1) % 7) * GROUP + 12 + (k - 1) // 7


def put_geo(dst, at, f, area):
    for k in range(3):
        dst[(k,) + at] = 0.25 * f[k] * f[3 + k]
        dst[(5 + k,) + at] = SLOPE / f[k]
    for v in range(2):
        dst[(3 + v,) + at] = f[12 + v] * (f[6 + 3 * v] + f[7 + 3 * v] + f[8 + 3 * v])
    dst[(8,) + at] = 1.0 / area


def fields(grid, views):
    return [Field(grid, lambda r, c, f=f: f(*span(r, c))) for f in views]


def run(grid, x, kites, dist, derived, swap=lambda i, f: f):
    f = fields(grid, derived)
    d = fields(grid, dist)
    cc, dd, outputs, stages = chain(
        grid, x[0:3], x[3], x[4:7], x[7], d, f[0:3], fields(grid, kites), f[3:5], swap
    )
    return cc, dd, outputs(f[5:9]), stages


def build(fields_of):
    for f in fields_of:
        for r in range(f.grid[0]):
            for c in range(f.grid[1]):
                f(r, c)


class Strips:
    def __init__(self, levels, cols):
        _, lane = iotas()
        self.levels, self.lane = levels, lane
        self.head, self.tail = slice(0, LANE), slice(cols - LANE, cols)
        pos = lane & (GROUP - 1)
        self.pos, self.group = pos, lane >> 4
        self.index = jnp.where(pos < 5, jnp.maximum(pos - 2, 0), jnp.minimum(pos + LANE - 11, LANE - 1))
        self.back = [
            jnp.where(lane < LANE // 2, l * GROUP + 2, l * GROUP + 11 - LANE + lane) & (LANE - 1)
            for l in range(levels)
        ]

    def own(self, f, rs):
        return pick(jnp.where(self.lane < LANE // 2, f(rs, self.head), f(rs, self.tail)), self.index)

    def own_levels(self, src, rs):
        got = [[self.own(f, rs) for f in level_views(l, src)] for l in range(self.levels)]
        out = got[0]
        for l in range(1, self.levels):
            out = [jnp.where(self.group == l, x, y) for x, y in zip(got[l], out)]
        return out

    def insert(self, x, right, left):
        pos = self.pos
        return jnp.where((pos == 11) | (pos == 12), right, jnp.where(pos == 1, left, x))

    def with_level(self, k, x, right, left):
        return self.insert(x, roll(right, 11 - SLOT[k], 1), roll(left, 2 - SLOT[k], 1))

    def with_geo(self, k, x, right, left):
        at = geo_slot(k)
        rt = pick(right, jnp.where(self.pos == 12, at + 1, at))
        lt = pick(left, jnp.full((SUB, LANE), at - 1, jnp.int32))
        return self.insert(x, rt, lt)

    def masks(self):
        lane = self.lane
        first, end, ends = lane == 0, lane == LANE - 1, lane >= LANE - 2
        return [(None, end), (None, end), (first, None), (first, end)] + [(first, ends)] * 3


def strip_chain(grid, x, raw, area, swap=lambda i, f: f):
    ws = [Field(grid, lambda r, c, k=k: 0.25 * raw[k](r, c) * raw[3 + k](r, c)) for k in range(3)]

    def weighed(v):
        a = [raw[6 + 3 * v + k] for k in range(3)]
        return Field(grid, lambda r, c: raw[12 + v](r, c) * (a[0](r, c) + a[1](r, c) + a[2](r, c)))

    cc, dd, outputs, stages = chain(
        grid, x[0:3], x[3], x[4:7], x[7], raw[0:3], ws, raw[6:12], [weighed(v) for v in range(2)], swap
    )
    scale = [Field(grid, lambda r, c, k=k: SLOPE / raw[k](r, c)) for k in range(3)]
    scale.append(Field(grid, lambda r, c: 1.0 / area(r, c)))
    return cc, dd, outputs(scale), stages


def planes(vert, kin, cell, edge):
    return [(vert, (0,)), (vert, (1,)), (kin, ()), (cell, ())] + [(edge, (k,)) for k in range(3)]


def main_kernel(counts, *refs):
    hbm = refs[:9]
    o_vert, o_kin, o_cell, o_edge = refs[9:13]
    bands = refs[13:22]
    g_right, g_left, saved, ssaved = refs[22:26]
    bufs = refs[26:35]
    p_right, p_left, geo, slev, sgeo, tally = refs[35:41]
    in_sem, own_sem, send_row, recv_row, send_col, recv_col = refs[41:47]
    ny, nx = counts
    py, px = lax.axis_index("py"), lax.axis_index("px")
    down, up = lax.rem(py + 1, ny), lax.rem(py + ny - 1, ny)
    right, left = lax.rem(px + 1, nx), lax.rem(px + nx - 1, nx)

    barrier = pltpu.get_barrier_semaphore()
    near = [
        (up, px), (down, px), (py, left), (py, right),
        (up, left), (up, right), (down, left), (down, right),
    ]
    for y, x in near:
        pl.semaphore_signal(barrier, inc=1, device_id={"py": y, "px": x}, device_id_type=MESH)

    b_area = bufs[8]
    levels, rows, cols = bufs[1].shape
    nr, nc = rows // SUB, cols // LANE
    sub, lane = iotas()

    def await_rows(sem, n):
        pltpu.make_async_copy(tally.at[0:n], tally.at[0:n], sem).wait()

    def part(ref, a, b, *lead):
        rest = (slice(None),) * (len(ref.shape) - 2 - len(lead))
        return ref.at[lead + rest + (slice(a, b), slice(None))]

    def count(ref):
        n = 1
        for d in ref.shape[:-1]:
            n *= d
        return n

    own = []
    for a, b in zip(hbm, bands):
        own.append(pltpu.make_async_copy(part(a, rows - 2, rows), part(b, 0, 2), own_sem.at[0]))
        own.append(pltpu.make_async_copy(part(a, 0, 2), part(b, 6, 8), own_sem.at[0]))
    for copy in own:
        copy.start()
    own_rows = sum(4 * count(b) // SUB for b in bands)
    late = (4, 5, 6, 7, 8, 0, 1, 2, 3)
    for i in late:
        pltpu.make_async_copy(hbm[i], bufs[i], in_sem.at[0 if i >= 4 else 1]).start()

    def remote(src, dst, send, recv, y, x):
        return pltpu.make_async_remote_copy(
            src_ref=src,
            dst_ref=dst,
            send_sem=send,
            recv_sem=recv,
            device_id={"py": y, "px": x},
            device_id_type=MESH,
        )

    vel, th, vt, tt, cd, el, kite, cor = bands[:8]
    to_up = [
        (2, vel, slice(1, 3)), (1, vel, 0), (2, th), (2, vt, slice(1, 3)), (1, vt, 0), (2, tt),
        (2, cd, slice(1, 3)), (1, cd, 0), (1, el, 2), (2, kite, 1), (1, kite, 0), (2, cor, 1), (1, cor, 0),
    ]
    to_down = [
        (2, vel, slice(0, 2)), (1, vel, 2), (2, th), (2, vt, slice(0, 2)), (1, vt, 2), (2, tt),
        (2, cd, slice(0, 2)), (1, cd, 2), (1, el, 0), (2, kite, 0), (1, kite, 1), (2, cor, 0), (1, cor, 1),
    ]
    sems = (send_row.at[0], recv_row.at[0])
    row_copies, sent = [], 0
    for n, b, *lead in to_up:
        src = part(b, 6, 6 + n, *lead)
        row_copies.append(remote(src, part(b, 2, 2 + n, *lead), *sems, up, px))
        sent += count(src)
    for n, b, *lead in to_down:
        src = part(b, 2 - n, 2, *lead)
        row_copies.append(remote(src, part(b, 6 - n, 6, *lead), *sems, down, px))
        sent += count(src)
    await_rows(own_sem.at[0], own_rows)
    pl.semaphore_wait(barrier, len(near))
    for copy in row_copies:
        copy.start()

    strips = Strips(levels, cols)
    head, tail = strips.head, strips.tail
    tiles = [slice(r * SUB, (r + 1) * SUB) for r in range(nr + 1)]

    await_rows(in_sem.at[0], sum(count(b) for b in bufs[4:]))
    own_geo = geo_views(bufs[4:8])
    items = [(geo_slot(k), k == 0, f) for k, f in enumerate(own_geo)]
    for l in range(levels):
        for k, f in enumerate(level_views(l, bufs[:4])):
            items.append((l * GROUP + SLOT[k], k in TWO, f))
    await_rows(in_sem.at[1], sum(count(b) for b in bufs[:4]))
    for rs in tiles[:nr]:
        ra = la = jnp.zeros((SUB, LANE), F32)
        for s, two, f in items:
            m = jnp.where(lane < LANE // 2, f(rs, head), f(rs, tail))
            m = roll(m, s, 1)
            ra = jnp.where((lane == s) | (lane == s + 1) if two else lane == s, m, ra)
            la = jnp.where(lane == (s + LANE - 1) % LANE, m, la)
        p_right[rs] = ra
        p_left[rs] = la

    def column(src, dst, i, y, x):
        return remote(src, dst, send_col.at[i], recv_col.at[i], y, x)

    col_copies = [
        column(p_right, g_right.at[0:rows], 0, py, left),
        column(p_left, g_left.at[0:rows], 1, py, right),
        column(p_right.at[rows - 2 : rows], g_right.at[rows + 4 : rows + 6], 2, down, left),
        column(p_right.at[0:2], g_right.at[rows + 2 : rows + 4], 3, up, left),
        column(p_left.at[0:2], g_left.at[rows + 2 : rows + 4], 4, up, right),
    ]
    for copy in col_copies:
        copy.start()

    for r in range(nr):
        for c in range(nc):
            put_geo(geo, span(r, c), [f(*span(r, c)) for f in own_geo], b_area[span(r, c)])

    for rs in tiles[:nr]:
        for k, x in enumerate(strips.own_levels(bufs[:4], rs)):
            slev[k, rs] = x
        for k, f in enumerate(own_geo + [view(b_area)]):
            sgeo[k, rs] = strips.own(f, rs)

    outputs_of = planes(o_vert, o_kin, o_cell, o_edge)

    def block(l):
        cc, dd, outs, _ = run(
            (nr, nc),
            fields((nr, nc), level_views(l, bufs[:4])),
            own_geo[6:12],
            own_geo[0:3],
            [view(geo, k) for k in range(9)],
        )
        for c in range(nc):
            for i, f in enumerate((cc, dd)):
                saved[i, l, :, span(0, c)[1]] = jnp.where(
                    sub < 4, roll(f(nr - 1, c), 2, 0), roll(f(0, c), -2, 0)
                )
        for r in range(nr):
            for c in range(nc):
                for (ref, lead), f in zip(outputs_of, outs):
                    ref[lead + (l,) + span(r, c)] = f(r, c)

    def inner(i, carry):
        for u in range(PAIR):
            block(i * PAIR + u)
        return carry

    lax.fori_loop(0, levels // PAIR, inner, 0)

    for copy in col_copies[:2]:
        copy.wait()
    grid = (nr, 1)
    x = [
        Field(
            grid,
            lambda r, c, k=k: strips.with_level(
                k, slev[k, tiles[r]], g_right[tiles[r]], g_left[tiles[r]]
            ),
        )
        for k in range(8)
    ]
    raw = [
        Field(
            grid,
            lambda r, c, k=k: strips.with_geo(
                k, sgeo[k, tiles[r]], g_right[tiles[r]], g_left[tiles[r]]
            ),
        )
        for k in range(14)
    ]
    cc, dd, outs, stages = strip_chain(grid, x, raw, lambda r, c: sgeo[14, tiles[r]])
    for stage in [x + raw] + stages + [outs]:
        build(stage)
    for i, f in enumerate((cc, dd)):
        ssaved[i] = jnp.where(sub < 4, roll(f(nr - 1, 0), 2, 0), roll(f(0, 0), -2, 0))
    for l in range(levels):
        for r in range(nr):
            moved = [pick(f(r, 0), strips.back[l]) for f in outs]
            for (ref, lead), z, (mf, me) in zip(outputs_of, moved, strips.masks()):
                if mf is not None:
                    pltpu.store(ref.at[lead + (l, tiles[r], head)], z, mask=mf)
                if me is not None:
                    pltpu.store(ref.at[lead + (l, tiles[r], tail)], z, mask=me)

    for copy in col_copies[2:]:
        copy.wait()
    await_rows(send_row.at[0], sent)
    await_rows(recv_row.at[0], sent)


def finish_kernel(*refs):
    kept = refs[0:4]
    bands = refs[4:13]
    g_right, g_left, saved, ssaved = refs[13:17]
    final = refs[17:21]
    ends = refs[21:25]
    kgeo, sem = refs[25:27]
    levels, rows, cols = kept[1].shape
    nr, nc = rows // SUB, cols // LANE
    sub, lane = iotas()

    def send(src, dst, which):
        pltpu.make_async_copy(src, dst, sem.at[which]).start()

    def part(ref, a, b, *lead):
        rest = (slice(None),) * (len(ref.shape) - 2 - len(lead))
        return ref.at[lead + rest + (slice(a, b), slice(None))]

    changed = [(0, 1), (1, 0), (1, 1), (1, 1), (1, 2), (1, 1), (2, 1)]
    array_of = (0, 0, 1, 2, 3, 3, 3)
    src_of, end_of, dst_of = planes(*kept), planes(*ends), planes(*final)
    if nr > 2:
        for i, (a, b) in enumerate(zip(kept, final)):
            send(part(a, SUB, rows - SUB), part(b, SUB, rows - SUB), i)
    for (src, lead), (dst, _), (n_top, n_low), which in zip(src_of, dst_of, changed, array_of):
        for a, b in ((n_top, SUB), (rows - SUB, rows - n_low)):
            send(part(src, a, b, *lead), part(dst, a, b, *lead), which)

    strips = Strips(levels, cols)
    low, top = slice(0, SUB), slice(rows, rows + SUB)
    first_rows, last_rows = slice(0, SUB), slice(rows - SUB, rows)

    def border(g):
        a, b = roll(g[last_rows], 2, 0), roll(g[first_rows], -2, 0)
        return jnp.where(sub < 2, a, jnp.where(sub >= 6, b, g[top]))

    band_geo = geo_views(bands[4:8])
    one = (1, 1)
    const = lambda t: Field(one, lambda r, c: t)
    sides = border(g_right), border(g_left)
    own_levels = strips.own_levels(bands[:4], low)
    own_geo = [strips.own(f, low) for f in band_geo]
    area = strips.own(view(bands[8]), low)
    x = [const(strips.with_level(k, own_levels[k], *sides)) for k in range(8)]
    raw = [const(strips.with_geo(k, own_geo[k], *sides)) for k in range(14)]
    for c in range(nc):
        at = span(0, c)
        put_geo(kgeo, at, [f(*at) for f in band_geo], bands[8][at])

    merge = (sub == 0) | (sub == SUB - 1)

    def swap_with(grid, load):
        return lambda i, f: Field(grid, lambda r, c: jnp.where(merge, load(i, c), f(r, c)))

    _, _, souts, sstages = strip_chain(
        one, x, raw, lambda r, c: area, swap_with(one, lambda i, c: ssaved[i])
    )
    grid = (1, nc)
    jobs = []
    for l in range(levels):
        jobs.append(
            run(
                grid,
                fields(grid, level_views(l, bands[:4])),
                band_geo[6:12],
                band_geo[0:3],
                [view(kgeo, k) for k in range(9)],
                swap_with(grid, lambda i, c, l=l: saved[i, l, :, span(0, c)[1]]),
            )[2:]
        )

    masks = strips.masks()

    def finalize(i):
        end, lead = end_of[i]
        dst = dst_of[i][0]
        n_top, n_low = changed[i]
        y = souts[i](0, 0)
        zs = [pick(y, strips.back[l]) for l in range(levels)]
        for l in range(levels):
            for c in range(nc):
                t = jobs[l][0][i](0, c)
                for m, at in zip(masks[i], (0, nc - 1)):
                    if m is not None and at == c:
                        t = jnp.where(m, zs[l], t)
                end[lead + (l,) + span(0, c)] = t
        if n_top:
            send(part(end, 6, 6 + n_top, *lead), part(dst, 0, n_top, *lead), array_of[i])
        if n_low:
            send(part(end, 2 - n_low, 2, *lead), part(dst, rows - n_low, rows, *lead), array_of[i])

    ready = [(), (0, 1, 2), (3,), (4, 5, 6)]
    for stage, done in enumerate(ready):
        for _, stages in jobs:
            build(stages[stage])
        build(sstages[stage])
        for i in done:
            finalize(i)
    for i, (a, b) in enumerate(zip(kept, final)):
        pltpu.make_async_copy(a, b, sem.at[i]).wait()


def local(counts, vel, th, vt, tt, cd, el, area, kite, cor):
    args = (vel, th, vt, tt, cd, el, kite, cor, area)
    levels, rows, cols = th.shape
    outs = [(2, levels, rows, cols), (levels, rows, cols), (levels, rows, cols), (3, levels, rows, cols)]
    short = lambda s, n: s[:-2] + (n, cols)
    hbm, vmem = pl.BlockSpec(memory_space=pl.ANY), pl.BlockSpec(memory_space=pltpu.VMEM)
    side = (rows + SUB, LANE)
    passed = outs + [short(a.shape, SUB) for a in args]
    passed += [side, side, (2, levels, SUB, cols), (2, SUB, LANE)]
    kept = pl.pallas_call(
        lambda *refs: main_kernel(counts, *refs),
        out_shape=[pltpu.VMEM(s, F32) for s in passed],
        in_specs=[hbm] * len(args),
        out_specs=[vmem] * len(passed),
        scratch_shapes=[pltpu.VMEM(a.shape, F32) for a in args]
        + [
            pltpu.VMEM((rows, LANE), F32),
            pltpu.VMEM((rows, LANE), F32),
            pltpu.VMEM((9, rows, cols), F32),
            pltpu.VMEM((8, rows, LANE), F32),
            pltpu.VMEM((15, rows, LANE), F32),
            pltpu.VMEM((8 * levels * rows, 1, cols), F32),
        ]
        + [pltpu.SemaphoreType.DMA((n,)) for n in (2, 1, 1, 1, 5, 5)],
        compiler_params=pltpu.CompilerParams(collective_id=0, has_side_effects=True),
        name="main",
    )(*args)
    return pl.pallas_call(
        finish_kernel,
        out_shape=[jax.ShapeDtypeStruct(s, F32) for s in outs],
        in_specs=[vmem] * len(passed),
        out_specs=[pl.BlockSpec(memory_space=pltpu.HBM)] * len(outs),
        scratch_shapes=[pltpu.VMEM(short(s, SUB), F32) for s in outs]
        + [pltpu.VMEM((9, SUB, cols), F32), pltpu.SemaphoreType.DMA((4,))],
        name="finish",
    )(*[pltpu.with_memory_space_constraint(x, pltpu.VMEM) for x in kept])


def solution(mesh):
    counts = (mesh.shape["py"], mesh.shape["px"])
    p4, p3 = P(None, None, "py", "px"), P(None, "py", "px")
    return jax.shard_map(
        lambda *args: local(counts, *args),
        mesh=mesh,
        in_specs=(p4, p3, p4, p3, p3, p3, P("py", "px"), p4, p3),
        out_specs=(p4, p3, p3, p4),
        check_vma=False,
    )
```

```python
import jax
import jax.numpy as jnp
from jax import lax
from jax.experimental import pallas as pl
from jax.experimental.pallas import tpu as pltpu
from jax.sharding import PartitionSpec as P

SUB = 8
LANE = 128
GROUP = 16
PAIR = 2
PARTS = 2
SLOT = (0, 8, 9, 2, 4, 10, 11, 6)
TWO = (0, 3, 4, 7)
MESH = pl.DeviceIdType.MESH
F32 = jnp.float32
SLOPE = -0.5 / 36.0


def iotas():
    sub = lax.broadcasted_iota(jnp.int32, (SUB, LANE), 0)
    lane = lax.broadcasted_iota(jnp.int32, (SUB, LANE), 1)
    return sub, lane


def roll(x, shift, axis):
    n = (SUB, LANE)[axis]
    return pltpu.roll(x, shift % n, axis) if shift % n else x


def pick(x, index):
    return jnp.take_along_axis(x, index, axis=1)


def span(r, c):
    return (slice(r * SUB, (r + 1) * SUB), slice(c * LANE, (c + 1) * LANE))


class Field:
    def __init__(self, grid, make):
        self.grid, self.make, self.memo = grid, make, {}

    def __call__(self, r, c):
        key = (r % self.grid[0], c % self.grid[1])
        if key not in self.memo:
            self.memo[key] = self.make(*key)
        return self.memo[key]


def chain(grid, v, h, t, g, dist, ew, kt, ct, swap=lambda i, f: f):
    sub, lane = iotas()

    def lift(fn, *fields):
        return Field(grid, lambda r, c: fn(*[f(r, c) for f in fields]))

    def row_shift(f, a):
        rolled = Field(grid, lambda r, c: roll(f(r, c), -a, 0))
        if grid[0] == 1:
            return rolled
        keep = sub < SUB - 1 if a == 1 else sub > 0
        return Field(grid, lambda r, c: jnp.where(keep, rolled(r, c), rolled(r + a, c)))

    def col_shift(f, b):
        rolled = Field(grid, lambda r, c: roll(f(r, c), -b, 1))
        if grid[1] == 1:
            return rolled
        keep = lane < LANE - 1 if b == 1 else lane > 0
        return Field(grid, lambda r, c: jnp.where(keep, rolled(r, c), rolled(r, c + b)))

    def parts(vv, hh):
        flux = [lift(lambda a, b: a * b, vv[k], dist[k]) for k in range(3)]
        c0 = lift(lambda a, b, c: a + b - c, flux[0], row_shift(flux[2], 1), flux[1])
        c1 = lift(lambda a, b, c: a - b - c, flux[1], flux[2], col_shift(row_shift(flux[0], -1), 1))
        hc = col_shift(hh, 1)
        hr = row_shift(hh, 1)
        hd = row_shift(hc, -1)
        mix = lambda a, b, c, p, q, s: a * p + b * q + c * s
        h0 = lift(mix, kt[0], kt[1], kt[2], hh, hr, hc)
        h1 = lift(mix, kt[3], kt[4], kt[5], hh, hc, hd)
        return (c0, c1), (h0, h1)

    cv, hv = parts(v, h)
    cw, hw = parts(t, g)

    def potential(k):
        def make(r, c):
            a0 = ct[k](r, c) + cv[k](r, c)
            a1 = cw[k](r, c)
            b0 = hv[k](r, c)
            b1 = hw[k](r, c)
            bm, be = b0 + 0.5 * b1, b0 + b1
            m = bm * be
            scale_all = 1.0 / (b0 * m)
            mid = (a0 + a0 + a1) * (b0 * be)
            late = mid + (a0 + a1) * (b0 * bm)
            return (a0 * m + mid + late) * scale_all, late * scale_all

        both = Field(grid, make)
        return Field(grid, lambda r, c: both(r, c)[0]), Field(grid, lambda r, c: both(r, c)[1])

    p0, q0 = potential(0)
    p1, q1 = potential(1)
    add = lambda a, b: a + b
    add3 = lambda a, b, c: a + b + c

    def cell(f0, f1):
        f0_up = row_shift(f0, -1)
        f1_down = row_shift(f1, 1)
        pair = lift(add, f0, f1)
        return lift(add3, pair, f0_up, col_shift(lift(add, pair, f1_down), -1)), f0_up, f1_down, pair

    cc, p0_up, p1_down, pair = cell(p0, p1)
    dd = cell(q0, q1)[0]
    cc, dd = swap(0, cc), swap(1, dd)
    p1_low = col_shift(p1_down, -1)

    def neighbours(f):
        fc = col_shift(f, 1)
        return row_shift(f, 1), fc, row_shift(fc, -1)

    cn, dn = neighbours(cc), neighbours(dd)
    ends = [lift(add, p0, p1_low), pair, lift(add, p1, p0_up)]
    en = [
        lift(lambda w, a, b: w * (a * (a + b) + (1.0 / 3.0) * (b * b)), ew[k], v[k], t[k])
        for k in range(3)
    ]
    e_up = row_shift(en[0], -1)
    e_low = col_shift(lift(add, en[1], row_shift(en[2], 1)), -1)

    def outputs(scale):
        def edge(k):
            def make(r, c):
                slope = v[k](r, c) * (cn[k](r, c) - cc(r, c)) + t[k](r, c) * (dn[k](r, c) - dd(r, c))
                return ends[k](r, c) * (1.0 / 12.0) + scale[k](r, c) * slope

            return Field(grid, make)

        kin = Field(
            grid,
            lambda r, c: (en[0](r, c) + en[1](r, c) + en[2](r, c) + e_up(r, c) + e_low(r, c)) * scale[3](r, c),
        )
        return [
            lift(lambda a: a * (1.0 / 6.0), p0),
            lift(lambda a: a * (1.0 / 6.0), p1),
            kin,
            lift(lambda a: a * (1.0 / 36.0), cc),
        ] + [edge(k) for k in range(3)]

    stages = [[*cv, *hv, *cw, *hw, e_low], [p0, q0, p1, q1], [cc, dd, p1_low], [*cn, *dn]]
    return cc, dd, outputs, stages


def view(ref, *lead):
    return lambda r, c: ref[lead + (r, c)]


def level_views(l, src):
    vel, th, vt, tt = src
    return (
        [view(vel, k, l) for k in range(3)]
        + [view(th, l)]
        + [view(vt, k, l) for k in range(3)]
        + [view(tt, l)]
    )


def geo_views(src):
    cd, el, kite, cor = src
    return (
        [view(cd, k) for k in range(3)]
        + [view(el, k) for k in range(3)]
        + [view(kite, v, k) for v in range(2) for k in range(3)]
        + [view(cor, v) for v in range(2)]
    )


def geo_slot(k):
    return 12 if k == 0 else (1 + (k - 1) % 7) * GROUP + 12 + (k - 1) // 7


def put_geo(dst, at, f, area):
    for k in range(3):
        dst[(k,) + at] = 0.25 * f[k] * f[3 + k]
        dst[(5 + k,) + at] = SLOPE / f[k]
    for v in range(2):
        dst[(3 + v,) + at] = f[12 + v] * (f[6 + 3 * v] + f[7 + 3 * v] + f[8 + 3 * v])
    dst[(8,) + at] = 1.0 / area


def fields(grid, views):
    return [Field(grid, lambda r, c, f=f: f(*span(r, c))) for f in views]


def run(grid, x, kites, dist, derived, swap=lambda i, f: f):
    f = fields(grid, derived)
    d = fields(grid, dist)
    cc, dd, outputs, stages = chain(
        grid, x[0:3], x[3], x[4:7], x[7], d, f[0:3], fields(grid, kites), f[3:5], swap
    )
    return cc, dd, outputs(f[5:9]), stages


def build(fields_of):
    for f in fields_of:
        for r in range(f.grid[0]):
            for c in range(f.grid[1]):
                f(r, c)


class Strips:
    def __init__(self, levels, cols):
        _, lane = iotas()
        self.levels, self.lane = levels, lane
        self.head, self.tail = slice(0, LANE), slice(cols - LANE, cols)
        pos = lane & (GROUP - 1)
        self.pos, self.group = pos, lane >> 4
        self.index = jnp.where(pos < 5, jnp.maximum(pos - 2, 0), jnp.minimum(pos + LANE - 11, LANE - 1))
        self.back = [
            jnp.where(lane < LANE // 2, l * GROUP + 2, l * GROUP + 11 - LANE + lane) & (LANE - 1)
            for l in range(levels)
        ]

    def own(self, f, rs):
        return pick(jnp.where(self.lane < LANE // 2, f(rs, self.head), f(rs, self.tail)), self.index)

    def own_levels(self, src, rs):
        got = [[self.own(f, rs) for f in level_views(l, src)] for l in range(self.levels)]
        out = got[0]
        for l in range(1, self.levels):
            out = [jnp.where(self.group == l, x, y) for x, y in zip(got[l], out)]
        return out

    def insert(self, x, right, left):
        pos = self.pos
        return jnp.where((pos == 11) | (pos == 12), right, jnp.where(pos == 1, left, x))

    def with_level(self, k, x, right, left):
        return self.insert(x, roll(right, 11 - SLOT[k], 1), roll(left, 2 - SLOT[k], 1))

    def with_geo(self, k, x, right, left):
        at = geo_slot(k)
        rt = pick(right, jnp.where(self.pos == 12, at + 1, at))
        lt = pick(left, jnp.full((SUB, LANE), at - 1, jnp.int32))
        return self.insert(x, rt, lt)

    def masks(self):
        lane = self.lane
        first, end, ends = lane == 0, lane == LANE - 1, lane >= LANE - 2
        return [(None, end), (None, end), (first, None), (first, end)] + [(first, ends)] * 3


def strip_chain(grid, x, raw, area, swap=lambda i, f: f):
    ws = [Field(grid, lambda r, c, k=k: 0.25 * raw[k](r, c) * raw[3 + k](r, c)) for k in range(3)]

    def weighed(v):
        a = [raw[6 + 3 * v + k] for k in range(3)]
        return Field(grid, lambda r, c: raw[12 + v](r, c) * (a[0](r, c) + a[1](r, c) + a[2](r, c)))

    cc, dd, outputs, stages = chain(
        grid, x[0:3], x[3], x[4:7], x[7], raw[0:3], ws, raw[6:12], [weighed(v) for v in range(2)], swap
    )
    scale = [Field(grid, lambda r, c, k=k: SLOPE / raw[k](r, c)) for k in range(3)]
    scale.append(Field(grid, lambda r, c: 1.0 / area(r, c)))
    return cc, dd, outputs(scale), stages


def planes(vert, kin, cell, edge):
    return [(vert, (0,)), (vert, (1,)), (kin, ()), (cell, ())] + [(edge, (k,)) for k in range(3)]


def main_kernel(counts, *refs):
    hbm = refs[:9]
    o_vert, o_kin, o_cell, o_edge = refs[9:13]
    bands = refs[13:22]
    g_right, g_left, saved, ssaved = refs[22:26]
    bufs = refs[26:35]
    p_right, p_left, geo, slev, sgeo, tally = refs[35:41]
    in_sem, own_sem, send_row, recv_row, send_col, recv_col = refs[41:47]
    ny, nx = counts
    py, px = lax.axis_index("py"), lax.axis_index("px")
    down, up = lax.rem(py + 1, ny), lax.rem(py + ny - 1, ny)
    right, left = lax.rem(px + 1, nx), lax.rem(px + nx - 1, nx)

    barrier = pltpu.get_barrier_semaphore()
    near = [
        (up, px), (down, px), (py, left), (py, right),
        (up, left), (up, right), (down, left), (down, right),
    ]
    for y, x in near:
        pl.semaphore_signal(barrier, inc=1, device_id={"py": y, "px": x}, device_id_type=MESH)

    b_area = bufs[8]
    levels, rows, cols = bufs[1].shape
    nr, nc = rows // SUB, cols // LANE
    sub, lane = iotas()

    def await_rows(sem, n):
        pltpu.make_async_copy(tally.at[0:n], tally.at[0:n], sem).wait()

    def part(ref, a, b, *lead):
        rest = (slice(None),) * (len(ref.shape) - 2 - len(lead))
        return ref.at[lead + rest + (slice(a, b), slice(None))]

    def count(ref):
        n = 1
        for d in ref.shape[:-1]:
            n *= d
        return n

    for a, b in zip(hbm, bands):
        pltpu.make_async_copy(part(a, rows - 2, rows), part(b, 0, 2), own_sem.at[0]).start()
    for a, b in zip(hbm, bands):
        pltpu.make_async_copy(part(a, 0, 2), part(b, 6, 8), own_sem.at[1]).start()
    own_rows = sum(2 * count(b) // SUB for b in bands)
    for i in (4, 5, 6, 7, 8):
        pltpu.make_async_copy(hbm[i], bufs[i], in_sem.at[0]).start()
    cuts = [slice(i * levels // PARTS, (i + 1) * levels // PARTS) for i in range(PARTS)]
    for j, cut in enumerate(cuts):
        for a, b in zip(hbm[:4], bufs):
            at = (slice(None),) * (len(a.shape) - 3) + (cut,)
            pltpu.make_async_copy(a.at[at], b.at[at], in_sem.at[1 + j]).start()

    def remote(src, dst, send, recv, y, x):
        return pltpu.make_async_remote_copy(
            src_ref=src,
            dst_ref=dst,
            send_sem=send,
            recv_sem=recv,
            device_id={"py": y, "px": x},
            device_id_type=MESH,
        )

    vel, th, vt, tt, cd, el, kite, cor = bands[:8]
    to_up = [
        (2, vel, slice(1, 3)), (1, vel, 0), (2, th), (2, vt, slice(1, 3)), (1, vt, 0), (2, tt),
        (2, cd, slice(1, 3)), (1, cd, 0), (1, el, 2), (2, kite, 1), (1, kite, 0), (2, cor, 1), (1, cor, 0),
    ]
    to_down = [
        (2, vel, slice(0, 2)), (1, vel, 2), (2, th), (2, vt, slice(0, 2)), (1, vt, 2), (2, tt),
        (2, cd, slice(0, 2)), (1, cd, 2), (1, el, 0), (2, kite, 0), (1, kite, 1), (2, cor, 0), (1, cor, 1),
    ]
    sems = (send_row.at[0], recv_row.at[0])
    up_copies, down_copies, sent = [], [], 0
    for n, b, *lead in to_up:
        src = part(b, 6, 6 + n, *lead)
        up_copies.append(remote(src, part(b, 2, 2 + n, *lead), *sems, up, px))
        sent += count(src)
    for n, b, *lead in to_down:
        src = part(b, 2 - n, 2, *lead)
        down_copies.append(remote(src, part(b, 6 - n, 6, *lead), *sems, down, px))
        sent += count(src)
    await_rows(own_sem.at[0], own_rows)
    pl.semaphore_wait(barrier, len(near))
    for copy in down_copies:
        copy.start()

    strips = Strips(levels, cols)
    head, tail = strips.head, strips.tail
    tiles = [slice(r * SUB, (r + 1) * SUB) for r in range(nr + 1)]

    await_rows(in_sem.at[0], sum(count(b) for b in bufs[4:]))
    own_geo = geo_views(bufs[4:8])
    packed = [[jnp.zeros((SUB, LANE), F32)] * 2 for _ in range(nr)]

    def pack(items):
        for r in range(nr):
            rs, (ra, la) = tiles[r], packed[r]
            for s, two, f in items:
                m = jnp.where(lane < LANE // 2, f(rs, head), f(rs, tail))
                m = roll(m, s, 1)
                ra = jnp.where((lane == s) | (lane == s + 1) if two else lane == s, m, ra)
                la = jnp.where(lane == (s + LANE - 1) % LANE, m, la)
            packed[r] = [ra, la]

    pack([(geo_slot(k), k == 0, f) for k, f in enumerate(own_geo)])
    for j, cut in enumerate(cuts):
        await_rows(in_sem.at[1 + j], sum(count(b) for b in bufs[:4]) // PARTS)
        items = []
        for l in range(cut.start, cut.stop):
            for k, f in enumerate(level_views(l, bufs[:4])):
                items.append((l * GROUP + SLOT[k], k in TWO, f))
        pack(items)
    for r in range(nr):
        p_right[tiles[r]], p_left[tiles[r]] = packed[r]

    def column(src, dst, i, y, x):
        return remote(src, dst, send_col.at[i], recv_col.at[i], y, x)

    col_copies = [
        column(p_right, g_right.at[0:rows], 0, py, left),
        column(p_left, g_left.at[0:rows], 1, py, right),
        column(p_right.at[rows - 2 : rows], g_right.at[rows + 4 : rows + 6], 2, down, left),
        column(p_right.at[0:2], g_right.at[rows + 2 : rows + 4], 3, up, left),
        column(p_left.at[0:2], g_left.at[rows + 2 : rows + 4], 4, up, right),
    ]
    for copy in col_copies:
        copy.start()
    await_rows(own_sem.at[1], own_rows)
    for copy in up_copies:
        copy.start()

    for r in range(nr):
        for c in range(nc):
            put_geo(geo, span(r, c), [f(*span(r, c)) for f in own_geo], b_area[span(r, c)])

    for rs in tiles[:nr]:
        for k, x in enumerate(strips.own_levels(bufs[:4], rs)):
            slev[k, rs] = x
        for k, f in enumerate(own_geo + [view(b_area)]):
            sgeo[k, rs] = strips.own(f, rs)

    outputs_of = planes(o_vert, o_kin, o_cell, o_edge)

    def block(l):
        cc, dd, outs, _ = run(
            (nr, nc),
            fields((nr, nc), level_views(l, bufs[:4])),
            own_geo[6:12],
            own_geo[0:3],
            [view(geo, k) for k in range(9)],
        )
        for c in range(nc):
            for i, f in enumerate((cc, dd)):
                saved[i, l, :, span(0, c)[1]] = jnp.where(
                    sub < 4, roll(f(nr - 1, c), 2, 0), roll(f(0, c), -2, 0)
                )
        for r in range(nr):
            for c in range(nc):
                for (ref, lead), f in zip(outputs_of, outs):
                    ref[lead + (l,) + span(r, c)] = f(r, c)

    def inner(i, carry):
        for u in range(PAIR):
            block(i * PAIR + u)
        return carry

    lax.fori_loop(0, levels // PAIR, inner, 0)

    for copy in col_copies[:2]:
        copy.wait()
    grid = (nr, 1)
    x = [
        Field(
            grid,
            lambda r, c, k=k: strips.with_level(
                k, slev[k, tiles[r]], g_right[tiles[r]], g_left[tiles[r]]
            ),
        )
        for k in range(8)
    ]
    raw = [
        Field(
            grid,
            lambda r, c, k=k: strips.with_geo(
                k, sgeo[k, tiles[r]], g_right[tiles[r]], g_left[tiles[r]]
            ),
        )
        for k in range(14)
    ]
    cc, dd, outs, stages = strip_chain(grid, x, raw, lambda r, c: sgeo[14, tiles[r]])
    for stage in [x + raw] + stages + [outs]:
        build(stage)
    for i, f in enumerate((cc, dd)):
        ssaved[i] = jnp.where(sub < 4, roll(f(nr - 1, 0), 2, 0), roll(f(0, 0), -2, 0))
    for l in range(levels):
        for r in range(nr):
            moved = [pick(f(r, 0), strips.back[l]) for f in outs]
            for (ref, lead), z, (mf, me) in zip(outputs_of, moved, strips.masks()):
                if mf is not None:
                    pltpu.store(ref.at[lead + (l, tiles[r], head)], z, mask=mf)
                if me is not None:
                    pltpu.store(ref.at[lead + (l, tiles[r], tail)], z, mask=me)

    for copy in col_copies[2:]:
        copy.wait()
    await_rows(send_row.at[0], sent)
    await_rows(recv_row.at[0], sent)


def finish_kernel(*refs):
    kept = refs[0:4]
    bands = refs[4:13]
    g_right, g_left, saved, ssaved = refs[13:17]
    final = refs[17:21]
    ends = refs[21:25]
    kgeo, sem = refs[25:27]
    levels, rows, cols = kept[1].shape
    nr, nc = rows // SUB, cols // LANE
    sub, lane = iotas()

    def send(src, dst, which):
        pltpu.make_async_copy(src, dst, sem.at[which]).start()

    def part(ref, a, b, *lead):
        rest = (slice(None),) * (len(ref.shape) - 2 - len(lead))
        return ref.at[lead + rest + (slice(a, b), slice(None))]

    changed = [(0, 1), (1, 0), (1, 1), (1, 1), (1, 2), (1, 1), (2, 1)]
    array_of = (0, 0, 1, 2, 3, 3, 3)
    src_of, end_of, dst_of = planes(*kept), planes(*ends), planes(*final)
    if nr > 2:
        for i, (a, b) in enumerate(zip(kept, final)):
            send(part(a, SUB, rows - SUB), part(b, SUB, rows - SUB), i)
    for (src, lead), (dst, _), (n_top, n_low), which in zip(src_of, dst_of, changed, array_of):
        for a, b in ((n_top, SUB), (rows - SUB, rows - n_low)):
            send(part(src, a, b, *lead), part(dst, a, b, *lead), which)

    strips = Strips(levels, cols)
    low, top = slice(0, SUB), slice(rows, rows + SUB)
    first_rows, last_rows = slice(0, SUB), slice(rows - SUB, rows)

    def border(g):
        a, b = roll(g[last_rows], 2, 0), roll(g[first_rows], -2, 0)
        return jnp.where(sub < 2, a, jnp.where(sub >= 6, b, g[top]))

    band_geo = geo_views(bands[4:8])
    one = (1, 1)
    const = lambda t: Field(one, lambda r, c: t)
    sides = border(g_right), border(g_left)
    own_levels = strips.own_levels(bands[:4], low)
    own_geo = [strips.own(f, low) for f in band_geo]
    area = strips.own(view(bands[8]), low)
    x = [const(strips.with_level(k, own_levels[k], *sides)) for k in range(8)]
    raw = [const(strips.with_geo(k, own_geo[k], *sides)) for k in range(14)]
    for c in range(nc):
        at = span(0, c)
        put_geo(kgeo, at, [f(*at) for f in band_geo], bands[8][at])

    merge = (sub == 0) | (sub == SUB - 1)

    def swap_with(grid, load):
        return lambda i, f: Field(grid, lambda r, c: jnp.where(merge, load(i, c), f(r, c)))

    _, _, souts, sstages = strip_chain(
        one, x, raw, lambda r, c: area, swap_with(one, lambda i, c: ssaved[i])
    )
    grid = (1, nc)
    jobs = []
    for l in range(levels):
        jobs.append(
            run(
                grid,
                fields(grid, level_views(l, bands[:4])),
                band_geo[6:12],
                band_geo[0:3],
                [view(kgeo, k) for k in range(9)],
                swap_with(grid, lambda i, c, l=l: saved[i, l, :, span(0, c)[1]]),
            )[2:]
        )

    masks = strips.masks()

    def finalize(i):
        end, lead = end_of[i]
        dst = dst_of[i][0]
        n_top, n_low = changed[i]
        y = souts[i](0, 0)
        zs = [pick(y, strips.back[l]) for l in range(levels)]
        for l in range(levels):
            for c in range(nc):
                t = jobs[l][0][i](0, c)
                for m, at in zip(masks[i], (0, nc - 1)):
                    if m is not None and at == c:
                        t = jnp.where(m, zs[l], t)
                end[lead + (l,) + span(0, c)] = t
        if n_top:
            send(part(end, 6, 6 + n_top, *lead), part(dst, 0, n_top, *lead), array_of[i])
        if n_low:
            send(part(end, 2 - n_low, 2, *lead), part(dst, rows - n_low, rows, *lead), array_of[i])

    ready = [(), (0, 1, 2), (3,), (4, 5, 6)]
    for stage, done in enumerate(ready):
        for _, stages in jobs:
            build(stages[stage])
        build(sstages[stage])
        for i in done:
            finalize(i)
    for i, (a, b) in enumerate(zip(kept, final)):
        pltpu.make_async_copy(a, b, sem.at[i]).wait()


def local(counts, vel, th, vt, tt, cd, el, area, kite, cor):
    args = (vel, th, vt, tt, cd, el, kite, cor, area)
    levels, rows, cols = th.shape
    outs = [(2, levels, rows, cols), (levels, rows, cols), (levels, rows, cols), (3, levels, rows, cols)]
    short = lambda s, n: s[:-2] + (n, cols)
    hbm, vmem = pl.BlockSpec(memory_space=pl.ANY), pl.BlockSpec(memory_space=pltpu.VMEM)
    side = (rows + SUB, LANE)
    passed = outs + [short(a.shape, SUB) for a in args]
    passed += [side, side, (2, levels, SUB, cols), (2, SUB, LANE)]
    kept = pl.pallas_call(
        lambda *refs: main_kernel(counts, *refs),
        out_shape=[pltpu.VMEM(s, F32) for s in passed],
        in_specs=[hbm] * len(args),
        out_specs=[vmem] * len(passed),
        scratch_shapes=[pltpu.VMEM(a.shape, F32) for a in args]
        + [
            pltpu.VMEM((rows, LANE), F32),
            pltpu.VMEM((rows, LANE), F32),
            pltpu.VMEM((9, rows, cols), F32),
            pltpu.VMEM((8, rows, LANE), F32),
            pltpu.VMEM((15, rows, LANE), F32),
            pltpu.VMEM((8 * levels * rows, 1, cols), F32),
        ]
        + [pltpu.SemaphoreType.DMA((n,)) for n in (1 + PARTS, 2, 1, 1, 5, 5)],
        compiler_params=pltpu.CompilerParams(collective_id=0, has_side_effects=True),
        name="main",
    )(*args)
    return pl.pallas_call(
        finish_kernel,
        out_shape=[jax.ShapeDtypeStruct(s, F32) for s in outs],
        in_specs=[vmem] * len(passed),
        out_specs=[pl.BlockSpec(memory_space=pltpu.HBM)] * len(outs),
        scratch_shapes=[pltpu.VMEM(short(s, SUB), F32) for s in outs]
        + [pltpu.VMEM((9, SUB, cols), F32), pltpu.SemaphoreType.DMA((4,))],
        name="finish",
    )(*[pltpu.with_memory_space_constraint(x, pltpu.VMEM) for x in kept])


def solution(mesh):
    counts = (mesh.shape["py"], mesh.shape["px"])
    p4, p3 = P(None, None, "py", "px"), P(None, "py", "px")
    return jax.shard_map(
        lambda *args: local(counts, *args),
        mesh=mesh,
        in_specs=(p4, p3, p4, p3, p3, p3, P("py", "px"), p4, p3),
        out_specs=(p4, p3, p3, p4),
        check_vma=False,
    )
```

```python
import jax
import jax.numpy as jnp
from jax import lax
from jax.experimental import pallas as pl
from jax.experimental.pallas import tpu as pltpu
from jax.sharding import PartitionSpec as P

SUB = 8
LANE = 128
GROUP = 16
PAIR = 2
PARTS = 2
SLOT = (0, 8, 9, 2, 4, 10, 11, 6)
TWO = (0, 3, 4, 7)
MESH = pl.DeviceIdType.MESH
F32 = jnp.float32
SLOPE = -0.5 / 36.0


def iotas():
    sub = lax.broadcasted_iota(jnp.int32, (SUB, LANE), 0)
    lane = lax.broadcasted_iota(jnp.int32, (SUB, LANE), 1)
    return sub, lane


def roll(x, shift, axis):
    n = (SUB, LANE)[axis]
    return pltpu.roll(x, shift % n, axis) if shift % n else x


def pick(x, index):
    return jnp.take_along_axis(x, index, axis=1)


def span(r, c):
    return (slice(r * SUB, (r + 1) * SUB), slice(c * LANE, (c + 1) * LANE))


class Field:
    def __init__(self, grid, make):
        self.grid, self.make, self.memo = grid, make, {}

    def __call__(self, r, c):
        key = (r % self.grid[0], c % self.grid[1])
        if key not in self.memo:
            self.memo[key] = self.make(*key)
        return self.memo[key]


def chain(grid, v, h, t, g, dist, ew, kt, ct, swap=lambda i, f: f):
    sub, lane = iotas()

    def lift(fn, *fields):
        return Field(grid, lambda r, c: fn(*[f(r, c) for f in fields]))

    def row_shift(f, a):
        rolled = Field(grid, lambda r, c: roll(f(r, c), -a, 0))
        if grid[0] == 1:
            return rolled
        keep = sub < SUB - 1 if a == 1 else sub > 0
        return Field(grid, lambda r, c: jnp.where(keep, rolled(r, c), rolled(r + a, c)))

    def col_shift(f, b):
        rolled = Field(grid, lambda r, c: roll(f(r, c), -b, 1))
        if grid[1] == 1:
            return rolled
        keep = lane < LANE - 1 if b == 1 else lane > 0
        return Field(grid, lambda r, c: jnp.where(keep, rolled(r, c), rolled(r, c + b)))

    def parts(vv, hh):
        flux = [lift(lambda a, b: a * b, vv[k], dist[k]) for k in range(3)]
        c0 = lift(lambda a, b, c: a + b - c, flux[0], row_shift(flux[2], 1), flux[1])
        c1 = lift(lambda a, b, c: a - b - c, flux[1], flux[2], col_shift(row_shift(flux[0], -1), 1))
        hc = col_shift(hh, 1)
        hr = row_shift(hh, 1)
        hd = row_shift(hc, -1)
        mix = lambda a, b, c, p, q, s: a * p + b * q + c * s
        h0 = lift(mix, kt[0], kt[1], kt[2], hh, hr, hc)
        h1 = lift(mix, kt[3], kt[4], kt[5], hh, hc, hd)
        return (c0, c1), (h0, h1)

    cv, hv = parts(v, h)
    cw, hw = parts(t, g)

    def potential(k):
        def make(r, c):
            a0 = ct[k](r, c) + cv[k](r, c)
            a1 = cw[k](r, c)
            b0 = hv[k](r, c)
            b1 = hw[k](r, c)
            bm, be = b0 + 0.5 * b1, b0 + b1
            m = bm * be
            scale_all = 1.0 / (b0 * m)
            mid = (a0 + a0 + a1) * (b0 * be)
            late = mid + (a0 + a1) * (b0 * bm)
            return (a0 * m + mid + late) * scale_all, late * scale_all

        both = Field(grid, make)
        return Field(grid, lambda r, c: both(r, c)[0]), Field(grid, lambda r, c: both(r, c)[1])

    p0, q0 = potential(0)
    p1, q1 = potential(1)
    add = lambda a, b: a + b
    add3 = lambda a, b, c: a + b + c

    def cell(f0, f1):
        f0_up = row_shift(f0, -1)
        f1_down = row_shift(f1, 1)
        pair = lift(add, f0, f1)
        return lift(add3, pair, f0_up, col_shift(lift(add, pair, f1_down), -1)), f0_up, f1_down, pair

    cc, p0_up, p1_down, pair = cell(p0, p1)
    dd = cell(q0, q1)[0]
    cc, dd = swap(0, cc), swap(1, dd)
    p1_low = col_shift(p1_down, -1)

    def neighbours(f):
        fc = col_shift(f, 1)
        return row_shift(f, 1), fc, row_shift(fc, -1)

    cn, dn = neighbours(cc), neighbours(dd)
    ends = [lift(add, p0, p1_low), pair, lift(add, p1, p0_up)]
    en = [
        lift(lambda w, a, b: w * (a * (a + b) + (1.0 / 3.0) * (b * b)), ew[k], v[k], t[k])
        for k in range(3)
    ]
    e_up = row_shift(en[0], -1)
    e_low = col_shift(lift(add, en[1], row_shift(en[2], 1)), -1)

    def outputs(scale):
        def edge(k):
            def make(r, c):
                slope = v[k](r, c) * (cn[k](r, c) - cc(r, c)) + t[k](r, c) * (dn[k](r, c) - dd(r, c))
                return ends[k](r, c) * (1.0 / 12.0) + scale[k](r, c) * slope

            return Field(grid, make)

        kin = Field(
            grid,
            lambda r, c: (en[0](r, c) + en[1](r, c) + en[2](r, c) + e_up(r, c) + e_low(r, c)) * scale[3](r, c),
        )
        return [
            lift(lambda a: a * (1.0 / 6.0), p0),
            lift(lambda a: a * (1.0 / 6.0), p1),
            kin,
            lift(lambda a: a * (1.0 / 36.0), cc),
        ] + [edge(k) for k in range(3)]

    stages = [[*cv, *hv, *cw, *hw, e_low], [p0, q0, p1, q1], [cc, dd, p1_low], [*cn, *dn]]
    return cc, dd, outputs, stages


def view(ref, *lead):
    return lambda r, c: ref[lead + (r, c)]


def level_views(l, src):
    vel, th, vt, tt = src
    return (
        [view(vel, k, l) for k in range(3)]
        + [view(th, l)]
        + [view(vt, k, l) for k in range(3)]
        + [view(tt, l)]
    )


def geo_views(src):
    cd, el, kite, cor = src
    return (
        [view(cd, k) for k in range(3)]
        + [view(el, k) for k in range(3)]
        + [view(kite, v, k) for v in range(2) for k in range(3)]
        + [view(cor, v) for v in range(2)]
    )


def geo_slot(k):
    return 12 if k == 0 else (1 + (k - 1) % 7) * GROUP + 12 + (k - 1) // 7


def put_geo(dst, at, f, area):
    for k in range(3):
        dst[(k,) + at] = 0.25 * f[k] * f[3 + k]
        dst[(5 + k,) + at] = SLOPE / f[k]
    for v in range(2):
        dst[(3 + v,) + at] = f[12 + v] * (f[6 + 3 * v] + f[7 + 3 * v] + f[8 + 3 * v])
    dst[(8,) + at] = 1.0 / area


def fields(grid, views):
    return [Field(grid, lambda r, c, f=f: f(*span(r, c))) for f in views]


def run(grid, x, kites, dist, derived, swap=lambda i, f: f):
    f = fields(grid, derived)
    d = fields(grid, dist)
    cc, dd, outputs, stages = chain(
        grid, x[0:3], x[3], x[4:7], x[7], d, f[0:3], fields(grid, kites), f[3:5], swap
    )
    return cc, dd, outputs(f[5:9]), stages


def build(fields_of):
    for f in fields_of:
        for r in range(f.grid[0]):
            for c in range(f.grid[1]):
                f(r, c)


class Strips:
    def __init__(self, levels, cols):
        _, lane = iotas()
        self.levels, self.lane = levels, lane
        self.head, self.tail = slice(0, LANE), slice(cols - LANE, cols)
        pos = lane & (GROUP - 1)
        self.pos, self.group = pos, lane >> 4
        self.index = jnp.where(pos < 5, jnp.maximum(pos - 2, 0), jnp.minimum(pos + LANE - 11, LANE - 1))
        self.back = [
            jnp.where(lane < LANE // 2, l * GROUP + 2, l * GROUP + 11 - LANE + lane) & (LANE - 1)
            for l in range(levels)
        ]

    def own(self, f, rs):
        return pick(jnp.where(self.lane < LANE // 2, f(rs, self.head), f(rs, self.tail)), self.index)

    def own_levels(self, src, rs):
        got = [[self.own(f, rs) for f in level_views(l, src)] for l in range(self.levels)]
        out = got[0]
        for l in range(1, self.levels):
            out = [jnp.where(self.group == l, x, y) for x, y in zip(got[l], out)]
        return out

    def insert(self, x, right, left):
        pos = self.pos
        return jnp.where((pos == 11) | (pos == 12), right, jnp.where(pos == 1, left, x))

    def with_level(self, k, x, right, left):
        return self.insert(x, roll(right, 11 - SLOT[k], 1), roll(left, 2 - SLOT[k], 1))

    def with_geo(self, k, x, right, left):
        at = geo_slot(k)
        m = jnp.where(self.lane == at - 1, left, right)
        y = pick(m, jnp.where(self.pos == 11, at, jnp.where(self.pos == 12, at + 1, at - 1)))
        return self.insert(x, y, y)

    def masks(self):
        lane = self.lane
        first, end, ends = lane == 0, lane == LANE - 1, lane >= LANE - 2
        return [(None, end), (None, end), (first, None), (first, end)] + [(first, ends)] * 3


def strip_chain(grid, x, raw, area, swap=lambda i, f: f):
    ws = [Field(grid, lambda r, c, k=k: 0.25 * raw[k](r, c) * raw[3 + k](r, c)) for k in range(3)]

    def weighed(v):
        a = [raw[6 + 3 * v + k] for k in range(3)]
        return Field(grid, lambda r, c: raw[12 + v](r, c) * (a[0](r, c) + a[1](r, c) + a[2](r, c)))

    cc, dd, outputs, stages = chain(
        grid, x[0:3], x[3], x[4:7], x[7], raw[0:3], ws, raw[6:12], [weighed(v) for v in range(2)], swap
    )
    scale = [Field(grid, lambda r, c, k=k: SLOPE / raw[k](r, c)) for k in range(3)]
    scale.append(Field(grid, lambda r, c: 1.0 / area(r, c)))
    return cc, dd, outputs(scale), stages


def planes(vert, kin, cell, edge):
    return [(vert, (0,)), (vert, (1,)), (kin, ()), (cell, ())] + [(edge, (k,)) for k in range(3)]


def main_kernel(counts, *refs):
    hbm = refs[:9]
    o_vert, o_kin, o_cell, o_edge = refs[9:13]
    bands = refs[13:22]
    g_right, g_left, saved, ssaved = refs[22:26]
    bufs = refs[26:35]
    p_right, p_left, geo, slev, sgeo, tally = refs[35:41]
    in_sem, own_sem, send_row, recv_row, send_col, recv_col = refs[41:47]
    ny, nx = counts
    py, px = lax.axis_index("py"), lax.axis_index("px")
    down, up = lax.rem(py + 1, ny), lax.rem(py + ny - 1, ny)
    right, left = lax.rem(px + 1, nx), lax.rem(px + nx - 1, nx)

    barrier = pltpu.get_barrier_semaphore()
    near = [
        (up, px), (down, px), (py, left), (py, right),
        (up, left), (up, right), (down, left), (down, right),
    ]
    for y, x in near:
        pl.semaphore_signal(barrier, inc=1, device_id={"py": y, "px": x}, device_id_type=MESH)

    b_area = bufs[8]
    levels, rows, cols = bufs[1].shape
    nr, nc = rows // SUB, cols // LANE
    sub, lane = iotas()

    def await_rows(sem, n):
        pltpu.make_async_copy(tally.at[0:n], tally.at[0:n], sem).wait()

    def part(ref, a, b, *lead):
        rest = (slice(None),) * (len(ref.shape) - 2 - len(lead))
        return ref.at[lead + rest + (slice(a, b), slice(None))]

    def count(ref):
        n = 1
        for d in ref.shape[:-1]:
            n *= d
        return n

    for a, b in zip(hbm, bands):
        pltpu.make_async_copy(part(a, rows - 2, rows), part(b, 0, 2), own_sem.at[0]).start()
    for a, b in zip(hbm, bands):
        pltpu.make_async_copy(part(a, 0, 2), part(b, 6, 8), own_sem.at[1]).start()
    own_rows = sum(2 * count(b) // SUB for b in bands)
    for i in (4, 5, 6, 7, 8):
        pltpu.make_async_copy(hbm[i], bufs[i], in_sem.at[0]).start()
    cuts = [slice(i * levels // PARTS, (i + 1) * levels // PARTS) for i in range(PARTS)]
    for j, cut in enumerate(cuts):
        for a, b in zip(hbm[:4], bufs):
            at = (slice(None),) * (len(a.shape) - 3) + (cut,)
            pltpu.make_async_copy(a.at[at], b.at[at], in_sem.at[1 + j]).start()

    def remote(src, dst, send, recv, y, x):
        return pltpu.make_async_remote_copy(
            src_ref=src,
            dst_ref=dst,
            send_sem=send,
            recv_sem=recv,
            device_id={"py": y, "px": x},
            device_id_type=MESH,
        )

    vel, th, vt, tt, cd, el, kite, cor = bands[:8]
    to_up = [
        (2, vel, slice(1, 3)), (1, vel, 0), (2, th), (2, vt, slice(1, 3)), (1, vt, 0), (2, tt),
        (2, cd, slice(1, 3)), (1, cd, 0), (1, el, 2), (2, kite, 1), (1, kite, 0), (2, cor, 1), (1, cor, 0),
    ]
    to_down = [
        (2, vel, slice(0, 2)), (1, vel, 2), (2, th), (2, vt, slice(0, 2)), (1, vt, 2), (2, tt),
        (2, cd, slice(0, 2)), (1, cd, 2), (1, el, 0), (2, kite, 0), (1, kite, 1), (2, cor, 0), (1, cor, 1),
    ]
    sems = (send_row.at[0], recv_row.at[0])
    up_copies, down_copies, sent = [], [], 0
    for n, b, *lead in to_up:
        src = part(b, 6, 6 + n, *lead)
        up_copies.append(remote(src, part(b, 2, 2 + n, *lead), *sems, up, px))
        sent += count(src)
    for n, b, *lead in to_down:
        src = part(b, 2 - n, 2, *lead)
        down_copies.append(remote(src, part(b, 6 - n, 6, *lead), *sems, down, px))
        sent += count(src)
    await_rows(own_sem.at[0], own_rows)
    pl.semaphore_wait(barrier, len(near))
    for copy in down_copies:
        copy.start()

    strips = Strips(levels, cols)
    head, tail = strips.head, strips.tail
    tiles = [slice(r * SUB, (r + 1) * SUB) for r in range(nr + 1)]

    await_rows(in_sem.at[0], sum(count(b) for b in bufs[4:]))
    own_geo = geo_views(bufs[4:8])
    packed = [[jnp.zeros((SUB, LANE), F32)] * 2 for _ in range(nr)]

    def pack(items):
        for r in range(nr):
            rs, (ra, la) = tiles[r], packed[r]
            for s, two, f in items:
                m = jnp.where(lane < LANE // 2, f(rs, head), f(rs, tail))
                m = roll(m, s, 1)
                ra = jnp.where((lane == s) | (lane == s + 1) if two else lane == s, m, ra)
                la = jnp.where(lane == (s + LANE - 1) % LANE, m, la)
            packed[r] = [ra, la]

    pack([(geo_slot(k), k == 0, f) for k, f in enumerate(own_geo)])
    for j, cut in enumerate(cuts):
        await_rows(in_sem.at[1 + j], sum(count(b) for b in bufs[:4]) // PARTS)
        items = []
        for l in range(cut.start, cut.stop):
            for k, f in enumerate(level_views(l, bufs[:4])):
                items.append((l * GROUP + SLOT[k], k in TWO, f))
        pack(items)
    for r in range(nr):
        p_right[tiles[r]], p_left[tiles[r]] = packed[r]

    def column(src, dst, i, y, x):
        return remote(src, dst, send_col.at[i], recv_col.at[i], y, x)

    col_copies = [
        column(p_right, g_right.at[0:rows], 0, py, left),
        column(p_left, g_left.at[0:rows], 1, py, right),
        column(p_right.at[rows - 2 : rows], g_right.at[rows + 4 : rows + 6], 2, down, left),
        column(p_right.at[0:2], g_right.at[rows + 2 : rows + 4], 3, up, left),
        column(p_left.at[0:2], g_left.at[rows + 2 : rows + 4], 4, up, right),
    ]
    for copy in col_copies:
        copy.start()
    await_rows(own_sem.at[1], own_rows)
    for copy in up_copies:
        copy.start()

    for r in range(nr):
        for c in range(nc):
            put_geo(geo, span(r, c), [f(*span(r, c)) for f in own_geo], b_area[span(r, c)])

    for rs in tiles[:nr]:
        for k, x in enumerate(strips.own_levels(bufs[:4], rs)):
            slev[k, rs] = x
        for k, f in enumerate(own_geo + [view(b_area)]):
            sgeo[k, rs] = strips.own(f, rs)

    outputs_of = planes(o_vert, o_kin, o_cell, o_edge)

    def block(l):
        cc, dd, outs, _ = run(
            (nr, nc),
            fields((nr, nc), level_views(l, bufs[:4])),
            own_geo[6:12],
            own_geo[0:3],
            [view(geo, k) for k in range(9)],
        )
        for c in range(nc):
            for i, f in enumerate((cc, dd)):
                saved[i, l, :, span(0, c)[1]] = jnp.where(
                    sub < 4, roll(f(nr - 1, c), 2, 0), roll(f(0, c), -2, 0)
                )
        for r in range(nr):
            for c in range(nc):
                for (ref, lead), f in zip(outputs_of, outs):
                    ref[lead + (l,) + span(r, c)] = f(r, c)

    def inner(i, carry):
        for u in range(PAIR):
            block(i * PAIR + u)
        return carry

    lax.fori_loop(0, levels // PAIR, inner, 0)

    for copy in col_copies[:2]:
        copy.wait()
    grid = (nr, 1)
    x = [
        Field(
            grid,
            lambda r, c, k=k: strips.with_level(
                k, slev[k, tiles[r]], g_right[tiles[r]], g_left[tiles[r]]
            ),
        )
        for k in range(8)
    ]
    raw = [
        Field(
            grid,
            lambda r, c, k=k: strips.with_geo(
                k, sgeo[k, tiles[r]], g_right[tiles[r]], g_left[tiles[r]]
            ),
        )
        for k in range(14)
    ]
    cc, dd, outs, stages = strip_chain(grid, x, raw, lambda r, c: sgeo[14, tiles[r]])
    for stage in [x + raw] + stages + [outs]:
        build(stage)
    for i, f in enumerate((cc, dd)):
        ssaved[i] = jnp.where(sub < 4, roll(f(nr - 1, 0), 2, 0), roll(f(0, 0), -2, 0))
    for l in range(levels):
        for r in range(nr):
            moved = [pick(f(r, 0), strips.back[l]) for f in outs]
            for (ref, lead), z, (mf, me) in zip(outputs_of, moved, strips.masks()):
                if mf is not None:
                    pltpu.store(ref.at[lead + (l, tiles[r], head)], z, mask=mf)
                if me is not None:
                    pltpu.store(ref.at[lead + (l, tiles[r], tail)], z, mask=me)

    for copy in col_copies[2:]:
        copy.wait()
    await_rows(send_row.at[0], sent)
    await_rows(recv_row.at[0], sent)


def finish_kernel(*refs):
    kept = refs[0:4]
    bands = refs[4:13]
    g_right, g_left, saved, ssaved = refs[13:17]
    final = refs[17:21]
    ends = refs[21:25]
    kgeo, sem = refs[25:27]
    levels, rows, cols = kept[1].shape
    nr, nc = rows // SUB, cols // LANE
    sub, lane = iotas()

    def send(src, dst, which):
        pltpu.make_async_copy(src, dst, sem.at[which]).start()

    def part(ref, a, b, *lead):
        rest = (slice(None),) * (len(ref.shape) - 2 - len(lead))
        return ref.at[lead + rest + (slice(a, b), slice(None))]

    changed = [(0, 1), (1, 0), (1, 1), (1, 1), (1, 2), (1, 1), (2, 1)]
    array_of = (0, 0, 1, 2, 3, 3, 3)
    src_of, end_of, dst_of = planes(*kept), planes(*ends), planes(*final)
    if nr > 2:
        for i, (a, b) in enumerate(zip(kept, final)):
            send(part(a, SUB, rows - SUB), part(b, SUB, rows - SUB), i)
    for (src, lead), (dst, _), (n_top, n_low), which in zip(src_of, dst_of, changed, array_of):
        for a, b in ((n_top, SUB), (rows - SUB, rows - n_low)):
            send(part(src, a, b, *lead), part(dst, a, b, *lead), which)

    strips = Strips(levels, cols)
    low, top = slice(0, SUB), slice(rows, rows + SUB)
    first_rows, last_rows = slice(0, SUB), slice(rows - SUB, rows)

    def border(g):
        a, b = roll(g[last_rows], 2, 0), roll(g[first_rows], -2, 0)
        return jnp.where(sub < 2, a, jnp.where(sub >= 6, b, g[top]))

    band_geo = geo_views(bands[4:8])
    one = (1, 1)
    const = lambda t: Field(one, lambda r, c: t)
    sides = border(g_right), border(g_left)
    own_levels = strips.own_levels(bands[:4], low)
    own_geo = [strips.own(f, low) for f in band_geo]
    area = strips.own(view(bands[8]), low)
    x = [const(strips.with_level(k, own_levels[k], *sides)) for k in range(8)]
    raw = [const(strips.with_geo(k, own_geo[k], *sides)) for k in range(14)]
    for c in range(nc):
        at = span(0, c)
        put_geo(kgeo, at, [f(*at) for f in band_geo], bands[8][at])

    merge = (sub == 0) | (sub == SUB - 1)

    def swap_with(grid, load):
        return lambda i, f: Field(grid, lambda r, c: jnp.where(merge, load(i, c), f(r, c)))

    _, _, souts, sstages = strip_chain(
        one, x, raw, lambda r, c: area, swap_with(one, lambda i, c: ssaved[i])
    )
    grid = (1, nc)
    jobs = []
    for l in range(levels):
        jobs.append(
            run(
                grid,
                fields(grid, level_views(l, bands[:4])),
                band_geo[6:12],
                band_geo[0:3],
                [view(kgeo, k) for k in range(9)],
                swap_with(grid, lambda i, c, l=l: saved[i, l, :, span(0, c)[1]]),
            )[2:]
        )

    masks = strips.masks()

    def finalize(i):
        end, lead = end_of[i]
        dst = dst_of[i][0]
        n_top, n_low = changed[i]
        y = souts[i](0, 0)
        zs = [pick(y, strips.back[l]) for l in range(levels)]
        for l in range(levels):
            for c in range(nc):
                t = jobs[l][0][i](0, c)
                for m, at in zip(masks[i], (0, nc - 1)):
                    if m is not None and at == c:
                        t = jnp.where(m, zs[l], t)
                end[lead + (l,) + span(0, c)] = t
        if n_top:
            send(part(end, 6, 6 + n_top, *lead), part(dst, 0, n_top, *lead), array_of[i])
        if n_low:
            send(part(end, 2 - n_low, 2, *lead), part(dst, rows - n_low, rows, *lead), array_of[i])

    ready = [(), (0, 1, 2), (3,), (4, 5, 6)]
    for stage, done in enumerate(ready):
        for _, stages in jobs:
            build(stages[stage])
        build(sstages[stage])
        for i in done:
            finalize(i)
    for i, (a, b) in enumerate(zip(kept, final)):
        pltpu.make_async_copy(a, b, sem.at[i]).wait()


def local(counts, vel, th, vt, tt, cd, el, area, kite, cor):
    args = (vel, th, vt, tt, cd, el, kite, cor, area)
    levels, rows, cols = th.shape
    outs = [(2, levels, rows, cols), (levels, rows, cols), (levels, rows, cols), (3, levels, rows, cols)]
    short = lambda s, n: s[:-2] + (n, cols)
    hbm, vmem = pl.BlockSpec(memory_space=pl.ANY), pl.BlockSpec(memory_space=pltpu.VMEM)
    side = (rows + SUB, LANE)
    passed = outs + [short(a.shape, SUB) for a in args]
    passed += [side, side, (2, levels, SUB, cols), (2, SUB, LANE)]
    kept = pl.pallas_call(
        lambda *refs: main_kernel(counts, *refs),
        out_shape=[pltpu.VMEM(s, F32) for s in passed],
        in_specs=[hbm] * len(args),
        out_specs=[vmem] * len(passed),
        scratch_shapes=[pltpu.VMEM(a.shape, F32) for a in args]
        + [
            pltpu.VMEM((rows, LANE), F32),
            pltpu.VMEM((rows, LANE), F32),
            pltpu.VMEM((9, rows, cols), F32),
            pltpu.VMEM((8, rows, LANE), F32),
            pltpu.VMEM((15, rows, LANE), F32),
            pltpu.VMEM((8 * levels * rows, 1, cols), F32),
        ]
        + [pltpu.SemaphoreType.DMA((n,)) for n in (1 + PARTS, 2, 1, 1, 5, 5)],
        compiler_params=pltpu.CompilerParams(collective_id=0, has_side_effects=True),
        name="main",
    )(*args)
    return pl.pallas_call(
        finish_kernel,
        out_shape=[jax.ShapeDtypeStruct(s, F32) for s in outs],
        in_specs=[vmem] * len(passed),
        out_specs=[pl.BlockSpec(memory_space=pltpu.HBM)] * len(outs),
        scratch_shapes=[pltpu.VMEM(short(s, SUB), F32) for s in outs]
        + [pltpu.VMEM((9, SUB, cols), F32), pltpu.SemaphoreType.DMA((4,))],
        name="finish",
    )(*[pltpu.with_memory_space_constraint(x, pltpu.VMEM) for x in kept])


def solution(mesh):
    counts = (mesh.shape["py"], mesh.shape["px"])
    p4, p3 = P(None, None, "py", "px"), P(None, "py", "px")
    return jax.shard_map(
        lambda *args: local(counts, *args),
        mesh=mesh,
        in_specs=(p4, p3, p4, p3, p3, p3, P("py", "px"), p4, p3),
        out_specs=(p4, p3, p3, p4),
        check_vma=False,
    )
```

```python
import jax
import jax.numpy as jnp
from jax import lax
from jax.experimental import pallas as pl
from jax.experimental.pallas import tpu as pltpu
from jax.sharding import PartitionSpec as P

SUB = 8
LANE = 128
GROUP = 16
PAIR = 2
PARTS = 2
SLOT = (0, 8, 9, 2, 4, 10, 11, 6)
TWO = (0, 3, 4, 7)
MESH = pl.DeviceIdType.MESH
F32 = jnp.float32
SLOPE = -0.5 / 36.0


def iotas():
    sub = lax.broadcasted_iota(jnp.int32, (SUB, LANE), 0)
    lane = lax.broadcasted_iota(jnp.int32, (SUB, LANE), 1)
    return sub, lane


def roll(x, shift, axis):
    n = (SUB, LANE)[axis]
    return pltpu.roll(x, shift % n, axis) if shift % n else x


def pick(x, index):
    return jnp.take_along_axis(x, index, axis=1)


def span(r, c):
    return (slice(r * SUB, (r + 1) * SUB), slice(c * LANE, (c + 1) * LANE))


class Field:
    def __init__(self, grid, make):
        self.grid, self.make, self.memo = grid, make, {}

    def __call__(self, r, c):
        key = (r % self.grid[0], c % self.grid[1])
        if key not in self.memo:
            self.memo[key] = self.make(*key)
        return self.memo[key]


def chain(grid, v, h, t, g, dist, ew, kt, ct, swap=lambda i, f: f):
    sub, lane = iotas()

    def lift(fn, *fields):
        return Field(grid, lambda r, c: fn(*[f(r, c) for f in fields]))

    def row_shift(f, a):
        rolled = Field(grid, lambda r, c: roll(f(r, c), -a, 0))
        if grid[0] == 1:
            return rolled
        keep = sub < SUB - 1 if a == 1 else sub > 0
        return Field(grid, lambda r, c: jnp.where(keep, rolled(r, c), rolled(r + a, c)))

    def col_shift(f, b):
        rolled = Field(grid, lambda r, c: roll(f(r, c), -b, 1))
        if grid[1] == 1:
            return rolled
        keep = lane < LANE - 1 if b == 1 else lane > 0
        return Field(grid, lambda r, c: jnp.where(keep, rolled(r, c), rolled(r, c + b)))

    def parts(vv, hh):
        flux = [lift(lambda a, b: a * b, vv[k], dist[k]) for k in range(3)]
        c0 = lift(lambda a, b, c: a + b - c, flux[0], row_shift(flux[2], 1), flux[1])
        fc = col_shift(row_shift(flux[0], -1), 1)
        c1 = lift(lambda a, b, c: a - b - c, flux[1], flux[2], fc)
        hc = col_shift(hh, 1)
        hr = row_shift(hh, 1)
        hd = row_shift(hc, -1)
        mix = lambda a, b, c, p, q, s: a * p + b * q + c * s
        h0 = lift(mix, kt[0], kt[1], kt[2], hh, hr, hc)
        h1 = lift(mix, kt[3], kt[4], kt[5], hh, hc, hd)
        return (c0, c1), (h0, h1), [hc, fc]

    cv, hv, moved_v = parts(v, h)
    cw, hw, moved_t = parts(t, g)

    def potential(k):
        def make(r, c):
            a0 = ct[k](r, c) + cv[k](r, c)
            a1 = cw[k](r, c)
            b0 = hv[k](r, c)
            b1 = hw[k](r, c)
            bm, be = b0 + 0.5 * b1, b0 + b1
            m = bm * be
            scale_all = 1.0 / (b0 * m)
            mid = (a0 + a0 + a1) * (b0 * be)
            late = mid + (a0 + a1) * (b0 * bm)
            return (a0 * m + mid + late) * scale_all, late * scale_all

        both = Field(grid, make)
        return Field(grid, lambda r, c: both(r, c)[0]), Field(grid, lambda r, c: both(r, c)[1])

    p0, q0 = potential(0)
    p1, q1 = potential(1)
    add = lambda a, b: a + b
    add3 = lambda a, b, c: a + b + c

    def cell(f0, f1):
        f0_up = row_shift(f0, -1)
        f1_down = row_shift(f1, 1)
        pair = lift(add, f0, f1)
        return lift(add3, pair, f0_up, col_shift(lift(add, pair, f1_down), -1)), f0_up, f1_down, pair

    cc, p0_up, p1_down, pair = cell(p0, p1)
    dd = cell(q0, q1)[0]
    cc, dd = swap(0, cc), swap(1, dd)
    p1_low = col_shift(p1_down, -1)

    def neighbours(f):
        fc = col_shift(f, 1)
        return row_shift(f, 1), fc, row_shift(fc, -1)

    cn, dn = neighbours(cc), neighbours(dd)
    ends = [lift(add, p0, p1_low), pair, lift(add, p1, p0_up)]
    en = [
        lift(lambda w, a, b: w * (a * (a + b) + (1.0 / 3.0) * (b * b)), ew[k], v[k], t[k])
        for k in range(3)
    ]
    e_up = row_shift(en[0], -1)
    e_low = col_shift(lift(add, en[1], row_shift(en[2], 1)), -1)

    def outputs(scale):
        def edge(k):
            def make(r, c):
                slope = v[k](r, c) * (cn[k](r, c) - cc(r, c)) + t[k](r, c) * (dn[k](r, c) - dd(r, c))
                return ends[k](r, c) * (1.0 / 12.0) + scale[k](r, c) * slope

            return Field(grid, make)

        kin = Field(
            grid,
            lambda r, c: (en[0](r, c) + en[1](r, c) + en[2](r, c) + e_up(r, c) + e_low(r, c)) * scale[3](r, c),
        )
        return [
            lift(lambda a: a * (1.0 / 6.0), p0),
            lift(lambda a: a * (1.0 / 6.0), p1),
            kin,
            lift(lambda a: a * (1.0 / 36.0), cc),
        ] + [edge(k) for k in range(3)]

    stages = [moved_v + moved_t, [p0, q0, p1, q1, e_low], [cc, dd, p1_low], [*cn, *dn]]
    return cc, dd, outputs, stages


def view(ref, *lead):
    return lambda r, c: ref[lead + (r, c)]


def level_views(l, src):
    vel, th, vt, tt = src
    return (
        [view(vel, k, l) for k in range(3)]
        + [view(th, l)]
        + [view(vt, k, l) for k in range(3)]
        + [view(tt, l)]
    )


def geo_views(src):
    cd, el, kite, cor = src
    return (
        [view(cd, k) for k in range(3)]
        + [view(el, k) for k in range(3)]
        + [view(kite, v, k) for v in range(2) for k in range(3)]
        + [view(cor, v) for v in range(2)]
    )


def geo_slot(k):
    return 12 if k == 0 else (1 + (k - 1) % 7) * GROUP + 12 + (k - 1) // 7


def put_geo(dst, at, f, area):
    for k in range(3):
        dst[(k,) + at] = 0.25 * f[k] * f[3 + k]
        dst[(5 + k,) + at] = SLOPE / f[k]
    for v in range(2):
        dst[(3 + v,) + at] = f[12 + v] * (f[6 + 3 * v] + f[7 + 3 * v] + f[8 + 3 * v])
    dst[(8,) + at] = 1.0 / area


def fields(grid, views):
    return [Field(grid, lambda r, c, f=f: f(*span(r, c))) for f in views]


def run(grid, x, kites, dist, derived, swap=lambda i, f: f):
    f = fields(grid, derived)
    d = fields(grid, dist)
    cc, dd, outputs, stages = chain(
        grid, x[0:3], x[3], x[4:7], x[7], d, f[0:3], fields(grid, kites), f[3:5], swap
    )
    return cc, dd, outputs(f[5:9]), stages


def build(fields_of):
    for f in fields_of:
        for r in range(f.grid[0]):
            for c in range(f.grid[1]):
                f(r, c)


class Strips:
    def __init__(self, levels, cols):
        _, lane = iotas()
        self.levels, self.lane = levels, lane
        self.head, self.tail = slice(0, LANE), slice(cols - LANE, cols)
        pos = lane & (GROUP - 1)
        self.pos, self.group = pos, lane >> 4
        self.index = jnp.where(pos < 5, jnp.maximum(pos - 2, 0), jnp.minimum(pos + LANE - 11, LANE - 1))
        self.back = [
            jnp.where(lane < LANE // 2, l * GROUP + 2, l * GROUP + 11 - LANE + lane) & (LANE - 1)
            for l in range(levels)
        ]

    def own(self, f, rs):
        return pick(jnp.where(self.lane < LANE // 2, f(rs, self.head), f(rs, self.tail)), self.index)

    def own_levels(self, src, rs):
        got = [[self.own(f, rs) for f in level_views(l, src)] for l in range(self.levels)]
        out = got[0]
        for l in range(1, self.levels):
            out = [jnp.where(self.group == l, x, y) for x, y in zip(got[l], out)]
        return out

    def insert(self, x, right, left):
        pos = self.pos
        return jnp.where((pos == 11) | (pos == 12), right, jnp.where(pos == 1, left, x))

    def with_level(self, k, x, right, left):
        return self.insert(x, roll(right, 11 - SLOT[k], 1), roll(left, 2 - SLOT[k], 1))

    def with_geo(self, k, x, right, left):
        at = geo_slot(k)
        m = jnp.where(self.lane == at - 1, left, right)
        y = pick(m, jnp.where(self.pos == 11, at, jnp.where(self.pos == 12, at + 1, at - 1)))
        return self.insert(x, y, y)

    def masks(self):
        lane = self.lane
        first, end, ends = lane == 0, lane == LANE - 1, lane >= LANE - 2
        return [(None, end), (None, end), (first, None), (first, end)] + [(first, ends)] * 3


def strip_chain(grid, x, raw, area, swap=lambda i, f: f):
    ws = [Field(grid, lambda r, c, k=k: 0.25 * raw[k](r, c) * raw[3 + k](r, c)) for k in range(3)]

    def weighed(v):
        a = [raw[6 + 3 * v + k] for k in range(3)]
        return Field(grid, lambda r, c: raw[12 + v](r, c) * (a[0](r, c) + a[1](r, c) + a[2](r, c)))

    cc, dd, outputs, stages = chain(
        grid, x[0:3], x[3], x[4:7], x[7], raw[0:3], ws, raw[6:12], [weighed(v) for v in range(2)], swap
    )
    scale = [Field(grid, lambda r, c, k=k: SLOPE / raw[k](r, c)) for k in range(3)]
    scale.append(Field(grid, lambda r, c: 1.0 / area(r, c)))
    return cc, dd, outputs(scale), stages


def planes(vert, kin, cell, edge):
    return [(vert, (0,)), (vert, (1,)), (kin, ()), (cell, ())] + [(edge, (k,)) for k in range(3)]


def main_kernel(counts, *refs):
    hbm = refs[:9]
    o_vert, o_kin, o_cell, o_edge = refs[9:13]
    bands = refs[13:22]
    g_right, g_left, saved, ssaved = refs[22:26]
    bufs = refs[26:35]
    p_right, p_left, geo, slev, sgeo, tally = refs[35:41]
    in_sem, own_sem, send_row, recv_row, send_col, recv_col = refs[41:47]
    ny, nx = counts
    py, px = lax.axis_index("py"), lax.axis_index("px")
    down, up = lax.rem(py + 1, ny), lax.rem(py + ny - 1, ny)
    right, left = lax.rem(px + 1, nx), lax.rem(px + nx - 1, nx)

    barrier = pltpu.get_barrier_semaphore()
    near = [
        (up, px), (down, px), (py, left), (py, right),
        (up, left), (up, right), (down, left), (down, right),
    ]
    for y, x in near:
        pl.semaphore_signal(barrier, inc=1, device_id={"py": y, "px": x}, device_id_type=MESH)

    b_area = bufs[8]
    levels, rows, cols = bufs[1].shape
    nr, nc = rows // SUB, cols // LANE
    sub, lane = iotas()

    def await_rows(sem, n):
        pltpu.make_async_copy(tally.at[0:n], tally.at[0:n], sem).wait()

    def part(ref, a, b, *lead):
        rest = (slice(None),) * (len(ref.shape) - 2 - len(lead))
        return ref.at[lead + rest + (slice(a, b), slice(None))]

    def count(ref):
        n = 1
        for d in ref.shape[:-1]:
            n *= d
        return n

    for a, b in zip(hbm, bands):
        pltpu.make_async_copy(part(a, rows - 2, rows), part(b, 0, 2), own_sem.at[0]).start()
    for a, b in zip(hbm, bands):
        pltpu.make_async_copy(part(a, 0, 2), part(b, 6, 8), own_sem.at[1]).start()
    own_rows = sum(2 * count(b) // SUB for b in bands)
    for i in (4, 5, 6, 7, 8):
        pltpu.make_async_copy(hbm[i], bufs[i], in_sem.at[0]).start()
    cuts = [slice(i * levels // PARTS, (i + 1) * levels // PARTS) for i in range(PARTS)]
    for j, cut in enumerate(cuts):
        for a, b in zip(hbm[:4], bufs):
            at = (slice(None),) * (len(a.shape) - 3) + (cut,)
            pltpu.make_async_copy(a.at[at], b.at[at], in_sem.at[1 + j]).start()

    def remote(src, dst, send, recv, y, x):
        return pltpu.make_async_remote_copy(
            src_ref=src,
            dst_ref=dst,
            send_sem=send,
            recv_sem=recv,
            device_id={"py": y, "px": x},
            device_id_type=MESH,
        )

    vel, th, vt, tt, cd, el, kite, cor = bands[:8]
    to_up = [
        (2, vel, slice(1, 3)), (1, vel, 0), (2, th), (2, vt, slice(1, 3)), (1, vt, 0), (2, tt),
        (2, cd, slice(1, 3)), (1, cd, 0), (1, el, 2), (2, kite, 1), (1, kite, 0), (2, cor, 1), (1, cor, 0),
    ]
    to_down = [
        (2, vel, slice(0, 2)), (1, vel, 2), (2, th), (2, vt, slice(0, 2)), (1, vt, 2), (2, tt),
        (2, cd, slice(0, 2)), (1, cd, 2), (1, el, 0), (2, kite, 0), (1, kite, 1), (2, cor, 0), (1, cor, 1),
    ]
    sems = (send_row.at[0], recv_row.at[0])
    up_copies, down_copies, sent = [], [], 0
    for n, b, *lead in to_up:
        src = part(b, 6, 6 + n, *lead)
        up_copies.append(remote(src, part(b, 2, 2 + n, *lead), *sems, up, px))
        sent += count(src)
    for n, b, *lead in to_down:
        src = part(b, 2 - n, 2, *lead)
        down_copies.append(remote(src, part(b, 6 - n, 6, *lead), *sems, down, px))
        sent += count(src)
    await_rows(own_sem.at[0], own_rows)
    pl.semaphore_wait(barrier, len(near))
    for copy in down_copies:
        copy.start()

    strips = Strips(levels, cols)
    head, tail = strips.head, strips.tail
    tiles = [slice(r * SUB, (r + 1) * SUB) for r in range(nr + 1)]

    await_rows(in_sem.at[0], sum(count(b) for b in bufs[4:]))
    own_geo = geo_views(bufs[4:8])
    packed = [[jnp.zeros((SUB, LANE), F32)] * 2 for _ in range(nr)]

    def pack(items):
        for r in range(nr):
            rs, (ra, la) = tiles[r], packed[r]
            for s, two, f in items:
                m = jnp.where(lane < LANE // 2, f(rs, head), f(rs, tail))
                m = roll(m, s, 1)
                ra = jnp.where((lane == s) | (lane == s + 1) if two else lane == s, m, ra)
                la = jnp.where(lane == (s + LANE - 1) % LANE, m, la)
            packed[r] = [ra, la]

    pack([(geo_slot(k), k == 0, f) for k, f in enumerate(own_geo)])
    for j, cut in enumerate(cuts):
        await_rows(in_sem.at[1 + j], sum(count(b) for b in bufs[:4]) // PARTS)
        items = []
        for l in range(cut.start, cut.stop):
            for k, f in enumerate(level_views(l, bufs[:4])):
                items.append((l * GROUP + SLOT[k], k in TWO, f))
        pack(items)
    for r in range(nr):
        p_right[tiles[r]], p_left[tiles[r]] = packed[r]

    def column(src, dst, i, y, x):
        return remote(src, dst, send_col.at[i], recv_col.at[i], y, x)

    col_copies = [
        column(p_right, g_right.at[0:rows], 0, py, left),
        column(p_left, g_left.at[0:rows], 1, py, right),
        column(p_right.at[rows - 2 : rows], g_right.at[rows + 4 : rows + 6], 2, down, left),
        column(p_right.at[0:2], g_right.at[rows + 2 : rows + 4], 3, up, left),
        column(p_left.at[0:2], g_left.at[rows + 2 : rows + 4], 4, up, right),
    ]
    for copy in col_copies:
        copy.start()

    for r in range(nr):
        for c in range(nc):
            put_geo(geo, span(r, c), [f(*span(r, c)) for f in own_geo], b_area[span(r, c)])

    await_rows(own_sem.at[1], own_rows)
    for copy in up_copies:
        copy.start()
    for rs in tiles[:nr]:
        for k, x in enumerate(strips.own_levels(bufs[:4], rs)):
            slev[k, rs] = x
        for k, f in enumerate(own_geo + [view(b_area)]):
            sgeo[k, rs] = strips.own(f, rs)

    outputs_of = planes(o_vert, o_kin, o_cell, o_edge)

    def block(l):
        cc, dd, outs, _ = run(
            (nr, nc),
            fields((nr, nc), level_views(l, bufs[:4])),
            own_geo[6:12],
            own_geo[0:3],
            [view(geo, k) for k in range(9)],
        )
        for c in range(nc):
            for i, f in enumerate((cc, dd)):
                saved[i, l, :, span(0, c)[1]] = jnp.where(
                    sub < 4, roll(f(nr - 1, c), 2, 0), roll(f(0, c), -2, 0)
                )
        for r in range(nr):
            for c in range(nc):
                for (ref, lead), f in zip(outputs_of, outs):
                    ref[lead + (l,) + span(r, c)] = f(r, c)

    def inner(i, carry):
        for u in range(PAIR):
            block(i * PAIR + u)
        return carry

    lax.fori_loop(0, levels // PAIR, inner, 0)

    for copy in col_copies[:2]:
        copy.wait()
    grid = (nr, 1)
    x = [
        Field(
            grid,
            lambda r, c, k=k: strips.with_level(
                k, slev[k, tiles[r]], g_right[tiles[r]], g_left[tiles[r]]
            ),
        )
        for k in range(8)
    ]
    raw = [
        Field(
            grid,
            lambda r, c, k=k: strips.with_geo(
                k, sgeo[k, tiles[r]], g_right[tiles[r]], g_left[tiles[r]]
            ),
        )
        for k in range(14)
    ]
    cc, dd, outs, stages = strip_chain(grid, x, raw, lambda r, c: sgeo[14, tiles[r]])
    for stage in [x + raw] + stages + [outs]:
        build(stage)
    for i, f in enumerate((cc, dd)):
        ssaved[i] = jnp.where(sub < 4, roll(f(nr - 1, 0), 2, 0), roll(f(0, 0), -2, 0))
    for l in range(levels):
        for r in range(nr):
            moved = [pick(f(r, 0), strips.back[l]) for f in outs]
            for (ref, lead), z, (mf, me) in zip(outputs_of, moved, strips.masks()):
                if mf is not None:
                    pltpu.store(ref.at[lead + (l, tiles[r], head)], z, mask=mf)
                if me is not None:
                    pltpu.store(ref.at[lead + (l, tiles[r], tail)], z, mask=me)

    for copy in col_copies[2:]:
        copy.wait()
    await_rows(send_row.at[0], sent)
    await_rows(recv_row.at[0], sent)


def finish_kernel(*refs):
    kept = refs[0:4]
    bands = refs[4:13]
    g_right, g_left, saved, ssaved = refs[13:17]
    final = refs[17:21]
    ends = refs[21:25]
    kgeo, sem = refs[25:27]
    levels, rows, cols = kept[1].shape
    nr, nc = rows // SUB, cols // LANE
    sub, lane = iotas()

    def send(src, dst, which):
        pltpu.make_async_copy(src, dst, sem.at[which]).start()

    def part(ref, a, b, *lead):
        rest = (slice(None),) * (len(ref.shape) - 2 - len(lead))
        return ref.at[lead + rest + (slice(a, b), slice(None))]

    changed = [(0, 1), (1, 0), (1, 1), (1, 1), (1, 2), (1, 1), (2, 1)]
    array_of = (0, 0, 1, 2, 3, 3, 3)
    src_of, end_of, dst_of = planes(*kept), planes(*ends), planes(*final)
    if nr > 2:
        for i, (a, b) in enumerate(zip(kept, final)):
            send(part(a, SUB, rows - SUB), part(b, SUB, rows - SUB), i)
    for (src, lead), (dst, _), (n_top, n_low), which in zip(src_of, dst_of, changed, array_of):
        for a, b in ((n_top, SUB), (rows - SUB, rows - n_low)):
            send(part(src, a, b, *lead), part(dst, a, b, *lead), which)

    strips = Strips(levels, cols)
    low, top = slice(0, SUB), slice(rows, rows + SUB)
    first_rows, last_rows = slice(0, SUB), slice(rows - SUB, rows)

    def border(g):
        a, b = roll(g[last_rows], 2, 0), roll(g[first_rows], -2, 0)
        return jnp.where(sub < 2, a, jnp.where(sub >= 6, b, g[top]))

    band_geo = geo_views(bands[4:8])
    one = (1, 1)
    const = lambda t: Field(one, lambda r, c: t)
    sides = border(g_right), border(g_left)
    own_levels = strips.own_levels(bands[:4], low)
    own_geo = [strips.own(f, low) for f in band_geo]
    area = strips.own(view(bands[8]), low)
    x = [const(strips.with_level(k, own_levels[k], *sides)) for k in range(8)]
    raw = [const(strips.with_geo(k, own_geo[k], *sides)) for k in range(14)]
    for c in range(nc):
        at = span(0, c)
        put_geo(kgeo, at, [f(*at) for f in band_geo], bands[8][at])

    merge = (sub == 0) | (sub == SUB - 1)

    def swap_with(grid, load):
        return lambda i, f: Field(grid, lambda r, c: jnp.where(merge, load(i, c), f(r, c)))

    _, _, souts, sstages = strip_chain(
        one, x, raw, lambda r, c: area, swap_with(one, lambda i, c: ssaved[i])
    )
    grid = (1, nc)
    jobs = []
    for l in range(levels):
        jobs.append(
            run(
                grid,
                fields(grid, level_views(l, bands[:4])),
                band_geo[6:12],
                band_geo[0:3],
                [view(kgeo, k) for k in range(9)],
                swap_with(grid, lambda i, c, l=l: saved[i, l, :, span(0, c)[1]]),
            )[2:]
        )

    masks = strips.masks()

    def finalize(i):
        end, lead = end_of[i]
        dst = dst_of[i][0]
        n_top, n_low = changed[i]
        y = souts[i](0, 0)
        zs = [pick(y, strips.back[l]) for l in range(levels)]
        for l in range(levels):
            for c in range(nc):
                t = jobs[l][0][i](0, c)
                for m, at in zip(masks[i], (0, nc - 1)):
                    if m is not None and at == c:
                        t = jnp.where(m, zs[l], t)
                end[lead + (l,) + span(0, c)] = t
        if n_top:
            send(part(end, 6, 6 + n_top, *lead), part(dst, 0, n_top, *lead), array_of[i])
        if n_low:
            send(part(end, 2 - n_low, 2, *lead), part(dst, rows - n_low, rows, *lead), array_of[i])

    ready = [(), (0, 1, 2), (3,), (4, 5, 6)]
    for stage, done in enumerate(ready):
        for _, stages in jobs:
            build(stages[stage])
        build(sstages[stage])
        for i in done:
            finalize(i)
    for i, (a, b) in enumerate(zip(kept, final)):
        pltpu.make_async_copy(a, b, sem.at[i]).wait()


def local(counts, vel, th, vt, tt, cd, el, area, kite, cor):
    args = (vel, th, vt, tt, cd, el, kite, cor, area)
    levels, rows, cols = th.shape
    outs = [(2, levels, rows, cols), (levels, rows, cols), (levels, rows, cols), (3, levels, rows, cols)]
    short = lambda s, n: s[:-2] + (n, cols)
    hbm, vmem = pl.BlockSpec(memory_space=pl.ANY), pl.BlockSpec(memory_space=pltpu.VMEM)
    side = (rows + SUB, LANE)
    passed = outs + [short(a.shape, SUB) for a in args]
    passed += [side, side, (2, levels, SUB, cols), (2, SUB, LANE)]
    kept = pl.pallas_call(
        lambda *refs: main_kernel(counts, *refs),
        out_shape=[pltpu.VMEM(s, F32) for s in passed],
        in_specs=[hbm] * len(args),
        out_specs=[vmem] * len(passed),
        scratch_shapes=[pltpu.VMEM(a.shape, F32) for a in args]
        + [
            pltpu.VMEM((rows, LANE), F32),
            pltpu.VMEM((rows, LANE), F32),
            pltpu.VMEM((9, rows, cols), F32),
            pltpu.VMEM((8, rows, LANE), F32),
            pltpu.VMEM((15, rows, LANE), F32),
            pltpu.VMEM((8 * levels * rows, 1, cols), F32),
        ]
        + [pltpu.SemaphoreType.DMA((n,)) for n in (1 + PARTS, 2, 1, 1, 5, 5)],
        compiler_params=pltpu.CompilerParams(collective_id=0, has_side_effects=True),
        name="main",
    )(*args)
    return pl.pallas_call(
        finish_kernel,
        out_shape=[jax.ShapeDtypeStruct(s, F32) for s in outs],
        in_specs=[vmem] * len(passed),
        out_specs=[pl.BlockSpec(memory_space=pltpu.HBM)] * len(outs),
        scratch_shapes=[pltpu.VMEM(short(s, SUB), F32) for s in outs]
        + [pltpu.VMEM((9, SUB, cols), F32), pltpu.SemaphoreType.DMA((4,))],
        name="finish",
    )(*[pltpu.with_memory_space_constraint(x, pltpu.VMEM) for x in kept])


def solution(mesh):
    counts = (mesh.shape["py"], mesh.shape["px"])
    p4, p3 = P(None, None, "py", "px"), P(None, "py", "px")
    return jax.shard_map(
        lambda *args: local(counts, *args),
        mesh=mesh,
        in_specs=(p4, p3, p4, p3, p3, p3, P("py", "px"), p4, p3),
        out_specs=(p4, p3, p3, p4),
        check_vma=False,
    )
```
